128 devices in a mesh: row: 8 (over z, core), col: 16 (over y, x).
Axes of the slice: x: 4, y: 4, z: 4, core: 2. Of those that a mesh axis runs over, the one named last changes fastest.
Arguments:
- load_amp: float32 [4096, 8192], P('row', 'col'), may hold values from 0.05 to 1
- load_mask: int32 [4096, 8192], P('row', 'col'), may hold values 0 or 1
- leak: float32 [4096, 8192], P('row', 'col'), may hold values from 0.001 to 0.05
- coarse_leak: float32 [1024, 2048], P('row', 'col'), may hold values from 0.01 to 0.5
- coarse_init: float32 [1024, 2048], P('row', 'col'), may hold values from 0 to 1
- via_fine: int32 [8, 32768], P('row', 'col'), may hold values from 0 to 262143
- via_coarse: int32 [8, 32768], P('row', 'col'), may hold values from 0 to 262143, as said below
- via_count: int32 [8, 256], P('row', 'col'), may hold values from 0 to 128, as said below
Outputs:
- fine_drop: float32 [4096, 8192], P('row', 'col')
- coarse_drop: float32 [1024, 2048], P('row', 'col')
The draws below stay inside these ranges and needn't reach their ends.
Inputs may be any that keep to these rules, and one draw needn't show every extreme that they name: `via_coarse`: slot s of a tile names a coarse node whose stored column lies in s // 128 * 128 to s // 128 * 128 + 127. `via_count`: slots of an owner past its count are padding and carry arbitrary indices. In each tile row some owner gets 128 live slots from every tile of that row.
All inputs are finite; a program needn't handle non-finite values. No bound on the sum of `load_mask` on one device may be relied on, other than what follows from the above.
Results may differ from the reference program's by a relative error of at most 0.00022.
Values sent between devices are 32-bit elements; how exact they have to be, the bound alone decides.
A program may use at most 64 MiB of HBM per device.

```python
import math
import jax
import jax.numpy as jnp

FR = 512
FC = 512
CR = 128
CC = 128
GROUP = 16
VOWN = 128
ITERS = 4
OUTER = 1
CSWEEP = 2
NFR = 4096
NFC = 8192
NCR = 1024
NCC = 2048
VMAX = 2048
N_ROW = 8
N_COL = 16


def draw_via_coarse(key, part):
    columns = NCC // CC
    tiles_down = NCR // CR
    slot_all = jnp.arange(columns * VMAX, dtype=jnp.int32)
    owner = slot_all % VMAX // VOWN
    key_row, key_col = jax.random.split(jax.random.fold_in(key, 11))
    shape = (tiles_down, columns * VMAX)
    row_pick = jax.random.randint(key_row, shape, 0, CR, dtype=jnp.int32)
    col_pick = jax.random.randint(key_col, shape, 0, CC, dtype=jnp.int32)
    return (row_pick * NCC + owner[None, :] * CC + col_pick).astype(jnp.int32)


def draw_via_count(key, part):
    columns = NCC // CC
    tiles_down = NCR // CR
    key_base, key_full = jax.random.split(jax.random.fold_in(key, 23))
    base = jax.random.randint(key_base, (tiles_down, columns * columns), 0, VOWN + 1, dtype=jnp.int32)
    chosen = jax.random.randint(key_full, (tiles_down, 1), 0, columns, dtype=jnp.int32)
    owner = jnp.arange(columns * columns, dtype=jnp.int32) % columns
    return jnp.where(owner[None, :] == chosen, VOWN, base).astype(jnp.int32)


def touch_ends(array, stream_key, low, high):
    shape = array.shape
    place = [jax.random.randint(jax.random.fold_in(stream_key, axis), (), 0, shape[axis]) for axis in range(len(shape))]
    array = array.at[tuple(place)].set(low)
    longest = shape.index(max(shape))
    place[longest] = (place[longest] + 1) % shape[longest]
    return array.at[tuple(place)].set(high)


def levels(own_key, dims, cuts, low, top_value):
    level, own = 1.0, jax.random.fold_in(own_key, 6)
    for dim, blocks in cuts:
        draws = jnp.exp(jax.random.uniform(jax.random.fold_in(own, dim), (blocks,), jnp.float32, low / len(cuts), top_value / len(cuts)))
        level = level * jnp.repeat(draws, dims[dim] // blocks).reshape([-1 if axis == dim else 1 for axis in range(len(dims))])
    return level


def setup_inputs(seed: int = 0) -> dict:
    key_of = jax.random.split(jax.random.key(seed), 9)
    load_amp = jnp.clip(jnp.exp(math.log(1.0) - 2.9957323 * jax.random.uniform(key_of[0], (NFR, NFC), jnp.float32) ** levels(key_of[0], (NFR, NFC), ((0, 8), (1, 16)), -0.2, 0.2)), 0.05, 1.0)
    load_mask = touch_ends((jax.random.randint(key_of[1], (NFR, NFC), 0, 2) < 1).astype(jnp.int32), jax.random.fold_in(key_of[1], 1), 0, 1)
    leak = jnp.clip(jnp.exp(math.log(0.05) - 3.912023 * jax.random.uniform(key_of[2], (NFR, NFC), jnp.float32) ** levels(key_of[2], (NFR, NFC), ((0, 8), (1, 16)), -0.2, 0.2)), 0.001, 0.05)
    coarse_leak = jnp.clip(jnp.exp(math.log(0.5) - 3.912023 * jax.random.uniform(key_of[3], (NCR, NCC), jnp.float32) ** levels(key_of[3], (NCR, NCC), ((0, 8), (1, 16)), -0.2, 0.2)), 0.01, 0.5)
    coarse_init = jnp.clip(1.0 * jax.random.uniform(key_of[4], (NCR, NCC), jnp.float32) ** levels(key_of[4], (NCR, NCC), ((0, 8), (1, 16)), -0.2, 0.2), 0.0, 1.0)
    via_fine = touch_ends(jax.random.randint(key_of[5], (N_ROW, VMAX * N_COL), 0, FR * FC), jax.random.fold_in(key_of[5], 1), 0, (FR * FC) - 1).astype(jnp.int32)
    via_coarse = draw_via_coarse(jax.random.fold_in(key_of[8], 71), 0)
    via_count = draw_via_count(jax.random.fold_in(key_of[8], 71), 0)
    return {"load_amp": load_amp, "load_mask": load_mask, "leak": leak, "coarse_leak": coarse_leak, "coarse_init": coarse_init, "via_fine": via_fine, "via_coarse": via_coarse, "via_count": via_count}


via_conductance = 2.0
coarse_conductance = 4.0
relaxation = 0.8


def fine_apply(field, diagonal):
    padded = jnp.pad(field, 1)
    beside = padded[2:, 1:-1] + padded[:-2, 1:-1] + padded[1:-1, 2:] + padded[1:-1, :-2]
    return diagonal * field - beside


def to_physical(stored):
    return stored.reshape(NCR, N_COL, CC // GROUP, GROUP).transpose(0, 2, 1, 3).reshape(NCR, NCC)


def to_stored(physical):
    return physical.reshape(NCR, CC // GROUP, N_COL, GROUP).transpose(0, 2, 1, 3).reshape(NCR, NCC)


def coarse_apply(stored, diagonal):
    padded = jnp.pad(to_physical(stored), 1)
    beside = padded[2:, 1:-1] + padded[:-2, 1:-1] + padded[1:-1, 2:] + padded[1:-1, :-2]
    return diagonal * stored - coarse_conductance * to_stored(beside)


def reference(load_amp, load_mask, leak, coarse_leak, coarse_init, via_fine, via_coarse, via_count):
    tile_row = jnp.arange(N_ROW, dtype=jnp.int32)[:, None]
    slot_all = jnp.arange(N_COL * VMAX, dtype=jnp.int32)[None, :]
    tile_col = slot_all // VMAX
    within = slot_all % VMAX
    owner = within // VOWN
    position = within % VOWN
    count_index = jnp.broadcast_to(tile_col * N_COL + owner, via_fine.shape).astype(jnp.int32)
    counts = jnp.take_along_axis(via_count, count_index, axis=1)
    weight = jnp.where(position < counts, via_conductance, 0.0).astype(jnp.float32).reshape(-1)
    fine_index = ((tile_row * FR + via_fine // FC) * NFC + tile_col * FC + via_fine % FC).reshape(-1)
    coarse_index = ((tile_row * CR + via_coarse // NCC) * NCC + via_coarse % NCC).reshape(-1)
    fine_diag = 4.0 + leak + jnp.zeros(NFR * NFC, jnp.float32).at[fine_index].add(weight).reshape(NFR, NFC)
    coarse_diag = 4.0 * coarse_conductance + coarse_leak + jnp.zeros(NCR * NCC, jnp.float32).at[coarse_index].add(weight).reshape(NCR, NCC)
    load = load_amp * load_mask.astype(jnp.float32)
    volt = coarse_init
    solution = jnp.zeros((NFR, NFC), jnp.float32)
    for outer_turn in range(OUTER):
        at_via = volt.reshape(-1)[coarse_index]
        rhs = load + jnp.zeros(NFR * NFC, jnp.float32).at[fine_index].add(weight * at_via).reshape(NFR, NFC)
        residual = rhs - fine_apply(solution, fine_diag)
        precond = residual / fine_diag
        direction = precond
        product = jnp.sum(residual * precond)
        for iteration in range(ITERS):
            image = fine_apply(direction, fine_diag)
            alpha = product / jnp.sum(direction * image)
            solution = solution + alpha * direction
            residual = residual - alpha * image
            if iteration + 1 < ITERS:
                precond = residual / fine_diag
                renewed = jnp.sum(residual * precond)
                direction = precond + (renewed / product) * direction
                product = renewed
        at_fine = weight * solution.reshape(-1)[fine_index]
        sources = jnp.zeros(NCR * NCC, jnp.float32).at[coarse_index].add(at_fine).reshape(NCR, NCC)
        for sweep_turn in range(CSWEEP):
            volt = volt + relaxation * (sources - coarse_apply(volt, coarse_diag)) / coarse_diag
    return solution, volt
```

```python
import functools

import jax
import jax.numpy as jnp
from jax import lax
from jax.experimental import pallas as pl
from jax.experimental.pallas import tpu as pltpu
from jax.sharding import PartitionSpec as P

MESH = pl.DeviceIdType.MESH
F32, BF16, I32 = jnp.float32, jnp.bfloat16, jnp.int32
GROUP = 16
NB = 4
OWN = 16
TILE = 512
ROWS = TILE + 2 * OWN
COARSE = 128
VIA = 2.0
CG = 4.0
RELAX = 0.8
NN = (((1,), (0,)), ((), ()))
NT = (((1,), (1,)), ((), ()))


def iota(shape, dim):
    return lax.broadcasted_iota(I32, shape, dim)


def dot(a, b, dims):
    return lax.dot_general(a, b, dims, preferred_element_type=F32)


def parts(x, n):
    out = []
    for _ in range(n):
        p = x.astype(BF16)
        out.append(p)
        x = x - p.astype(F32)
    return out


def kernel(
    nrow, ncol,
    amp_h, mask_h, leak_h, cleak, cinit, vfine, vcoarse, vcount,
    fine_h, coarse_o,
    amp, mask, leak, rt, ct, cva, cvb, field, dinv, diag, inj,
    req, held, look, atvia, vals, arrived,
    crow, ccol, tbig, htop, hbot, hleft, hright, hcorner, csend,
    mom, red_a, red_b, outb, ubuf, seam, crecv, srecv,
    in_sem, out_sem, rq_s, rq_r, rs_s, rs_r, ar_s, ar_r,
    ha_s, ha_r, ra_s, ra_r, rb_s, rb_r, ce_s, ce_r,
):
    slots = ncol * 128
    ri, ci = lax.axis_index("row"), lax.axis_index("col")

    loads = []
    for n, (src, dst) in enumerate(((leak_h, leak), (amp_h, amp), (mask_h, mask))):
        for j in range(NB):
            cp = pltpu.make_async_copy(src.at[:, pl.ds(j * 128, 128)], dst.at[j], in_sem.at[n, j])
            cp.start()
            loads.append(cp)

    for buf in (htop, hbot, hleft, hright, hcorner, crecv):
        buf[...] = jnp.zeros(buf.shape, F32)

    bar = pltpu.get_barrier_semaphore()
    for d in range(1, ncol):
        pl.semaphore_signal(bar, inc=1, device_id={"col": lax.rem(ci + d, ncol)}, device_id_type=MESH)
    for d in range(1, nrow):
        pl.semaphore_signal(bar, inc=1, device_id={"row": lax.rem(ri + d, nrow)}, device_id_type=MESH)
    for dr in (1, nrow - 1):
        for dc in (1, ncol - 1):
            pl.semaphore_signal(
                bar, inc=1,
                device_id={"row": lax.rem(ri + dr, nrow), "col": lax.rem(ci + dc, ncol)},
                device_id_type=MESH,
            )
    pl.semaphore_wait(bar, ncol + nrow + 2)

    lane = iota((1, 128), 1)

    def exchange(src, dst, ssem, rsem):
        cps = []
        for d in range(1, ncol):
            cp = pltpu.make_async_remote_copy(
                src_ref=src.at[d], dst_ref=dst.at[ci], send_sem=ssem.at[d], recv_sem=rsem.at[d],
                device_id={"col": lax.rem(ci + d, ncol)}, device_id_type=MESH,
            )
            cp.start()
            cps.append(cp)
        return cps

    def make_req(d, _):
        o = lax.rem(ci + d, ncol)
        idx = vcoarse[:, pl.ds(pl.multiple_of(o * 128, 128), 128)]
        node = lax.shift_right_logical(idx, lax.full_like(idx, (slots).bit_length() - 1)) * 128 + (idx & 127)
        r = jnp.where(lane < vcount[0, o], node, -1)
        req[d] = r
        return _

    lax.fori_loop(0, ncol, make_req, 0)
    held[ci] = req[0]
    rq = exchange(req, held, rq_s, rq_r)

    def make_fine(o, _):
        at = pl.ds(pl.multiple_of(o * 128, 128), 128)
        idx = vfine[:, at]
        live = lane < vcount[0, o]
        r = jnp.where(live, idx >> 9, -1)
        c = idx & 511
        for q in range(4):
            i = iota((128, 128), 0) + q * 128
            rt[q * 128:(q + 1) * 128, at] = jnp.where(i == r, 1.0, 0.0).astype(BF16)
            ct[q * 128:(q + 1) * 128, at] = jnp.where(i == c, 1.0, 0.0).astype(BF16)
        return _

    lax.fori_loop(0, ncol, make_fine, 0)
    for cp in loads[:NB]:
        cp.wait()
    for h in range(2):
        t = dot(rt[...], ct[h * 256:(h + 1) * 256, :], NT)
        for q in range(2):
            j = 2 * h + q
            dg = 4.0 + leak[j] + VIA * t[:, q * 128:(q + 1) * 128]
            diag[j] = dg
            dinv[j, OWN:OWN + TILE] = 1.0 / dg

    row8 = iota((8, 128), 1)

    def halo_copies(f, src):
        up, dn = lax.rem(ri + nrow - 1, nrow), lax.rem(ri + 1, nrow)
        lf, rg = lax.rem(ci + ncol - 1, ncol), lax.rem(ci + 1, ncol)
        hu, hd, hl, hr = ri > 0, ri < nrow - 1, ci > 0, ci < ncol - 1
        first, last = pl.ds(OWN, 8), pl.ds(OWN + TILE - 8, 8)
        own = pl.ds(0, NB)
        plan = (
            (hu, hd, src.at[own, first], hbot.at[f], {"row": up}),
            (hd, hu, src.at[own, last], htop.at[f], {"row": dn}),
            (hl, hr, csend.at[f, 0], hright.at[f], {"col": lf}),
            (hr, hl, csend.at[f, 1], hleft.at[f], {"col": rg}),
            (hu & hl, hd & hr, src.at[0, first], hcorner.at[f, 0], {"row": up, "col": lf}),
            (hu & hr, hd & hl, src.at[NB - 1, first], hcorner.at[f, 1], {"row": up, "col": rg}),
            (hd & hl, hu & hr, src.at[0, last], hcorner.at[f, 2], {"row": dn, "col": lf}),
            (hd & hr, hu & hl, src.at[NB - 1, last], hcorner.at[f, 3], {"row": dn, "col": rg}),
        )
        out = []
        for n, (to, frm, s, d, dev) in enumerate(plan):
            cp = pltpu.make_async_remote_copy(
                src_ref=s, dst_ref=d, send_sem=ha_s.at[f, n], recv_sem=ha_r.at[f, n],
                device_id=dev, device_id_type=MESH,
            )
            out.append((to, frm, cp))
        return out

    def halo_start(f, src):
        own = slice(OWN, OWN + TILE)
        csend[f, 0] = jnp.transpose(src[0, own])[:8]
        csend[f, 1] = jnp.transpose(src[NB - 1, own])[120:]
        cps = halo_copies(f, src)
        for to, _, cp in cps:
            pl.when(to)(cp.start)
        return cps

    def halo_finish(f, dst, cps):
        for _, frm, cp in cps:
            pl.when(frm)(cp.wait_recv)
        dst[0:NB, OWN - 8:OWN] = htop[f]
        dst[0:NB, OWN + TILE:OWN + TILE + 8] = hbot[f]
        x = jnp.concatenate([hright[f], jnp.zeros((112, TILE), F32), hleft[f]], axis=0)
        dst[NB, OWN:OWN + TILE] = jnp.transpose(x)
        near = row8 < 64
        dst[NB, OWN + TILE:OWN + TILE + 8] = jnp.where(near, hcorner[f, 0], hcorner[f, 1])
        dst[NB, OWN - 8:OWN] = jnp.where(near, hcorner[f, 2], hcorner[f, 3])

    def halo_sent(cps):
        for to, _, cp in cps:
            pl.when(to)(cp.wait_send)

    for buf in (dinv, field.at[0], field.at[1], field.at[2], field.at[3]):
        buf[:, 0:8] = jnp.zeros((NB + 1, 8, 128), F32)
        buf[:, ROWS - 8:ROWS] = jnp.zeros((NB + 1, 8, 128), F32)
    dcp = halo_start(0, dinv)

    u = cinit[...]
    uparts = parts(u, 3)
    ci128 = iota((128, 128), 0)
    for d in range(ncol):
        k = lax.rem(ci + ncol - d, ncol)
        if d:
            rq[d - 1].wait_recv()
        at = pl.ds(pl.multiple_of(k * 128, 128), 128)
        idx = held[k]
        crow[:, at] = jnp.where(ci128 == (idx >> 7), 1.0, 0.0).astype(BF16)
        ccol[:, at] = jnp.where(ci128 == (idx & 127), 1.0, 0.0).astype(BF16)
    t = dot(uparts[0], ccol[...], NN)
    for p in uparts[1:]:
        t = t + dot(p, ccol[...], NN)
    tbig[...] = t
    for d in range(ncol):
        k = lax.rem(ci + d, ncol)
        at = pl.ds(pl.multiple_of(k * 128, 128), 128)
        idx = held[k]
        look[d] = jnp.sum(jnp.where(ci128 == (idx >> 7), tbig[:, at], 0.0), axis=0, keepdims=True)
    atvia[ci] = look[0]
    rs = exchange(look, atvia, rs_s, rs_r)

    cdiag = 4.0 * CG + cleak[...] + VIA * dot(crow[...], ccol[...], NT)
    rdiag = RELAX / cdiag

    def coarse_start(s, u):
        ubuf[s] = u
        seam_t = jnp.transpose(u)
        tbig[:, 0:128] = seam_t
        for e, j in enumerate((0, GROUP - 1)):
            seam[s, e] = jnp.concatenate(
                [seam_t[g * GROUP + j:g * GROUP + j + 1] for g in range(128 // GROUP)], axis=0
            )
        up, dn = lax.rem(ri + nrow - 1, nrow), lax.rem(ri + 1, nrow)
        lf, rg = lax.rem(ci + ncol - 1, ncol), lax.rem(ci + 1, ncol)
        true = ri >= 0
        plan = (
            (ri > 0, ri < nrow - 1, ubuf.at[s, pl.ds(0, 8)], crecv.at[s, 1], {"row": up}),
            (ri < nrow - 1, ri > 0, ubuf.at[s, pl.ds(120, 8)], crecv.at[s, 0], {"row": dn}),
            (None, None, seam.at[s, 0], srecv.at[s, 1], {"col": lf}),
            (None, None, seam.at[s, 1], srecv.at[s, 0], {"col": rg}),
        )
        cps = []
        for n, (to, frm, sr, ds, dev) in enumerate(plan):
            cp = pltpu.make_async_remote_copy(
                src_ref=sr, dst_ref=ds, send_sem=ce_s.at[s, n], recv_sem=ce_r.at[s, n],
                device_id=dev, device_id_type=MESH,
            )
            if to is None:
                cp.start()
            else:
                pl.when(to)(cp.start)
            cps.append((to, frm, cp))
        return cps

    def coarse_beside(s, u, cps):
        for _, frm, cp in cps:
            if frm is None:
                cp.wait_recv()
            else:
                pl.when(frm)(cp.wait_recv)
        li, si = iota((128, 128), 1), ci128
        up = jnp.where(si == 0, crecv[s, 0, 7:8, :], pltpu.roll(u, 1, 0))
        dn = jnp.where(si == 127, crecv[s, 1, 0:1, :], pltpu.roll(u, 127, 0))
        g = iota((8, 128), 0)
        fl, fr = srecv[s, 0], srecv[s, 1]
        fl = jnp.where(ci == 0, jnp.where(g == 0, 0.0, pltpu.roll(fl, 1, 0)), fl)
        fr = jnp.where(ci == ncol - 1, jnp.where(g == 7, 0.0, pltpu.roll(fr, 7, 0)), fr)

        def spread(x):
            return jnp.concatenate([jnp.broadcast_to(x[q:q + 1], (GROUP, 128)) for q in range(8)], axis=0)

        x = jnp.transpose(jnp.where(si % GROUP == 0, spread(fl), spread(fr)))
        left = jnp.where(li % GROUP == 0, x, pltpu.roll(u, 1, 1))
        right = jnp.where(li % GROUP == GROUP - 1, x, pltpu.roll(u, 127, 1))
        return up + dn + left + right

    def coarse_sent(cps):
        for to, _, cp in cps:
            if to is None:
                cp.wait_send()
            else:
                pl.when(to)(cp.wait_send)

    c0 = coarse_start(0, u)
    for cp in loads[NB:]:
        cp.wait()
    halo_finish(0, dinv, dcp)

    def make_inj(o):
        at = pl.ds(pl.multiple_of(o * 128, 128), 128)
        p = parts(atvia[o], 2)
        col = ct[:, at]
        cva[:, at] = col * p[0]
        cvb[:, at] = col * p[1]

    for d in range(ncol):
        if d:
            rs[d - 1].wait_recv()
        make_inj(lax.rem(ci + ncol - d, ncol))
    v0 = field.at[0]
    for h in range(2):
        hs = slice(h * 256, (h + 1) * 256)
        t = dot(rt[...], cva[hs, :], NT) + dot(rt[...], cvb[hs, :], NT)
        for q in range(2):
            j = 2 * h + q
            rhs = amp[j] * mask[j].astype(F32) + VIA * t[:, q * 128:(q + 1) * 128]
            v0[j, OWN:OWN + TILE] = rhs * dinv[j, OWN:OWN + TILE]
    fcp = halo_start(1, v0)
    halo_finish(1, v0, fcp)

    first_lane, last_lane = row8 == 0, row8 == 127

    def beside(v, r):
        c = [v[j, pl.ds(r, 8)] for j in range(NB + 1)]
        rr = [pltpu.roll(x, 1, 1) for x in c]
        rl = [pltpu.roll(x, 127, 1) for x in c]
        out = []
        for j in range(NB + 1):
            left = jnp.where(first_lane, rr[(j - 1) % (NB + 1)], rr[j])
            right = jnp.where(last_lane, rl[(j + 1) % (NB + 1)], rl[j])
            out.append(v[j, pl.ds(r - 1, 8)] + v[j, pl.ds(r + 1, 8)] + left + right)
        return c, out

    def power(k):
        v, nxt = field.at[k], field.at[k + 1] if k < 3 else None
        count = (4, 4, 2, 1)[k]

        def rows(r, sums):
            c, nb = beside(v, r)
            sums = list(sums) if sums is not None else None
            for j in range(NB + 1):
                w = None
                if nxt is not None:
                    w = dinv[j, pl.ds(r, 8)] * nb[j]
                    nxt[j, pl.ds(r, 8)] = w
                if sums is not None and j < NB:
                    dv = diag[j, pl.ds(r - OWN, 8)] * c[j]
                    av = dv - nb[j]
                    sums[0] += c[j] * av
                    if count > 1:
                        sums[1] += w * av
                    if count > 2:
                        sums[2] += c[j] * dv
                        sums[3] += c[j] * nb[j]
            return tuple(sums) if sums is not None else None

        if nxt is not None:
            rows(OWN - 8, None)
            rows(OWN + TILE, None)

        def step(i, sums):
            return rows(pl.multiple_of(OWN + i * 8, 8), sums)

        z = jnp.zeros((8, 128), F32)
        return lax.fori_loop(0, TILE // 8, step, (z,) * count, unroll=2)

    n = 0
    for k in range(4):
        for s in power(k):
            mom[n // 8, n % 8:n % 8 + 1] = jnp.sum(s, axis=0, keepdims=True)
            n += 1
    mom[1, 3:8] = jnp.zeros((5, 128), F32)

    def reduce(src, buf, axis, me, size, ssem, rsem):
        cps = []
        for d in range(1, size):
            cp = pltpu.make_async_remote_copy(
                src_ref=src, dst_ref=buf.at[me], send_sem=ssem.at[d], recv_sem=rsem.at[d],
                device_id={axis: lax.rem(me + d, size)}, device_id_type=MESH,
            )
            cp.start()
            cps.append(cp)
        buf[me] = src[...]
        for cp in cps:
            cp.wait_recv()
        t = buf[0]
        for q in range(1, size):
            t = t + buf[q]
        for cp in cps:
            cp.wait_send()
        return t

    mom[...] = reduce(mom, red_a, "col", ci, ncol, ra_s, ra_r)
    tot = reduce(mom, red_b, "row", ri, nrow, rb_s, rb_r)
    tot = jnp.sum(tot, axis=2, keepdims=True)

    def m(q):
        return jnp.broadcast_to(tot[q // 8, q % 8:q % 8 + 1], (1, 128))

    eta = [m(q) for q in (0, 1, 4, 5, 8, 9, 10)]
    nu = [m(q) for q in (2, 3, 6, 7)]
    hm = [[eta[i + j] for j in range(4)] for i in range(4)]
    low = [[None] * 4 for _ in range(4)]
    piv = []
    for j in range(4):
        pj = hm[j][j]
        for q in range(j):
            pj = pj - low[j][q] * low[j][q] * piv[q]
        ok = pj > 1e-6 * hm[j][j]
        piv.append(pj)
        inv = jnp.where(ok, 1.0 / jnp.where(ok, pj, 1.0), 0.0)
        low[j][j] = inv
        for i in range(j + 1, 4):
            e = hm[i][j]
            for q in range(j):
                e = e - low[i][q] * low[j][q] * piv[q]
            low[i][j] = e * inv
    y = list(nu)
    for i in range(4):
        for q in range(i):
            y[i] = y[i] - low[i][q] * y[q]
    y = [y[i] * low[i][i] for i in range(4)]
    for i in (2, 1, 0):
        for q in range(i + 1, 4):
            y[i] = y[i] - low[q][i] * y[q]
    coef = [jnp.broadcast_to(c, (8, 128)) for c in y]

    def combine(i, _):
        r = pl.multiple_of(i * 16, 16)
        for j in range(NB):
            at = slice(j * 128, (j + 1) * 128)
            acc = []
            for q in range(2):
                rq_ = pl.ds(OWN + r + 8 * q, 8)
                a = coef[0] * field[0, j, rq_]
                for k in range(1, 4):
                    a = a + coef[k] * field[k, j, rq_]
                acc.append(a)
            a = jnp.concatenate(acc, axis=0)
            outb[pl.ds(r, 16), at] = a
            pa, pb = parts(a, 2)
            cva[pl.ds(r, 16), at] = pa
            cvb[pl.ds(r, 16), at] = pb
        return _

    lax.fori_loop(0, TILE // 16, combine, 0)
    ocp = pltpu.make_async_copy(outb, fine_h, out_sem)
    ocp.start()

    for o in range(0, ncol, 2):
        at = slice(o * 128, (o + 2) * 128)
        t = dot(cva[:, 0:TILE], ct[:, at], NN) + dot(cvb[:, 0:TILE], ct[:, at], NN)
        s = VIA * jnp.sum(t * rt[:, at].astype(F32), axis=0, keepdims=True)
        vals[o] = s[:, 0:128]
        vals[o + 1] = s[:, 128:256]
    arrived[ci] = vals[ci]
    ar = []
    for d in range(1, ncol):
        o = lax.rem(ci + d, ncol)
        cp = pltpu.make_async_remote_copy(
            src_ref=vals.at[o], dst_ref=arrived.at[ci], send_sem=ar_s.at[d], recv_sem=ar_r.at[d],
            device_id={"col": o}, device_id_type=MESH,
        )
        cp.start()
        ar.append(cp)

    p0 = u + rdiag * (CG * coarse_beside(0, u, c0) - cdiag * u)

    src = jnp.zeros((128, 128), F32)
    for d in range(ncol):
        if d:
            ar[d - 1].wait_recv()
        k = lax.rem(ci + ncol - d, ncol)
        at = pl.ds(pl.multiple_of(k * 128, 128), 128)
        pp = parts(arrived[k], 3)
        col = ccol[:, at]
        for n in range(3):
            rt[n * 128:(n + 1) * 128, at] = col * pp[n]
    for n in range(3):
        src = src + dot(crow[...], rt[n * 128:(n + 1) * 128, :], NT)
    u1 = p0 + rdiag * src
    c1 = coarse_start(1, u1)
    coarse_o[...] = u1 + rdiag * (src + CG * coarse_beside(1, u1, c1) - cdiag * u1)

    for cp in rq + rs + ar:
        cp.wait_send()
    halo_sent(dcp)
    halo_sent(fcp)
    coarse_sent(c0)
    coarse_sent(c1)
    ocp.wait()


def solution(mesh):
    nrow, ncol = mesh.shape["row"], mesh.shape["col"]
    slots = ncol * 128
    dma = pltpu.SemaphoreType.DMA

    def step(*args):
        vm = pl.BlockSpec(memory_space=pltpu.VMEM)
        anyspace = pl.BlockSpec(memory_space=pl.ANY)
        slab = (NB, TILE, 128)
        row = (ncol, 1, 128)
        return pl.pallas_call(
            functools.partial(kernel, nrow, ncol),
            out_shape=(
                jax.ShapeDtypeStruct((TILE, TILE), F32),
                jax.ShapeDtypeStruct((COARSE, COARSE), F32),
            ),
            in_specs=[anyspace, anyspace, anyspace, vm, vm, vm, vm, pl.BlockSpec(memory_space=pltpu.SMEM)],
            out_specs=(anyspace, vm),
            scratch_shapes=[
                pltpu.VMEM(slab, F32), pltpu.VMEM(slab, I32), pltpu.VMEM(slab, F32),
                pltpu.VMEM((TILE, slots), BF16), pltpu.VMEM((TILE, slots), BF16),
                pltpu.VMEM((TILE, slots), BF16), pltpu.VMEM((TILE, slots), BF16),
                pltpu.VMEM((4, NB + 1, ROWS, 128), F32), pltpu.VMEM((NB + 1, ROWS, 128), F32),
                pltpu.VMEM(slab, F32), pltpu.VMEM((8, 128), F32),
                pltpu.VMEM(row, I32), pltpu.VMEM(row, I32), pltpu.VMEM(row, F32), pltpu.VMEM(row, F32),
                pltpu.VMEM(row, F32), pltpu.VMEM(row, F32),
                pltpu.VMEM((128, slots), BF16), pltpu.VMEM((128, slots), BF16), pltpu.VMEM((128, slots), F32),
                pltpu.VMEM((2, NB, 8, 128), F32), pltpu.VMEM((2, NB, 8, 128), F32),
                pltpu.VMEM((2, 8, TILE), F32), pltpu.VMEM((2, 8, TILE), F32),
                pltpu.VMEM((2, 4, 8, 128), F32), pltpu.VMEM((2, 2, 8, TILE), F32),
                pltpu.VMEM((2, 8, 128), F32), pltpu.VMEM((ncol, 2, 8, 128), F32), pltpu.VMEM((nrow, 2, 8, 128), F32),
                pltpu.VMEM((TILE, TILE), F32),
                pltpu.VMEM((2, 128, 128), F32), pltpu.VMEM((2, 2, 8, 128), F32),
                pltpu.VMEM((2, 2, 8, 128), F32), pltpu.VMEM((2, 2, 8, 128), F32),
                dma((3, NB)), dma(()),
                dma((ncol,)), dma((ncol,)), dma((ncol,)), dma((ncol,)), dma((ncol,)), dma((ncol,)),
                dma((2, 8)), dma((2, 8)), dma((ncol,)), dma((ncol,)), dma((nrow,)), dma((nrow,)),
                dma((2, 4)), dma((2, 4)),
            ],
            compiler_params=pltpu.CompilerParams(collective_id=0, has_side_effects=True, vmem_limit_bytes=50 << 20),
        )(*args)

    spec = P("row", "col")
    return jax.shard_map(
        step, mesh=mesh, in_specs=(spec,) * 8, out_specs=(spec, spec), check_vma=False
    )
```

```python
import functools

import jax
import jax.numpy as jnp
from jax import lax
from jax.experimental import pallas as pl
from jax.experimental.pallas import tpu as pltpu
from jax.sharding import PartitionSpec as P

MESH = pl.DeviceIdType.MESH
F32, BF16, I32 = jnp.float32, jnp.bfloat16, jnp.int32
GROUP = 16
NB = 4
OWN = 16
TILE = 512
ROWS = TILE + 2 * OWN
COARSE = 128
VIA = 2.0
CG = 4.0
RELAX = 0.8
NN = (((1,), (0,)), ((), ()))
NT = (((1,), (1,)), ((), ()))


def iota(shape, dim):
    return lax.broadcasted_iota(I32, shape, dim)


def dot(a, b, dims):
    return lax.dot_general(a, b, dims, preferred_element_type=F32)


def parts(x, n):
    out = []
    for _ in range(n):
        p = x.astype(BF16)
        out.append(p)
        x = x - p.astype(F32)
    return out


class Phases:
    def __init__(self):
        self.open = None

    def __call__(self, name):
        if self.open is not None:
            self.open.__exit__(None, None, None)
        self.open = None
        if name:
            self.open = jax.named_scope(name)
            self.open.__enter__()


def peer_order(n):
    if n != 16:
        return list(range(n))
    return sorted(range(n), key=lambda d: min(d // 4, 4 - d // 4) + min(d % 4, 4 - d % 4))


def kernel(
    nrow, ncol,
    amp_h, mask_h, leak_h, cleak_h, cinit_h, vfine_h, vcoarse_h, vcount_h,
    fine_o, coarse_o,
    amp, mask, leak, rt, ct, cva, cvb, field, dinv, diag, inj, pa, pb,
    req, held, look, atvia, vals, arrived,
    crow, ccol, htop, hbot, hleft, hright, hcorner, csend,
    mom, red_a, red_b, split, ubuf, seam, crecv, srecv,
    cleak, cinit, vfine, vcoarse, vcount,
    in_sem, small_sem, rq_s, rq_r, rs_s, rs_r, ar_s, ar_r,
    ha_s, ha_r, ra_s, ra_r, rb_s, rb_r, ce_s, ce_r,
):
    slots = ncol * 128
    phase = Phases()
    phase("start")
    ri, ci = lax.axis_index("row"), lax.axis_index("col")

    small = []
    for n, (src, dst) in enumerate((
        (vcount_h, vcount), (vcoarse_h, vcoarse), (vfine_h, vfine), (cinit_h, cinit), (cleak_h, cleak)
    )):
        cp = pltpu.make_async_copy(src, dst, small_sem.at[n])
        cp.start()
        small.append(cp)
    loads = []
    for n, (src, dst) in enumerate(((leak_h, leak), (amp_h, amp), (mask_h, mask))):
        for j in range(NB):
            cp = pltpu.make_async_copy(src.at[:, pl.ds(j * 128, 128)], dst.at[j], in_sem.at[n, j])
            cp.start()
            loads.append(cp)

    for buf in (htop, hbot, hleft, hright, hcorner, crecv):
        buf[...] = jnp.zeros(buf.shape, F32)

    phase("barrier")
    order = peer_order(ncol)

    def peer(p, sign):
        if ncol != 16:
            return lax.rem(ci + (order[p] if sign > 0 else ncol - order[p]), ncol)
        dy, dx = order[p] // 4, order[p] % 4
        y, x = ci // 4, lax.rem(ci, 4)
        if sign < 0:
            dy, dx = 4 - dy, 4 - dx
        return lax.rem(y + dy, 4) * 4 + lax.rem(x + dx, 4)

    bar = pltpu.get_barrier_semaphore()
    for d in range(1, ncol):
        pl.semaphore_signal(bar, inc=1, device_id={"col": lax.rem(ci + d, ncol)}, device_id_type=MESH)
    for d in range(1, nrow):
        pl.semaphore_signal(bar, inc=1, device_id={"row": lax.rem(ri + d, nrow)}, device_id_type=MESH)
    for dr in (1, nrow - 1):
        for dc in (1, ncol - 1):
            pl.semaphore_signal(
                bar, inc=1,
                device_id={"row": lax.rem(ri + dr, nrow), "col": lax.rem(ci + dc, ncol)},
                device_id_type=MESH,
            )
    phase("wait_small")
    for cp in small:
        cp.wait()
    lane = iota((1, 128), 1)

    def exchange(src, dst, ssem, rsem, sign):
        cps = []
        for p in reversed(range(1, ncol)):
            cp = pltpu.make_async_remote_copy(
                src_ref=src.at[p], dst_ref=dst.at[p], send_sem=ssem.at[p], recv_sem=rsem.at[p],
                device_id={"col": peer(p, sign)}, device_id_type=MESH,
            )
            cp.start()
            cps.append(cp)
        return cps[::-1]

    phase("fine_onehot")
    for p in range(ncol):
        o = peer(p, 1)
        idx = vfine[:, pl.ds(pl.multiple_of(o * 128, 128), 128)]
        at = slice(p * 128, (p + 1) * 128)
        r = jnp.where(lane < vcount[0, o], idx >> 9, -1)
        c = idx & 511
        for q in range(4):
            i = iota((128, 128), 0) + q * 128
            rt[q * 128:(q + 1) * 128, at] = jnp.where(i == r, 1.0, 0.0).astype(BF16)
            ct[q * 128:(q + 1) * 128, at] = jnp.where(i == c, 1.0, 0.0).astype(BF16)
    phase("count_dot")
    for cp in loads[:NB]:
        cp.wait()
    for h in range(2):
        t = dot(rt[...], ct[h * 256:(h + 1) * 256, :], NT)
        for q in range(2):
            j = 2 * h + q
            dg = 4.0 + leak[j] + VIA * t[:, q * 128:(q + 1) * 128]
            diag[j] = dg
            dinv[j, OWN:OWN + TILE] = 1.0 / dg

    phase("barrier_wait")
    pl.semaphore_wait(bar, ncol + nrow + 2)

    phase("requests")
    for p in reversed(range(ncol)):
        o = peer(p, 1)
        idx = vcoarse[:, pl.ds(pl.multiple_of(o * 128, 128), 128)]
        node = lax.shift_right_logical(idx, lax.full_like(idx, (slots).bit_length() - 1)) * 128 + (idx & 127)
        (req if p else held)[p] = jnp.where(lane < vcount[0, o], node, -1)
    rq = exchange(req, held, rq_s, rq_r, 1)

    row8 = iota((8, 128), 1)

    def halo_copies(f, src):
        up, dn = lax.rem(ri + nrow - 1, nrow), lax.rem(ri + 1, nrow)
        lf, rg = lax.rem(ci + ncol - 1, ncol), lax.rem(ci + 1, ncol)
        hu, hd, hl, hr = ri > 0, ri < nrow - 1, ci > 0, ci < ncol - 1
        first, last = pl.ds(OWN, 8), pl.ds(OWN + TILE - 8, 8)
        own = pl.ds(0, NB)
        plan = (
            (hu, hd, src.at[own, first], hbot.at[f], {"row": up}),
            (hd, hu, src.at[own, last], htop.at[f], {"row": dn}),
            (hl, hr, csend.at[f, 0], hright.at[f], {"col": lf}),
            (hr, hl, csend.at[f, 1], hleft.at[f], {"col": rg}),
            (hu & hl, hd & hr, src.at[0, first], hcorner.at[f, 0], {"row": up, "col": lf}),
            (hu & hr, hd & hl, src.at[NB - 1, first], hcorner.at[f, 1], {"row": up, "col": rg}),
            (hd & hl, hu & hr, src.at[0, last], hcorner.at[f, 2], {"row": dn, "col": lf}),
            (hd & hr, hu & hl, src.at[NB - 1, last], hcorner.at[f, 3], {"row": dn, "col": rg}),
        )
        out = []
        for n, (to, frm, s, d, dev) in enumerate(plan):
            cp = pltpu.make_async_remote_copy(
                src_ref=s, dst_ref=d, send_sem=ha_s.at[f, n], recv_sem=ha_r.at[f, n],
                device_id=dev, device_id_type=MESH,
            )
            out.append((to, frm, cp))
        return out

    def halo_start(f, src):
        own = slice(OWN, OWN + TILE)
        csend[f, 0] = jnp.transpose(src[0, own])[:8]
        csend[f, 1] = jnp.transpose(src[NB - 1, own])[120:]
        cps = halo_copies(f, src)
        for to, _, cp in cps:
            pl.when(to)(cp.start)
        return cps

    def halo_finish(f, dst, cps):
        for _, frm, cp in cps:
            pl.when(frm)(cp.wait_recv)
        dst[0:NB, OWN - 8:OWN] = htop[f]
        dst[0:NB, OWN + TILE:OWN + TILE + 8] = hbot[f]
        x = jnp.concatenate([hright[f], jnp.zeros((112, TILE), F32), hleft[f]], axis=0)
        dst[NB, OWN:OWN + TILE] = jnp.transpose(x)
        near = row8 < 64
        dst[NB, OWN + TILE:OWN + TILE + 8] = jnp.where(near, hcorner[f, 0], hcorner[f, 1])
        dst[NB, OWN - 8:OWN] = jnp.where(near, hcorner[f, 2], hcorner[f, 3])

    def halo_sent(cps):
        for to, _, cp in cps:
            pl.when(to)(cp.wait_send)

    phase("dinv_halo")
    for buf in (dinv, field.at[0], field.at[1], field.at[2], field.at[3]):
        buf[:, 0:8] = jnp.zeros((NB + 1, 8, 128), F32)
        buf[:, ROWS - 8:ROWS] = jnp.zeros((NB + 1, 8, 128), F32)
    dcp = halo_start(0, dinv)

    phase("wait_req")
    u = cinit[...]
    split[0:256] = jnp.concatenate(parts(u, 2), axis=0)
    ci128 = iota((128, 128), 0)
    for p in range(ncol):
        if p:
            rq[p - 1].wait_recv()
        at = slice(p * 128, (p + 1) * 128)
        idx = held[p]
        crow[:, at] = jnp.where(ci128 == (idx >> 7), 1.0, 0.0).astype(BF16)
        ccol[:, at] = jnp.where(ci128 == (idx & 127), 1.0, 0.0).astype(BF16)
    phase("lookup")
    rs = [None] * ncol
    for n in reversed(range(ncol // 2)):
        at = slice(n * 256, (n + 1) * 256)
        t = dot(split[0:256], ccol[:, at], NN)
        t = jnp.sum((t[:128] + t[128:]) * crow[:, at].astype(F32), axis=0, keepdims=True)
        for p in (2 * n + 1, 2 * n):
            (look if p else atvia)[p] = t[:, (p - 2 * n) * 128:(p - 2 * n + 1) * 128]
            if p:
                rs[p] = pltpu.make_async_remote_copy(
                    src_ref=look.at[p], dst_ref=atvia.at[p], send_sem=rs_s.at[p], recv_sem=rs_r.at[p],
                    device_id={"col": peer(p, -1)}, device_id_type=MESH,
                )
                rs[p].start()
    rs = rs[1:]

    phase("coarse_diag")
    cdiag = 4.0 * CG + cleak[...] + VIA * dot(crow[...], ccol[...], NT)
    rdiag = RELAX / cdiag

    def coarse_start(s, u):
        ubuf[s] = u
        seam_t = jnp.transpose(u)
        for e, j in enumerate((0, GROUP - 1)):
            seam[s, e] = jnp.concatenate(
                [seam_t[g * GROUP + j:g * GROUP + j + 1] for g in range(128 // GROUP)], axis=0
            )
        up, dn = lax.rem(ri + nrow - 1, nrow), lax.rem(ri + 1, nrow)
        lf, rg = lax.rem(ci + ncol - 1, ncol), lax.rem(ci + 1, ncol)
        true = ri >= 0
        plan = (
            (ri > 0, ri < nrow - 1, ubuf.at[s, pl.ds(0, 8)], crecv.at[s, 1], {"row": up}),
            (ri < nrow - 1, ri > 0, ubuf.at[s, pl.ds(120, 8)], crecv.at[s, 0], {"row": dn}),
            (None, None, seam.at[s, 0], srecv.at[s, 1], {"col": lf}),
            (None, None, seam.at[s, 1], srecv.at[s, 0], {"col": rg}),
        )
        cps = []
        for n, (to, frm, sr, ds, dev) in enumerate(plan):
            cp = pltpu.make_async_remote_copy(
                src_ref=sr, dst_ref=ds, send_sem=ce_s.at[s, n], recv_sem=ce_r.at[s, n],
                device_id=dev, device_id_type=MESH,
            )
            if to is None:
                cp.start()
            else:
                pl.when(to)(cp.start)
            cps.append((to, frm, cp))
        return cps

    def coarse_beside(s, u, cps):
        for _, frm, cp in cps:
            if frm is None:
                cp.wait_recv()
            else:
                pl.when(frm)(cp.wait_recv)
        li, si = iota((128, 128), 1), ci128
        up = jnp.where(si == 0, crecv[s, 0, 7:8, :], pltpu.roll(u, 1, 0))
        dn = jnp.where(si == 127, crecv[s, 1, 0:1, :], pltpu.roll(u, 127, 0))
        g = iota((8, 128), 0)
        fl, fr = srecv[s, 0], srecv[s, 1]
        fl = jnp.where(ci == 0, jnp.where(g == 0, 0.0, pltpu.roll(fl, 1, 0)), fl)
        fr = jnp.where(ci == ncol - 1, jnp.where(g == 7, 0.0, pltpu.roll(fr, 7, 0)), fr)

        def spread(x):
            return jnp.concatenate([jnp.broadcast_to(x[q:q + 1], (GROUP, 128)) for q in range(8)], axis=0)

        x = jnp.transpose(jnp.where(si % GROUP == 0, spread(fl), spread(fr)))
        left = jnp.where(li % GROUP == 0, x, pltpu.roll(u, 1, 1))
        right = jnp.where(li % GROUP == GROUP - 1, x, pltpu.roll(u, 127, 1))
        return up + dn + left + right

    def coarse_sent(cps):
        for to, _, cp in cps:
            if to is None:
                cp.wait_send()
            else:
                pl.when(to)(cp.wait_send)

    phase("coarse_start")
    c0 = coarse_start(0, u)
    for cp in loads[NB:]:
        cp.wait()
    phase("dinv_finish")
    halo_finish(0, dinv, dcp)

    def make_inj(o):
        at = pl.ds(pl.multiple_of(o * 128, 128), 128)
        p = parts(atvia[o], 2)
        col = ct[:, at]
        cva[:, at] = col * p[0]
        cvb[:, at] = col * p[1]

    v0 = field.at[0]
    half = ncol // 2
    for part in range(2):
        phase(f"wait_resp{part}")
        for p in range(part * half, (part + 1) * half):
            if p:
                rs[p - 1].wait_recv()
            at = slice(p * 128, (p + 1) * 128)
            pp = parts(atvia[p], 2)
            col = ct[:, at]
            cva[:, at] = col * pp[0]
            cvb[:, at] = col * pp[1]
        phase(f"inject_dot{part}")
        ks = slice(part * half * 128, (part + 1) * half * 128)
        for h in range(2):
            hs = slice(h * 256, (h + 1) * 256)
            t = dot(rt[:, ks], cva[hs, ks], NT) + dot(rt[:, ks], cvb[hs, ks], NT)
            for q in range(2):
                j = 2 * h + q
                tq = VIA * t[:, q * 128:(q + 1) * 128]
                if part == 0:
                    inj[j] = amp[j] * mask[j].astype(F32) + tq
                else:
                    z = (inj[j] + tq) * dinv[j, OWN:OWN + TILE]
                    v0[j, OWN:OWN + TILE] = z
                    za, zb = parts(z, 2)
                    pa[0, :, j * 128:(j + 1) * 128] = za
                    pb[0, :, j * 128:(j + 1) * 128] = zb
    phase("halo_start")
    fcp = halo_start(1, v0)

    def gather(k):
        for n in range(ncol // 2):
            at = slice(n * 256, (n + 1) * 256)
            t = dot(pa[k], ct[:, at], NN) + dot(pb[k], ct[:, at], NN)
            t = VIA * jnp.sum(t * rt[:, at].astype(F32), axis=0, keepdims=True)
            for p in (2 * n, 2 * n + 1):
                (vals if p else arrived)[p, k:k + 1] = t[:, (p - 2 * n) * 128:(p - 2 * n + 1) * 128]

    phase("gather0")
    gather(0)
    phase("halo_finish")
    halo_finish(1, v0, fcp)

    phase("powers")
    def beside(v, r, h):
        lanes = iota((h, 128), 1)
        first_lane, last_lane = lanes == 0, lanes == 127
        c = [v[j, pl.ds(r, h)] for j in range(NB + 1)]
        rr = [pltpu.roll(x, 1, 1) for x in c]
        rl = [pltpu.roll(x, 127, 1) for x in c]
        out = []
        for j in range(NB + 1):
            left = jnp.where(first_lane, rr[(j - 1) % (NB + 1)], rr[j])
            right = jnp.where(last_lane, rl[(j + 1) % (NB + 1)], rl[j])
            out.append(v[j, pl.ds(r - 1, h)] + v[j, pl.ds(r + 1, h)] + left + right)
        return c, out

    def power(k):
        v, nxt = field.at[k], field.at[k + 1] if k < 3 else None
        count = (4, 4, 2, 1)[k]

        def rows(r, h, sums):
            c, nb = beside(v, r, h)
            sums = list(sums) if sums is not None else None

            def add(n, x):
                for q in range(h // 8):
                    sums[n] = sums[n] + x[q * 8:(q + 1) * 8]

            for j in range(NB + 1):
                w = None
                if nxt is not None:
                    w = dinv[j, pl.ds(r, h)] * nb[j]
                    nxt[j, pl.ds(r, h)] = w
                if sums is not None and j < NB:
                    if nxt is not None:
                        wa, wb = parts(w, 2)
                        pa[k + 1, pl.ds(r - OWN, h), j * 128:(j + 1) * 128] = wa
                        pb[k + 1, pl.ds(r - OWN, h), j * 128:(j + 1) * 128] = wb
                    dv = diag[j, pl.ds(r - OWN, h)] * c[j]
                    av = dv - nb[j]
                    add(0, c[j] * av)
                    if count > 1:
                        add(1, w * av)
                    if count > 2:
                        add(2, c[j] * dv)
                        add(3, c[j] * nb[j])
            return tuple(sums) if sums is not None else None

        if nxt is not None:
            rows(OWN - 8, 8, None)
            rows(OWN + TILE, 8, None)

        def step(i, sums):
            return rows(pl.multiple_of(OWN + i * 16, 16), 16, sums)

        z = jnp.zeros((8, 128), F32)
        return lax.fori_loop(0, TILE // 16, step, (z,) * count, unroll=4)

    n = 0
    for k in range(4):
        for s in power(k):
            mom[n:n + 1] = jnp.sum(s, axis=0, keepdims=True)
            n += 1
    mom[11:16] = jnp.zeros((5, 128), F32)

    phase("lane_sum")
    t = jnp.sum(mom[...], axis=1, keepdims=True)
    red_a[ci] = jnp.sum(jnp.where(iota((16, 128), 0) == iota((16, 128), 1), t, 0.0), axis=0, keepdims=True)

    def reduce_start(buf, axis, me, size, ssem, rsem):
        cps = []
        for d in range(1, size):
            cp = pltpu.make_async_remote_copy(
                src_ref=buf.at[me], dst_ref=buf.at[me], send_sem=ssem.at[d], recv_sem=rsem.at[d],
                device_id={axis: lax.rem(me + d, size)}, device_id_type=MESH,
            )
            cp.start()
            cps.append(cp)
        return cps

    def reduce_finish(buf, size, cps):
        for cp in cps:
            cp.wait_recv()
        t = buf[0]
        for q in range(1, size):
            t = t + buf[q]
        return t

    ra = reduce_start(red_a, "col", ci, ncol, ra_s, ra_r)
    phase("gather1")
    gather(1)
    phase("reduce_col")
    red_b[ri] = reduce_finish(red_a, ncol, ra)
    rb = reduce_start(red_b, "row", ri, nrow, rb_s, rb_r)
    phase("gather23")
    gather(2)
    gather(3)
    ar = exchange(vals, arrived, ar_s, ar_r, 1)
    phase("sweep_pre")
    p0 = u + rdiag * (CG * coarse_beside(0, u, c0) - cdiag * u)
    phase("reduce_row")
    tot = reduce_finish(red_b, nrow, rb)

    phase("solve")
    def m(q):
        return jnp.broadcast_to(jnp.sum(jnp.where(lane == q, tot, 0.0), axis=1, keepdims=True), (1, 128))

    eta = [m(q) for q in (0, 1, 4, 5, 8, 9, 10)]
    nu = [m(q) for q in (2, 3, 6, 7)]
    hm = [[eta[i + j] for j in range(4)] for i in range(4)]
    low = [[None] * 4 for _ in range(4)]
    piv = []
    for j in range(4):
        pj = hm[j][j]
        for q in range(j):
            pj = pj - low[j][q] * low[j][q] * piv[q]
        ok = pj > 1e-6 * hm[j][j]
        piv.append(pj)
        inv = jnp.where(ok, 1.0 / jnp.where(ok, pj, 1.0), 0.0)
        low[j][j] = inv
        for i in range(j + 1, 4):
            e = hm[i][j]
            for q in range(j):
                e = e - low[i][q] * low[j][q] * piv[q]
            low[i][j] = e * inv
    y = list(nu)
    for i in range(4):
        for q in range(i):
            y[i] = y[i] - low[i][q] * y[q]
    y = [y[i] * low[i][i] for i in range(4)]
    for i in (2, 1, 0):
        for q in range(i + 1, 4):
            y[i] = y[i] - low[q][i] * y[q]
    phase("combine")

    def combine(i, _):
        r = pl.multiple_of(i * 16, 16)
        for j in range(NB):
            rows = pl.ds(OWN + r, 16)
            a = y[0] * field[0, j, rows]
            for k in range(1, 4):
                a = a + y[k] * field[k, j, rows]
            fine_o[pl.ds(r, 16), j * 128:(j + 1) * 128] = a
        return _

    lax.fori_loop(0, TILE // 16, combine, 0, unroll=4)

    phase("wait_vals")
    for p in range(ncol):
        if p:
            ar[p - 1].wait_recv()
        at = slice(p * 128, (p + 1) * 128)
        a = y[0] * arrived[p, 0:1]
        for k in range(1, 4):
            a = a + y[k] * arrived[p, k:k + 1]
        hot = crow[:, at]
        for n, x in enumerate(parts(a, 2)):
            cva[n * 128:(n + 1) * 128, at] = hot * x
    phase("sources")
    t = dot(cva[0:256, :], ccol[...], NT)
    src = t[:128] + t[128:]
    u1 = p0 + rdiag * src
    phase("edges1")
    c1 = coarse_start(1, u1)
    phase("sweep2")
    coarse_o[...] = u1 + rdiag * (src + CG * coarse_beside(1, u1, c1) - cdiag * u1)

    phase("drain")
    for cp in rq + rs + ar + ra + rb:
        cp.wait_send()
    halo_sent(dcp)
    halo_sent(fcp)
    coarse_sent(c0)
    coarse_sent(c1)
    phase("")


def solution(mesh):
    nrow, ncol = mesh.shape["row"], mesh.shape["col"]
    slots = ncol * 128
    dma = pltpu.SemaphoreType.DMA

    def step(*args):
        vm = pl.BlockSpec(memory_space=pltpu.VMEM)
        anyspace = pl.BlockSpec(memory_space=pl.ANY)
        hbm = pl.BlockSpec(memory_space=pltpu.HBM)
        slab = (NB, TILE, 128)
        row = (ncol, 1, 128)
        return pl.pallas_call(
            functools.partial(kernel, nrow, ncol),
            out_shape=(
                pltpu.VMEM((TILE, TILE), F32),
                pltpu.VMEM((COARSE, COARSE), F32),
            ),
            in_specs=[hbm] * 8,
            out_specs=(vm, vm),
            scratch_shapes=[
                pltpu.VMEM(slab, F32), pltpu.VMEM(slab, I32), pltpu.VMEM(slab, F32),
                pltpu.VMEM((TILE, slots), BF16), pltpu.VMEM((TILE, slots), BF16),
                pltpu.VMEM((TILE, slots), BF16), pltpu.VMEM((TILE, slots), BF16),
                pltpu.VMEM((4, NB + 1, ROWS, 128), F32), pltpu.VMEM((NB + 1, ROWS, 128), F32),
                pltpu.VMEM(slab, F32), pltpu.VMEM(slab, F32),
                pltpu.VMEM((4, TILE, TILE), BF16), pltpu.VMEM((4, TILE, TILE), BF16),
                pltpu.VMEM(row, I32), pltpu.VMEM(row, I32), pltpu.VMEM(row, F32), pltpu.VMEM(row, F32),
                pltpu.VMEM((ncol, 4, 128), F32), pltpu.VMEM((ncol, 4, 128), F32),
                pltpu.VMEM((128, slots), BF16), pltpu.VMEM((128, slots), BF16),
                pltpu.VMEM((2, NB, 8, 128), F32), pltpu.VMEM((2, NB, 8, 128), F32),
                pltpu.VMEM((2, 8, TILE), F32), pltpu.VMEM((2, 8, TILE), F32),
                pltpu.VMEM((2, 4, 8, 128), F32), pltpu.VMEM((2, 2, 8, TILE), F32),
                pltpu.VMEM((16, 128), F32), pltpu.VMEM((ncol, 1, 128), F32), pltpu.VMEM((nrow, 1, 128), F32),
                pltpu.VMEM((256, 128), BF16),
                pltpu.VMEM((2, 128, 128), F32), pltpu.VMEM((2, 2, 8, 128), F32),
                pltpu.VMEM((2, 2, 8, 128), F32), pltpu.VMEM((2, 2, 8, 128), F32),
                pltpu.VMEM((COARSE, COARSE), F32), pltpu.VMEM((COARSE, COARSE), F32),
                pltpu.VMEM((1, slots), I32), pltpu.VMEM((1, slots), I32), pltpu.SMEM((1, ncol), I32),
                dma((3, NB)), dma((5,)),
                dma((ncol,)), dma((ncol,)), dma((ncol,)), dma((ncol,)), dma((ncol,)), dma((ncol,)),
                dma((2, 8)), dma((2, 8)), dma((ncol,)), dma((ncol,)), dma((nrow,)), dma((nrow,)),
                dma((2, 4)), dma((2, 4)),
            ],
            compiler_params=pltpu.CompilerParams(collective_id=0, has_side_effects=True, vmem_limit_bytes=50 << 20),
        )(*[pltpu.with_memory_space_constraint(x, pltpu.HBM) for x in args])

    spec = P("row", "col")
    return jax.shard_map(
        step, mesh=mesh, in_specs=(spec,) * 8, out_specs=(spec, spec), check_vma=False
    )
```

```python
import functools

import jax
import jax.numpy as jnp
from jax import lax
from jax.experimental import pallas as pl
from jax.experimental.pallas import tpu as pltpu
from jax.sharding import PartitionSpec as P

MESH = pl.DeviceIdType.MESH
F32, BF16, I32 = jnp.float32, jnp.bfloat16, jnp.int32
GROUP = 16
NB = 4
OWN = 16
TILE = 512
ROWS = TILE + 2 * OWN
COARSE = 128
FUSED = ()
VIA = 2.0
CG = 4.0
RELAX = 0.8
NN = (((1,), (0,)), ((), ()))
NT = (((1,), (1,)), ((), ()))


def place(c):
    return (c & 3) * 128 + (c >> 2)


def iota(shape, dim):
    return lax.broadcasted_iota(I32, shape, dim)


def dot(a, b, dims):
    return lax.dot_general(a, b, dims, preferred_element_type=F32)


def parts(x, n):
    out = []
    for _ in range(n):
        p = x.astype(BF16)
        out.append(p)
        x = x - p.astype(F32)
    return out


class Phases:
    def __init__(self):
        self.open = None

    def __call__(self, name):
        if self.open is not None:
            self.open.__exit__(None, None, None)
        self.open = None
        if name:
            self.open = jax.named_scope(name)
            self.open.__enter__()


def peer_order(n):
    if n != 16:
        return list(range(n))
    return sorted(range(n), key=lambda d: min(d // 4, 4 - d // 4) + min(d % 4, 4 - d % 4))


def kernel(
    nrow, ncol,
    amp_h, mask_h, leak_h, cleak_h, cinit_h, vfine_h, vcoarse_h, vcount_h,
    fine_o, coarse_o,
    amp, mask, leak, perm, rt, ct, cva, cvb, f0, f1, f2, f3, turned, dinv, diag, inj, pa0, pa1, pa2, pa3, pb0, pb1, pb2, pb3,
    req, held, look, atvia, vals, arrived,
    crow, ccol, htop, hbot, hleft, hright, hcorner, csend, corner,
    mom, red_a, red_b, split, ubuf, seam, crecv, srecv,
    cleak, cinit, vfine, vcoarse, vcount,
    in_sem, small_sem, rq_s, rq_r, rs_s, rs_r, ar_s, ar_r,
    ha_s, ha_r, ra_s, ra_r, rb_s, rb_r, ce_s, ce_r,
):
    field, pa, pb = (f0, f1, f2, f3), (pa0, pa1, pa2, pa3), (pb0, pb1, pb2, pb3)
    slots = ncol * 128
    phase = Phases()
    phase("start")
    ri, ci = lax.axis_index("row"), lax.axis_index("col")

    small = []
    for n, (src, dst) in enumerate((
        (vcount_h, vcount), (vcoarse_h, vcoarse), (vfine_h, vfine), (cinit_h, cinit), (cleak_h, cleak)
    )):
        cp = pltpu.make_async_copy(src, dst, small_sem.at[n])
        cp.start()
        small.append(cp)
    loads = []
    for n, (src, dst) in enumerate(((leak_h, leak), (amp_h, amp), (mask_h, mask))):
        cp = pltpu.make_async_copy(src, dst, in_sem.at[n])
        cp.start()
        loads.append(cp)

    for buf in (htop, hbot, hleft, hright, hcorner, crecv, csend):
        buf[...] = jnp.zeros(buf.shape, F32)

    phase("barrier")
    order = peer_order(ncol)

    def peer(p, sign):
        if ncol != 16:
            return lax.rem(ci + (order[p] if sign > 0 else ncol - order[p]), ncol)
        dy, dx = order[p] // 4, order[p] % 4
        y, x = ci // 4, lax.rem(ci, 4)
        if sign < 0:
            dy, dx = 4 - dy, 4 - dx
        return lax.rem(y + dy, 4) * 4 + lax.rem(x + dx, 4)

    bar = pltpu.get_barrier_semaphore()
    for d in range(1, ncol):
        pl.semaphore_signal(bar, inc=1, device_id={"col": lax.rem(ci + d, ncol)}, device_id_type=MESH)
    for d in range(1, nrow):
        pl.semaphore_signal(bar, inc=1, device_id={"row": lax.rem(ri + d, nrow)}, device_id_type=MESH)
    for dr in (1, nrow - 1):
        for dc in (1, ncol - 1):
            pl.semaphore_signal(
                bar, inc=1,
                device_id={"row": lax.rem(ri + dr, nrow), "col": lax.rem(ci + dc, ncol)},
                device_id_type=MESH,
            )
    phase("wait_small")
    for cp in small:
        cp.wait()
    lane = iota((1, 128), 1)

    def exchange(src, dst, ssem, rsem, sign):
        cps = []
        for p in reversed(range(1, ncol)):
            cp = pltpu.make_async_remote_copy(
                src_ref=src.at[p], dst_ref=dst.at[p], send_sem=ssem.at[p], recv_sem=rsem.at[p],
                device_id={"col": peer(p, sign)}, device_id_type=MESH,
            )
            cp.start()
            cps.append(cp)
        return cps[::-1]

    phase("requests")
    for p in reversed(range(ncol)):
        o = peer(p, 1)
        idx = vcoarse[:, pl.ds(pl.multiple_of(o * 128, 128), 128)]
        node = lax.shift_right_logical(idx, lax.full_like(idx, (slots).bit_length() - 1)) * 128 + (idx & 127)
        (req if p else held)[p] = jnp.where(lane < vcount[0, o], node, -1)
    phase("barrier_wait")
    pl.semaphore_wait(bar, ncol + nrow + 2)

    phase("send_req")
    rq = exchange(req, held, rq_s, rq_r, 1)

    phase("fine_onehot")
    for p in range(ncol):
        o = peer(p, 1)
        idx = vfine[:, pl.ds(pl.multiple_of(o * 128, 128), 128)]
        at = slice(p * 128, (p + 1) * 128)
        r = jnp.where(lane < vcount[0, o], idx >> 9, -1)
        c = place(idx & 511)
        for q in range(4):
            i = iota((128, 128), 0) + q * 128
            rt[q * 128:(q + 1) * 128, at] = jnp.where(i == r, 1.0, 0.0).astype(BF16)
            ct[q * 128:(q + 1) * 128, at] = jnp.where(i == c, 1.0, 0.0).astype(BF16)
    perm[...] = jnp.where(place(iota((TILE, TILE), 0)) == iota((TILE, TILE), 1), 1.0, 0.0).astype(BF16)
    phase("count_dot")
    loads[0].wait()
    pa2[...], pb2[...] = parts(leak[...], 2)
    for h in range(2):
        hs = slice(h * 256, (h + 1) * 256)
        t = VIA * dot(rt[...], ct[hs, :], NT)
        t = t + (dot(pa2[...], perm[:, hs], NN) + dot(pb2[...], perm[:, hs], NN))
        for q in range(2):
            j = 2 * h + q
            dg = 4.0 + t[:, q * 128:(q + 1) * 128]
            diag[j] = dg
            dinv[j, OWN:OWN + TILE] = 1.0 / dg

    row8 = iota((8, 128), 1)

    def halo_copies(f, src):
        up, dn = lax.rem(ri + nrow - 1, nrow), lax.rem(ri + 1, nrow)
        lf, rg = lax.rem(ci + ncol - 1, ncol), lax.rem(ci + 1, ncol)
        hu, hd, hl, hr = ri > 0, ri < nrow - 1, ci > 0, ci < ncol - 1
        first, last = pl.ds(OWN, 8), pl.ds(OWN + TILE - 8, 8)
        own = pl.ds(0, NB)
        plan = (
            (hu, hd, src.at[own, first], hbot.at[f], {"row": up}),
            (hd, hu, src.at[own, last], htop.at[f], {"row": dn}),
            (hl, hr, csend.at[f, 0], hright.at[f], {"col": lf}),
            (hr, hl, csend.at[f, 1], hleft.at[f], {"col": rg}),
            (hu & hl, hd & hr, corner.at[f, 0], hcorner.at[f, 0], {"row": up, "col": lf}),
            (hu & hr, hd & hl, corner.at[f, 0], hcorner.at[f, 1], {"row": up, "col": rg}),
            (hd & hl, hu & hr, corner.at[f, 1], hcorner.at[f, 2], {"row": dn, "col": lf}),
            (hd & hr, hu & hl, corner.at[f, 1], hcorner.at[f, 3], {"row": dn, "col": rg}),
        )
        out = []
        for n, (to, frm, s, d, dev) in enumerate(plan):
            cp = pltpu.make_async_remote_copy(
                src_ref=s, dst_ref=d, send_sem=ha_s.at[f, n], recv_sem=ha_r.at[f, n],
                device_id=dev, device_id_type=MESH,
            )
            out.append((to, frm, cp))
        return out

    def halo_start(f, src):
        own = slice(OWN, OWN + TILE)
        for j in range(NB):
            t = jnp.transpose(src[j, own])
            csend[f, 0, j:j + 1] = t[0:1]
            csend[f, 1, 4 + j:5 + j] = t[127:128]
        for e, r in enumerate((OWN, OWN + TILE - 8)):
            x = jnp.zeros((8, 128), F32)
            for j in range(NB):
                b = src[j, r:r + 8]
                x = jnp.where(row8 == j, pltpu.roll(b, j, 1) if j else b, x)
                x = jnp.where(row8 == 124 + j, pltpu.roll(b, 125 + j, 1) if j < 3 else b, x)
            corner[f, e] = x
        cps = halo_copies(f, src)
        for to, _, cp in cps:
            pl.when(to)(cp.start)
        return cps

    def halo_finish(f, dst, cps):
        for _, frm, cp in cps:
            pl.when(frm)(cp.wait_recv)
        dst[0:NB, OWN - 8:OWN] = htop[f]
        dst[0:NB, OWN + TILE:OWN + TILE + 8] = hbot[f]
        x = jnp.concatenate([hright[f], jnp.zeros((112, TILE), F32), hleft[f]], axis=0)
        dst[NB, OWN:OWN + TILE] = jnp.transpose(x)
        near = row8 < 64
        dst[NB, OWN + TILE:OWN + TILE + 8] = jnp.where(near, hcorner[f, 0], hcorner[f, 1])
        dst[NB, OWN - 8:OWN] = jnp.where(near, hcorner[f, 2], hcorner[f, 3])

    def halo_sent(cps):
        for to, _, cp in cps:
            pl.when(to)(cp.wait_send)

    phase("dinv_halo")
    for buf in (dinv, f0, f1, f2, f3):
        buf[:, 0:8] = jnp.zeros((NB + 1, 8, 128), F32)
        buf[:, ROWS - 8:ROWS] = jnp.zeros((NB + 1, 8, 128), F32)
    dcp = halo_start(0, dinv)

    phase("wait_req")
    u = cinit[...]
    split[0:256] = jnp.concatenate(parts(u, 2), axis=0)
    ci128 = iota((128, 128), 0)
    for p in range(ncol):
        if p:
            rq[p - 1].wait_recv()
        at = slice(p * 128, (p + 1) * 128)
        idx = held[p]
        crow[:, at] = jnp.where(ci128 == (idx >> 7), 1.0, 0.0).astype(BF16)
        ccol[:, at] = jnp.where(ci128 == (idx & 127), 1.0, 0.0).astype(BF16)
    phase("lookup")
    for n in range(ncol // 2):
        at = slice(n * 256, (n + 1) * 256)
        t = dot(split[0:256], ccol[:, at], NN)
        t = jnp.sum((t[:128] + t[128:]) * crow[:, at].astype(F32), axis=0, keepdims=True)
        for p in (2 * n, 2 * n + 1):
            (look if p else atvia)[p] = t[:, (p - 2 * n) * 128:(p - 2 * n + 1) * 128]
    rs = exchange(look, atvia, rs_s, rs_r, -1)

    phase("coarse_diag")
    cdiag = 4.0 * CG + cleak[...] + VIA * dot(crow[...], ccol[...], NT)
    rdiag = RELAX / cdiag

    def coarse_start(s, u):
        ubuf[s] = u
        seam_t = jnp.transpose(u)
        for e, j in enumerate((0, GROUP - 1)):
            seam[s, e] = jnp.concatenate(
                [seam_t[g * GROUP + j:g * GROUP + j + 1] for g in range(128 // GROUP)], axis=0
            )
        up, dn = lax.rem(ri + nrow - 1, nrow), lax.rem(ri + 1, nrow)
        lf, rg = lax.rem(ci + ncol - 1, ncol), lax.rem(ci + 1, ncol)
        true = ri >= 0
        plan = (
            (ri > 0, ri < nrow - 1, ubuf.at[s, pl.ds(0, 8)], crecv.at[s, 1], {"row": up}),
            (ri < nrow - 1, ri > 0, ubuf.at[s, pl.ds(120, 8)], crecv.at[s, 0], {"row": dn}),
            (None, None, seam.at[s, 0], srecv.at[s, 1], {"col": lf}),
            (None, None, seam.at[s, 1], srecv.at[s, 0], {"col": rg}),
        )
        cps = []
        for n, (to, frm, sr, ds, dev) in enumerate(plan):
            cp = pltpu.make_async_remote_copy(
                src_ref=sr, dst_ref=ds, send_sem=ce_s.at[s, n], recv_sem=ce_r.at[s, n],
                device_id=dev, device_id_type=MESH,
            )
            if to is None:
                cp.start()
            else:
                pl.when(to)(cp.start)
            cps.append((to, frm, cp))
        return cps

    def coarse_beside(s, u, cps):
        for _, frm, cp in cps:
            if frm is None:
                cp.wait_recv()
            else:
                pl.when(frm)(cp.wait_recv)
        li, si = iota((128, 128), 1), ci128
        up = jnp.where(si == 0, crecv[s, 0, 7:8, :], pltpu.roll(u, 1, 0))
        dn = jnp.where(si == 127, crecv[s, 1, 0:1, :], pltpu.roll(u, 127, 0))
        g = iota((8, 128), 0)
        fl, fr = srecv[s, 0], srecv[s, 1]
        fl = jnp.where(ci == 0, jnp.where(g == 0, 0.0, pltpu.roll(fl, 1, 0)), fl)
        fr = jnp.where(ci == ncol - 1, jnp.where(g == 7, 0.0, pltpu.roll(fr, 7, 0)), fr)

        def spread(x):
            return jnp.concatenate([jnp.broadcast_to(x[q:q + 1], (GROUP, 128)) for q in range(8)], axis=0)

        x = jnp.transpose(jnp.where(si % GROUP == 0, spread(fl), spread(fr)))
        left = jnp.where(li % GROUP == 0, x, pltpu.roll(u, 1, 1))
        right = jnp.where(li % GROUP == GROUP - 1, x, pltpu.roll(u, 127, 1))
        return up + dn + left + right

    def coarse_sent(cps):
        for to, _, cp in cps:
            if to is None:
                cp.wait_send()
            else:
                pl.when(to)(cp.wait_send)

    phase("coarse_start")
    c0 = coarse_start(0, u)
    phase("load")
    for cp in loads[1:]:
        cp.wait()
    pa1[...], pb1[...] = parts(amp[...] * mask[...].astype(F32), 2)
    for h in range(2):
        hs = slice(h * 256, (h + 1) * 256)
        t = dot(pa1[...], perm[:, hs], NN) + dot(pb1[...], perm[:, hs], NN)
        for q in range(2):
            inj[2 * h + q] = t[:, q * 128:(q + 1) * 128]
    phase("dinv_finish")
    halo_finish(0, dinv, dcp)

    def make_inj(o):
        at = pl.ds(pl.multiple_of(o * 128, 128), 128)
        p = parts(atvia[o], 2)
        col = ct[:, at]
        cva[:, at] = col * p[0]
        cvb[:, at] = col * p[1]

    v0 = f0
    half = ncol // 2
    for part in range(2):
        phase(f"wait_resp{part}")
        for p in range(part * half, (part + 1) * half):
            if p:
                rs[p - 1].wait_recv()
            at = slice(p * 128, (p + 1) * 128)
            c = vfine[:, pl.ds(pl.multiple_of(peer(p, 1) * 128, 128), 128)]
            c = place(c & 511)
            v = atvia[p]
            va = v.astype(BF16).astype(F32)
            vb = v - va
            for q in range(4):
                hot = iota((128, 128), 0) + q * 128 == c
                cva[q * 128:(q + 1) * 128, at] = jnp.where(hot, va, 0.0).astype(BF16)
                cvb[q * 128:(q + 1) * 128, at] = jnp.where(hot, vb, 0.0).astype(BF16)
        phase(f"inject_dot{part}")
        ks = slice(part * half * 128, (part + 1) * half * 128)
        for h in range(2):
            hs = slice(h * 256, (h + 1) * 256)
            t = dot(rt[:, ks], cva[hs, ks], NT) + dot(rt[:, ks], cvb[hs, ks], NT)
            for q in range(2):
                j = 2 * h + q
                tq = VIA * t[:, q * 128:(q + 1) * 128]
                if part == 0:
                    inj[j] = inj[j] + tq
                else:
                    z = (inj[j] + tq) * dinv[j, OWN:OWN + TILE]
                    v0[j, OWN:OWN + TILE] = z
                    za, zb = parts(z, 2)
                    pa0[:, j * 128:(j + 1) * 128] = za
                    pb0[:, j * 128:(j + 1) * 128] = zb
    phase("halo_start")
    fcp = halo_start(1, v0)

    def gather_part(k, n):
        at = slice(n * 256, n * 256 + 256) if isinstance(n, int) else pl.ds(pl.multiple_of(n * 256, 256), 256)
        t = dot(pa[k][...], ct[:, at], NN) + dot(pb[k][...], ct[:, at], NN)
        t = VIA * jnp.sum(t * rt[:, at].astype(F32), axis=0, keepdims=True)
        vals[2 * n, k:k + 1] = t[:, :128]
        vals[2 * n + 1, k:k + 1] = t[:, 128:]

    def gather(k):
        for n in range(ncol // 2):
            gather_part(k, n)

    phase("gather0")
    gather(0)
    phase("halo_finish")
    halo_finish(1, v0, fcp)

    phase("powers")
    def turn(v, r, h):
        rows = pl.ds(r, h)
        first, last, halo = v[0, rows], v[NB - 1, rows], v[NB, rows]
        turned[0, rows] = pltpu.roll(last, 1, 1)
        turned[1, rows] = pltpu.roll(halo, 1, 1)
        turned[2, rows] = pltpu.roll(first, 127, 1)
        turned[3, rows] = pltpu.roll(halo, 127, 1)

    def beside(v, r, h):
        lanes = iota((h, 128), 1)
        first_lane, last_lane = lanes == 0, lanes == 127
        rows = pl.ds(r, h)
        c = [v[j, rows] for j in range(NB + 1)]
        last_r, halo_r, first_l, halo_l = (turned[q, rows] for q in range(4))
        left = [jnp.where(first_lane, halo_r, last_r), *c[:NB - 1], jnp.where(first_lane, last_r, halo_r)]
        right = [*c[1:NB], jnp.where(last_lane, halo_l, first_l), jnp.where(last_lane, first_l, halo_l)]
        out = [
            v[j, pl.ds(r - 1, h)] + v[j, pl.ds(r + 1, h)] + left[j] + right[j] for j in range(NB + 1)
        ]
        return c, out

    def power(k):
        v, nxt = field[k], field[k + 1] if k < 3 else None
        count = (4, 4, 2, 1)[k]

        def rows(r, h, sums):
            c, nb = beside(v, r, h)
            sums = list(sums) if sums is not None else None

            def add(n, x):
                for q in range(h // 8):
                    sums[n] = sums[n] + x[q * 8:(q + 1) * 8]

            for j in range(NB + 1):
                w = None
                if nxt is not None:
                    w = dinv[j, pl.ds(r, h)] * nb[j]
                    nxt[j, pl.ds(r, h)] = w
                if sums is not None and j < NB:
                    if nxt is not None:
                        wa, wb = parts(w, 2)
                        pa[k + 1][pl.ds(r - OWN, h), j * 128:(j + 1) * 128] = wa
                        pb[k + 1][pl.ds(r - OWN, h), j * 128:(j + 1) * 128] = wb
                    dv = diag[j, pl.ds(r - OWN, h)] * c[j]
                    av = dv - nb[j]
                    add(0, c[j] * av)
                    if count > 1:
                        add(1, w * av)
                    if count > 2:
                        add(2, c[j] * dv)
                        add(3, c[j] * nb[j])
            return tuple(sums) if sums is not None else None

        steps = ncol // 2 if k in FUSED else 8
        each = TILE // steps
        turn(v, OWN, each)
        if nxt is not None:
            for r in (OWN - 8, OWN + TILE):
                turn(v, r, 8)
                rows(r, 8, None)

        def step(i, sums, last=False):
            r = OWN + i * each if last else pl.multiple_of(OWN + i * each, 16)
            if k in FUSED:
                gather_part(k, i)
            if not last:
                turn(v, r + each, each)
            for q in range(each // 16):
                sums = rows(r + q * 16, 16, sums)
            return sums

        z = jnp.zeros((8, 128), F32)
        sums = lax.fori_loop(0, steps - 1, step, (z,) * count)
        return step(steps - 1, sums, last=True)

    n = 0
    for k in range(4):
        phase(f"power{k}")
        for s in power(k):
            mom[n:n + 1] = jnp.sum(s, axis=0, keepdims=True)
            n += 1
    mom[11:16] = jnp.zeros((5, 128), F32)

    phase("lane_sum")
    t = jnp.sum(mom[...], axis=1, keepdims=True)
    red_a[ci] = jnp.sum(jnp.where(iota((16, 128), 0) == iota((16, 128), 1), t, 0.0), axis=0, keepdims=True)

    def reduce_start(buf, axis, me, size, ssem, rsem):
        cps = []
        for d in range(1, size):
            cp = pltpu.make_async_remote_copy(
                src_ref=buf.at[me], dst_ref=buf.at[me], send_sem=ssem.at[d], recv_sem=rsem.at[d],
                device_id={axis: lax.rem(me + d, size)}, device_id_type=MESH,
            )
            cp.start()
            cps.append(cp)
        return cps

    def reduce_finish(buf, size, cps):
        for cp in cps:
            cp.wait_recv()
        t = buf[0]
        for q in range(1, size):
            t = t + buf[q]
        return t

    ra = reduce_start(red_a, "col", ci, ncol, ra_s, ra_r)
    phase("gather12")
    gather(1)
    gather(2)
    phase("reduce_col")
    red_b[ri] = reduce_finish(red_a, ncol, ra)
    rb = reduce_start(red_b, "row", ri, nrow, rb_s, rb_r)
    phase("gather3")
    gather(3)
    arrived[0] = vals[0]
    ar = exchange(vals, arrived, ar_s, ar_r, 1)
    phase("sweep_pre")
    p0 = u + rdiag * (CG * coarse_beside(0, u, c0) - cdiag * u)
    phase("reduce_row")
    tot = reduce_finish(red_b, nrow, rb)

    phase("solve")
    def m(q):
        return jnp.broadcast_to(jnp.sum(jnp.where(lane == q, tot, 0.0), axis=1, keepdims=True), (1, 128))

    eta = [m(q) for q in (0, 1, 4, 5, 8, 9, 10)]
    nu = [m(q) for q in (2, 3, 6, 7)]
    hm = [[eta[i + j] for j in range(4)] for i in range(4)]
    low = [[None] * 4 for _ in range(4)]
    piv = []
    for j in range(4):
        pj = hm[j][j]
        for q in range(j):
            pj = pj - low[j][q] * low[j][q] * piv[q]
        ok = pj > 1e-6 * hm[j][j]
        piv.append(pj)
        inv = jnp.where(ok, 1.0 / jnp.where(ok, pj, 1.0), 0.0)
        low[j][j] = inv
        for i in range(j + 1, 4):
            e = hm[i][j]
            for q in range(j):
                e = e - low[i][q] * low[j][q] * piv[q]
            low[i][j] = e * inv
    y = list(nu)
    for i in range(4):
        for q in range(i):
            y[i] = y[i] - low[i][q] * y[q]
    y = [y[i] * low[i][i] for i in range(4)]
    for i in (2, 1, 0):
        for q in range(i + 1, 4):
            y[i] = y[i] - low[q][i] * y[q]
    phase("combine")

    def combine(i, _):
        r = pl.multiple_of(i * 16, 16)
        for j in range(NB):
            rows = pl.ds(OWN + r, 16)
            a = y[0] * f0[j, rows]
            for k in range(1, 4):
                a = a + y[k] * field[k][j, rows]
            at = slice(j * 128, (j + 1) * 128)
            for x, buf in zip(parts(a, 3), (pa0, pb0, pa1)):
                buf[pl.ds(r, 16), at] = x
        return _

    lax.fori_loop(0, TILE // 16, combine, 0, unroll=4)
    for h in range(2):
        hs = slice(h * 256, (h + 1) * 256)
        fine_o[:, hs] = sum(dot(buf[...], perm[hs, :], NT) for buf in (pa0, pb0, pa1))

    phase("wait_vals")
    for p in range(ncol):
        if p:
            ar[p - 1].wait_recv()
        at = slice(p * 128, (p + 1) * 128)
        a = y[0] * arrived[p, 0:1]
        for k in range(1, 4):
            a = a + y[k] * arrived[p, k:k + 1]
        hot = crow[:, at]
        for n, x in enumerate(parts(a, 2)):
            cva[n * 128:(n + 1) * 128, at] = hot * x
    phase("sources")
    t = dot(cva[0:256, :], ccol[...], NT)
    src = t[:128] + t[128:]
    u1 = p0 + rdiag * src
    phase("edges1")
    c1 = coarse_start(1, u1)
    phase("sweep2")
    coarse_o[...] = u1 + rdiag * (src + CG * coarse_beside(1, u1, c1) - cdiag * u1)

    phase("drain")
    for cp in rq + rs + ar + ra + rb:
        cp.wait_send()
    halo_sent(dcp)
    halo_sent(fcp)
    coarse_sent(c0)
    coarse_sent(c1)
    phase("")


def solution(mesh):
    nrow, ncol = mesh.shape["row"], mesh.shape["col"]
    slots = ncol * 128
    dma = pltpu.SemaphoreType.DMA

    def step(*args):
        vm = pl.BlockSpec(memory_space=pltpu.VMEM)
        anyspace = pl.BlockSpec(memory_space=pl.ANY)
        hbm = pl.BlockSpec(memory_space=pltpu.HBM)
        slab = (NB, TILE, 128)
        row = (ncol, 1, 128)
        return pl.pallas_call(
            functools.partial(kernel, nrow, ncol),
            out_shape=(
                pltpu.VMEM((TILE, TILE), F32),
                pltpu.VMEM((COARSE, COARSE), F32),
            ),
            in_specs=[hbm] * 8,
            out_specs=(vm, vm),
            scratch_shapes=[
                pltpu.VMEM((TILE, TILE), F32), pltpu.VMEM((TILE, TILE), I32), pltpu.VMEM((TILE, TILE), F32),
                pltpu.VMEM((TILE, TILE), BF16),
                pltpu.VMEM((TILE, slots), BF16), pltpu.VMEM((TILE, slots), BF16),
                pltpu.VMEM((TILE, slots), BF16), pltpu.VMEM((TILE, slots), BF16),
                *[pltpu.VMEM((NB + 1, ROWS, 128), F32)] * 4, pltpu.VMEM((4, ROWS, 128), F32), pltpu.VMEM((NB + 1, ROWS, 128), F32),
                pltpu.VMEM(slab, F32), pltpu.VMEM(slab, F32),
                *[pltpu.VMEM((TILE, TILE), BF16)] * 8,
                pltpu.VMEM(row, I32), pltpu.VMEM(row, I32), pltpu.VMEM(row, F32), pltpu.VMEM(row, F32),
                pltpu.VMEM((ncol, 4, 128), F32), pltpu.VMEM((ncol, 4, 128), F32),
                pltpu.VMEM((128, slots), BF16), pltpu.VMEM((128, slots), BF16),
                pltpu.VMEM((2, NB, 8, 128), F32), pltpu.VMEM((2, NB, 8, 128), F32),
                pltpu.VMEM((2, 8, TILE), F32), pltpu.VMEM((2, 8, TILE), F32),
                pltpu.VMEM((2, 4, 8, 128), F32), pltpu.VMEM((2, 2, 8, TILE), F32), pltpu.VMEM((2, 2, 8, 128), F32),
                pltpu.VMEM((16, 128), F32), pltpu.VMEM((ncol, 1, 128), F32), pltpu.VMEM((nrow, 1, 128), F32),
                pltpu.VMEM((256, 128), BF16),
                pltpu.VMEM((2, 128, 128), F32), pltpu.VMEM((2, 2, 8, 128), F32),
                pltpu.VMEM((2, 2, 8, 128), F32), pltpu.VMEM((2, 2, 8, 128), F32),
                pltpu.VMEM((COARSE, COARSE), F32), pltpu.VMEM((COARSE, COARSE), F32),
                pltpu.VMEM((1, slots), I32), pltpu.VMEM((1, slots), I32), pltpu.SMEM((1, ncol), I32),
                dma((3,)), dma((5,)),
                dma((ncol,)), dma((ncol,)), dma((ncol,)), dma((ncol,)), dma((ncol,)), dma((ncol,)),
                dma((2, 8)), dma((2, 8)), dma((ncol,)), dma((ncol,)), dma((nrow,)), dma((nrow,)),
                dma((2, 4)), dma((2, 4)),
            ],
            compiler_params=pltpu.CompilerParams(
                collective_id=0, has_side_effects=True, vmem_limit_bytes=50 << 20),
        )(*[pltpu.with_memory_space_constraint(x, pltpu.HBM) for x in args])

    spec = P("row", "col")
    return jax.shard_map(
        step, mesh=mesh, in_specs=(spec,) * 8, out_specs=(spec, spec), check_vma=False
    )
```

```python
import functools

import jax
import jax.numpy as jnp
from jax import lax
from jax.experimental import pallas as pl
from jax.experimental.pallas import tpu as pltpu
from jax.sharding import PartitionSpec as P

MESH = pl.DeviceIdType.MESH
F32, BF16, I32 = jnp.float32, jnp.bfloat16, jnp.int32
GROUP = 16
NB = 4
OWN = 16
TILE = 512
ROWS = TILE + 2 * OWN
COARSE = 128
FUSED = ()
VIA = 2.0
CG = 4.0
RELAX = 0.8
NN = (((1,), (0,)), ((), ()))
NT = (((1,), (1,)), ((), ()))


def place(c):
    return (c & 3) * 128 + (c >> 2)


def iota(shape, dim):
    return lax.broadcasted_iota(I32, shape, dim)


def dot(a, b, dims):
    return lax.dot_general(a, b, dims, preferred_element_type=F32)


def parts(x, n):
    out = []
    for _ in range(n):
        p = x.astype(BF16)
        out.append(p)
        x = x - p.astype(F32)
    return out


class Phases:
    def __init__(self):
        self.open = None

    def __call__(self, name):
        if self.open is not None:
            self.open.__exit__(None, None, None)
        self.open = None
        if name:
            self.open = jax.named_scope(name)
            self.open.__enter__()


def peer_order(n):
    if n != 16:
        return list(range(n))
    return sorted(range(n), key=lambda d: min(d // 4, 4 - d // 4) + min(d % 4, 4 - d % 4))


def kernel(
    nrow, ncol,
    amp_h, mask_h, leak_h, cleak_h, cinit_h, vfine_h, vcoarse_h, vcount_h,
    fine_h, coarse_h,
    amp, mask, leak, perm, rt, ct, cva, cvb, f0, f1, f2, f3, turned, dinv, diag, inj, pa0, pa1, pa2, pa3, pb0, pb1, pb2, pb3,
    req, held, held_side, held_row, look, atvia, vals, arrived, arrived_row, side_hot,
    crow, ccol, htop, hbot, hleft, hright, hcorner, csend, corner,
    mom, red_a, red_b, split, ubuf, seam, crecv, srecv, fine_o, coarse_o,
    cleak, cinit, vfine, vcoarse, vcount,
    in_sem, small_sem, out_sem, rq_s, rq_r, rs_s, rs_r, ar_s, ar_r,
    go, qs_s, qs_r, qr_s, qr_r, vr_s, vr_r, ha_s, ha_r, sum_sem, ce_s, ce_r,
):
    field, pa, pb = (f0, f1, f2, f3), (pa0, pa1, pa2, pa3), (pb0, pb1, pb2, pb3)
    slots = ncol * 128
    phase = Phases()
    phase("start")
    ri, ci = lax.axis_index("row"), lax.axis_index("col")

    small = []
    for n, (src, dst) in enumerate((
        (vcount_h, vcount), (vcoarse_h, vcoarse), (vfine_h, vfine), (cinit_h, cinit), (cleak_h, cleak)
    )):
        cp = pltpu.make_async_copy(src, dst, small_sem.at[n])
        cp.start()
        small.append(cp)
    loads = []
    for n, (src, dst) in enumerate(((leak_h, leak), (amp_h, amp), (mask_h, mask))):
        cp = pltpu.make_async_copy(src, dst, in_sem.at[n])
        cp.start()
        loads.append(cp)

    for buf in (htop, hbot, hleft, hright, hcorner, crecv, csend):
        buf[...] = jnp.zeros(buf.shape, F32)
    arrived_row[...] = jnp.zeros(arrived_row.shape, F32)
    held_row[...] = jnp.full(held_row.shape, -1, I32)

    phase("barrier")
    order = peer_order(ncol)

    def peer(p, sign):
        if ncol != 16:
            return lax.rem(ci + (order[p] if sign > 0 else ncol - order[p]), ncol)
        dy, dx = order[p] // 4, order[p] % 4
        y, x = ci // 4, lax.rem(ci, 4)
        if sign < 0:
            dy, dx = 4 - dy, 4 - dx
        return lax.rem(y + dy, 4) * 4 + lax.rem(x + dx, 4)

    bar = pltpu.get_barrier_semaphore()
    for d in range(1, ncol):
        pl.semaphore_signal(bar, inc=1, device_id={"col": lax.rem(ci + d, ncol)}, device_id_type=MESH)
    for d in range(1, nrow):
        pl.semaphore_signal(bar, inc=1, device_id={"row": lax.rem(ri + d, nrow)}, device_id_type=MESH)
    for dr in (1, nrow - 1):
        for dc in (1, ncol - 1):
            pl.semaphore_signal(
                bar, inc=1,
                device_id={"row": lax.rem(ri + dr, nrow), "col": lax.rem(ci + dc, ncol)},
                device_id_type=MESH,
            )
    phase("wait_small")
    for cp in small:
        cp.wait()
    lane = iota((1, 128), 1)

    def wait_bytes(ref, sem):
        pltpu.make_async_copy(ref, ref, sem).wait()

    half = ncol // 2

    class Exchange:
        def __init__(self, src, dst, ssem, rsem, sign):
            self.dst, self.ssem, self.rsem = dst, ssem, rsem
            for p in reversed(range(1, ncol)):
                pltpu.make_async_remote_copy(
                    src_ref=src(p), dst_ref=dst.at[p], send_sem=ssem, recv_sem=rsem.at[p // half],
                    device_id={"col": peer(p, sign)}, device_id_type=MESH,
                ).start()

        def arrived(self, p):
            if p == 1:
                wait_bytes(self.dst.at[pl.ds(1, half - 1)], self.rsem.at[0])
            if p == half:
                wait_bytes(self.dst.at[pl.ds(half, half)], self.rsem.at[1])

        def sent(self):
            wait_bytes(self.dst.at[pl.ds(1, ncol - 1)], self.ssem)

    class RowExchange:
        def __init__(self, src, dst, ssem, rsem):
            self.dst, self.ssem, self.rsem = dst, ssem, rsem
            self.sides = ((0, 1, ri < nrow - 1, ri > 0), (1, nrow - 1, ri > 0, ri < nrow - 1))
            for side, dr, to, _ in self.sides:

                @pl.when(to)
                def _():
                    for p in reversed(range(ncol)):
                        pltpu.make_async_remote_copy(
                            src_ref=src.at[1 + peer(p, 1)], dst_ref=dst.at[side, p],
                            send_sem=ssem.at[side], recv_sem=rsem.at[side],
                            device_id={"row": lax.rem(ri + dr, nrow), "col": peer(p, 1)}, device_id_type=MESH,
                        ).start()

        def arrived(self):
            for side, _, _, frm in self.sides:
                pl.when(frm)(lambda: wait_bytes(self.dst.at[side], self.rsem.at[side]))

        def sent(self):
            for side, _, to, _ in self.sides:
                pl.when(to)(lambda: wait_bytes(self.dst.at[side], self.ssem.at[side]))

    phase("requests")
    for p in reversed(range(ncol)):
        o = peer(p, 1)
        idx = vcoarse[:, pl.ds(pl.multiple_of(o * 128, 128), 128)]
        node = lax.shift_right_logical(idx, lax.full_like(idx, (slots).bit_length() - 1)) * 128 + (idx & 127)
        node = jnp.where(lane < vcount[0, o], node, -1)
        req[1 + o] = node
        if p == 0:
            held[0] = node
    req[0] = req[ncol]
    req[ncol + 1] = req[1]
    for q in range(3):
        held_side[0, q] = req[ci + q]
    phase("barrier_wait")
    pl.semaphore_wait(bar, ncol + nrow + 2)

    @pl.when(ri < nrow - 1)
    def _():
        pl.semaphore_signal(go.at[0], inc=1, device_id={"row": lax.rem(ri + 1, nrow)}, device_id_type=MESH)

    @pl.when(ri > 0)
    def _():
        pl.semaphore_signal(go.at[1], inc=1, device_id={"row": lax.rem(ri + nrow - 1, nrow)}, device_id_type=MESH)


    phase("send_req")
    rq = Exchange(lambda p: req.at[1 + peer(p, 1)], held, rq_s, rq_r, 1)

    phase("fine_onehot")
    for p in range(ncol):
        o = peer(p, 1)
        idx = vfine[:, pl.ds(pl.multiple_of(o * 128, 128), 128)]
        at = slice(p * 128, (p + 1) * 128)
        r = jnp.where(lane < vcount[0, o], idx >> 9, -1)
        c = place(idx & 511)
        for q in range(4):
            i = iota((128, 128), 0) + q * 128
            rt[q * 128:(q + 1) * 128, at] = jnp.where(i == r, 1.0, 0.0).astype(BF16)
            ct[q * 128:(q + 1) * 128, at] = jnp.where(i == c, 1.0, 0.0).astype(BF16)
    perm[...] = jnp.where(place(iota((TILE, TILE), 0)) == iota((TILE, TILE), 1), 1.0, 0.0).astype(BF16)
    phase("count_dot")
    loads[0].wait()
    pa2[...], pb2[...] = parts(leak[...], 2)
    for h in range(2):
        hs = slice(h * 256, (h + 1) * 256)
        t = VIA * dot(rt[...], ct[hs, :], NT)
        t = t + (dot(pa2[...], perm[:, hs], NN) + dot(pb2[...], perm[:, hs], NN))
        for q in range(2):
            j = 2 * h + q
            dg = 4.0 + t[:, q * 128:(q + 1) * 128]
            diag[j] = dg
            dinv[j, OWN:OWN + TILE] = 1.0 / dg

    row8 = iota((8, 128), 1)

    def halo_copies(f, src):
        up, dn = lax.rem(ri + nrow - 1, nrow), lax.rem(ri + 1, nrow)
        lf, rg = lax.rem(ci + ncol - 1, ncol), lax.rem(ci + 1, ncol)
        hu, hd, hl, hr = ri > 0, ri < nrow - 1, ci > 0, ci < ncol - 1
        first, last = pl.ds(OWN, 8), pl.ds(OWN + TILE - 8, 8)
        own = pl.ds(0, NB)
        plan = (
            (hu, hd, src.at[own, first], hbot.at[f], {"row": up}),
            (hd, hu, src.at[own, last], htop.at[f], {"row": dn}),
            (hl, hr, csend.at[f, 0], hright.at[f], {"col": lf}),
            (hr, hl, csend.at[f, 1], hleft.at[f], {"col": rg}),
            (hu & hl, hd & hr, corner.at[f, 0], hcorner.at[f, 0], {"row": up, "col": lf}),
            (hu & hr, hd & hl, corner.at[f, 0], hcorner.at[f, 1], {"row": up, "col": rg}),
            (hd & hl, hu & hr, corner.at[f, 1], hcorner.at[f, 2], {"row": dn, "col": lf}),
            (hd & hr, hu & hl, corner.at[f, 1], hcorner.at[f, 3], {"row": dn, "col": rg}),
        )
        out = []
        for n, (to, frm, s, d, dev) in enumerate(plan):
            cp = pltpu.make_async_remote_copy(
                src_ref=s, dst_ref=d, send_sem=ha_s.at[f, n], recv_sem=ha_r.at[f, n],
                device_id=dev, device_id_type=MESH,
            )
            out.append((to, frm, cp))
        return out

    def halo_start(f, src):
        own = slice(OWN, OWN + TILE)
        for j in range(NB):
            t = jnp.transpose(src[j, own])
            csend[f, 0, j:j + 1] = t[0:1]
            csend[f, 1, 4 + j:5 + j] = t[127:128]
        for e, r in enumerate((OWN, OWN + TILE - 8)):
            x = jnp.zeros((8, 128), F32)
            for j in range(NB):
                b = src[j, r:r + 8]
                x = jnp.where(row8 == j, pltpu.roll(b, j, 1) if j else b, x)
                x = jnp.where(row8 == 124 + j, pltpu.roll(b, 125 + j, 1) if j < 3 else b, x)
            corner[f, e] = x
        cps = halo_copies(f, src)
        for to, _, cp in cps:
            pl.when(to)(cp.start)
        return cps

    def halo_finish(f, dst, cps):
        for _, frm, cp in cps:
            pl.when(frm)(cp.wait_recv)
        dst[0:NB, OWN - 8:OWN] = htop[f]
        dst[0:NB, OWN + TILE:OWN + TILE + 8] = hbot[f]
        x = jnp.concatenate([hright[f], jnp.zeros((112, TILE), F32), hleft[f]], axis=0)
        dst[NB, OWN:OWN + TILE] = jnp.transpose(x)
        near = row8 < 64
        dst[NB, OWN + TILE:OWN + TILE + 8] = jnp.where(near, hcorner[f, 0], hcorner[f, 1])
        dst[NB, OWN - 8:OWN] = jnp.where(near, hcorner[f, 2], hcorner[f, 3])

    def halo_sent(cps):
        for to, _, cp in cps:
            pl.when(to)(cp.wait_send)

    phase("dinv_halo")
    for buf in (dinv, f0, f1, f2, f3):
        buf[:, 0:8] = jnp.zeros((NB + 1, 8, 128), F32)
        buf[:, ROWS - 8:ROWS] = jnp.zeros((NB + 1, 8, 128), F32)
    dcp = halo_start(0, dinv)
    phase("send_side")
    pl.when(ri > 0)(lambda: pl.semaphore_wait(go.at[0], 1))
    pl.when(ri < nrow - 1)(lambda: pl.semaphore_wait(go.at[1], 1))
    qs = Exchange(lambda p: req.at[pl.ds(peer(p, 1), 3)], held_side, qs_s, qs_r, 1)
    qr = RowExchange(req, held_row, qr_s, qr_r)

    phase("wait_req")
    u = cinit[...]
    split[0:256] = jnp.concatenate(parts(u, 2), axis=0)
    ci128 = iota((128, 128), 0)
    for p in range(ncol):
        rq.arrived(p)
        at = slice(p * 128, (p + 1) * 128)
        idx = held[p]
        crow[:, at] = jnp.where(ci128 == (idx >> 7), 1.0, 0.0).astype(BF16)
        ccol[:, at] = jnp.where(ci128 == (idx & 127), 1.0, 0.0).astype(BF16)
    phase("lookup")
    for n in range(ncol // 2):
        at = slice(n * 256, (n + 1) * 256)
        t = dot(split[0:256], ccol[:, at], NN)
        t = jnp.sum((t[:128] + t[128:]) * crow[:, at].astype(F32), axis=0, keepdims=True)
        for p in (2 * n, 2 * n + 1):
            (look if p else atvia)[p] = t[:, (p - 2 * n) * 128:(p - 2 * n + 1) * 128]
    rs = Exchange(lambda p: look.at[p], atvia, rs_s, rs_r, -1)

    phase("coarse_diag")
    cdiag = 4.0 * CG + cleak[...] + VIA * dot(crow[...], ccol[...], NT)
    rdiag = RELAX / cdiag

    def coarse_start(s, u):
        ubuf[s] = u
        seam_t = jnp.transpose(u)
        for e, j in enumerate((0, GROUP - 1)):
            seam[s, e] = jnp.concatenate(
                [seam_t[g * GROUP + j:g * GROUP + j + 1] for g in range(128 // GROUP)], axis=0
            )
        up, dn = lax.rem(ri + nrow - 1, nrow), lax.rem(ri + 1, nrow)
        lf, rg = lax.rem(ci + ncol - 1, ncol), lax.rem(ci + 1, ncol)
        true = ri >= 0
        plan = (
            (ri > 0, ri < nrow - 1, ubuf.at[s, pl.ds(0, 8)], crecv.at[s, 1], {"row": up}),
            (ri < nrow - 1, ri > 0, ubuf.at[s, pl.ds(120, 8)], crecv.at[s, 0], {"row": dn}),
            (None, None, seam.at[s, 0], srecv.at[s, 1], {"col": lf}),
            (None, None, seam.at[s, 1], srecv.at[s, 0], {"col": rg}),
        )
        cps = []
        for n, (to, frm, sr, ds, dev) in enumerate(plan):
            cp = pltpu.make_async_remote_copy(
                src_ref=sr, dst_ref=ds, send_sem=ce_s.at[s, n], recv_sem=ce_r.at[s, n],
                device_id=dev, device_id_type=MESH,
            )
            if to is None:
                cp.start()
            else:
                pl.when(to)(cp.start)
            cps.append((to, frm, cp))
        return cps

    def coarse_wait(cps):
        for _, frm, cp in cps:
            if frm is None:
                cp.wait_recv()
            else:
                pl.when(frm)(cp.wait_recv)

    def coarse_beside(u, up, dn, fl, fr):
        li, si = iota((128, 128), 1), ci128
        up = jnp.where(si == 0, up, pltpu.roll(u, 1, 0))
        dn = jnp.where(si == 127, dn, pltpu.roll(u, 127, 0))
        g = iota((8, 128), 0)
        fl = jnp.where(ci == 0, jnp.where(g == 0, 0.0, pltpu.roll(fl, 1, 0)), fl)
        fr = jnp.where(ci == ncol - 1, jnp.where(g == 7, 0.0, pltpu.roll(fr, 7, 0)), fr)

        def spread(x):
            return jnp.concatenate([jnp.broadcast_to(x[q:q + 1], (GROUP, 128)) for q in range(8)], axis=0)

        x = jnp.transpose(jnp.where(si % GROUP == 0, spread(fl), spread(fr)))
        left = jnp.where(li % GROUP == 0, x, pltpu.roll(u, 1, 1))
        right = jnp.where(li % GROUP == GROUP - 1, x, pltpu.roll(u, 127, 1))
        return up + dn + left + right

    def coarse_sent(cps):
        for to, _, cp in cps:
            if to is None:
                cp.wait_send()
            else:
                pl.when(to)(cp.wait_send)

    phase("coarse_start")
    c0 = coarse_start(0, u)
    phase("load")
    for cp in loads[1:]:
        cp.wait()
    pa1[...], pb1[...] = parts(amp[...] * mask[...].astype(F32), 2)
    for h in range(2):
        hs = slice(h * 256, (h + 1) * 256)
        t = dot(pa1[...], perm[:, hs], NN) + dot(pb1[...], perm[:, hs], NN)
        for q in range(2):
            inj[2 * h + q] = t[:, q * 128:(q + 1) * 128]
    phase("dinv_finish")
    halo_finish(0, dinv, dcp)

    def make_inj(o):
        at = pl.ds(pl.multiple_of(o * 128, 128), 128)
        p = parts(atvia[o], 2)
        col = ct[:, at]
        cva[:, at] = col * p[0]
        cvb[:, at] = col * p[1]

    v0 = f0
    for part in range(2):
        phase(f"wait_resp{part}")
        for p in range(part * half, (part + 1) * half):
            rs.arrived(p)
            at = slice(p * 128, (p + 1) * 128)
            c = vfine[:, pl.ds(pl.multiple_of(peer(p, 1) * 128, 128), 128)]
            c = place(c & 511)
            v = atvia[p]
            va = v.astype(BF16).astype(F32)
            vb = v - va
            for q in range(4):
                hot = iota((128, 128), 0) + q * 128 == c
                cva[q * 128:(q + 1) * 128, at] = jnp.where(hot, va, 0.0).astype(BF16)
                cvb[q * 128:(q + 1) * 128, at] = jnp.where(hot, vb, 0.0).astype(BF16)
        phase(f"inject_dot{part}")
        ks = slice(part * half * 128, (part + 1) * half * 128)
        for h in range(2):
            hs = slice(h * 256, (h + 1) * 256)
            t = dot(rt[:, ks], cva[hs, ks], NT) + dot(rt[:, ks], cvb[hs, ks], NT)
            for q in range(2):
                j = 2 * h + q
                tq = VIA * t[:, q * 128:(q + 1) * 128]
                if part == 0:
                    inj[j] = inj[j] + tq
                else:
                    z = (inj[j] + tq) * dinv[j, OWN:OWN + TILE]
                    v0[j, OWN:OWN + TILE] = z
                    za, zb = parts(z, 2)
                    pa0[:, j * 128:(j + 1) * 128] = za
                    pb0[:, j * 128:(j + 1) * 128] = zb
    phase("halo_start")
    fcp = halo_start(1, v0)

    def gather_part(k, n):
        at = slice(n * 256, n * 256 + 256) if isinstance(n, int) else pl.ds(pl.multiple_of(n * 256, 256), 256)
        t = dot(pa[k][...], ct[:, at], NN) + dot(pb[k][...], ct[:, at], NN)
        t = VIA * jnp.sum(t * rt[:, at].astype(F32), axis=0, keepdims=True)
        for p in (2 * n, 2 * n + 1):
            vals[1 + peer(p, 1), k:k + 1] = t[:, (p - 2 * n) * 128:(p - 2 * n + 1) * 128]

    def gather(k):
        for n in range(ncol // 2):
            gather_part(k, n)

    phase("gather0")
    gather(0)
    phase("sweep_pre")
    coarse_wait(c0)
    p0 = u + rdiag * (
        CG * coarse_beside(u, crecv[0, 0, 7:8], crecv[0, 1, 0:1], srecv[0, 0], srecv[0, 1]) - cdiag * u
    )
    c1 = coarse_start(1, p0)
    c2 = coarse_start(2, rdiag)
    phase("side_hot")
    for p in (1, half):
        qs.arrived(p)
    qr.arrived()
    for p in range(ncol):
        at = slice(p * 128, (p + 1) * 128)
        nodes = (held_side[p, 0] >> 7, held_side[p, 2] >> 7, held_row[0, p] & 127, held_row[1, p] & 127)
        for q, x in enumerate(nodes):
            side_hot[q, :, at] = jnp.where(ci128 == x, 1.0, 0.0).astype(BF16)
    phase("halo_finish")
    halo_finish(1, v0, fcp)

    phase("powers")
    def turn(v, r, h):
        rows = pl.ds(r, h)
        first, last, halo = v[0, rows], v[NB - 1, rows], v[NB, rows]
        turned[0, rows] = pltpu.roll(last, 1, 1)
        turned[1, rows] = pltpu.roll(halo, 1, 1)
        turned[2, rows] = pltpu.roll(first, 127, 1)
        turned[3, rows] = pltpu.roll(halo, 127, 1)

    def beside(v, r, h):
        lanes = iota((h, 128), 1)
        first_lane, last_lane = lanes == 0, lanes == 127
        rows = pl.ds(r, h)
        c = [v[j, rows] for j in range(NB + 1)]
        last_r, halo_r, first_l, halo_l = (turned[q, rows] for q in range(4))
        left = [jnp.where(first_lane, halo_r, last_r), *c[:NB - 1], jnp.where(first_lane, last_r, halo_r)]
        right = [*c[1:NB], jnp.where(last_lane, halo_l, first_l), jnp.where(last_lane, first_l, halo_l)]
        out = [
            v[j, pl.ds(r - 1, h)] + v[j, pl.ds(r + 1, h)] + left[j] + right[j] for j in range(NB + 1)
        ]
        return c, out

    def power(k):
        v, nxt = field[k], field[k + 1] if k < 3 else None
        count = (4, 4, 2, 1)[k]

        def rows(r, h, sums):
            c, nb = beside(v, r, h)
            sums = list(sums) if sums is not None else None

            def add(n, x):
                for q in range(h // 8):
                    sums[n] = sums[n] + x[q * 8:(q + 1) * 8]

            for j in range(NB + 1):
                w = None
                if nxt is not None:
                    w = dinv[j, pl.ds(r, h)] * nb[j]
                    nxt[j, pl.ds(r, h)] = w
                if sums is not None and j < NB:
                    if nxt is not None:
                        wa, wb = parts(w, 2)
                        pa[k + 1][pl.ds(r - OWN, h), j * 128:(j + 1) * 128] = wa
                        pb[k + 1][pl.ds(r - OWN, h), j * 128:(j + 1) * 128] = wb
                    dv = diag[j, pl.ds(r - OWN, h)] * c[j]
                    av = dv - nb[j]
                    add(0, c[j] * av)
                    if count > 1:
                        add(1, w * av)
                    if count > 2:
                        add(2, c[j] * dv)
                        add(3, c[j] * nb[j])
            return tuple(sums) if sums is not None else None

        steps = ncol // 2 if k in FUSED else 8
        each = TILE // steps
        turn(v, OWN, each)
        if nxt is not None:
            for r in (OWN - 8, OWN + TILE):
                turn(v, r, 8)
                rows(r, 8, None)

        def step(i, sums, last=False):
            r = OWN + i * each if last else pl.multiple_of(OWN + i * each, 16)
            if k in FUSED:
                gather_part(k, i)
            if not last:
                turn(v, r + each, each)
            for q in range(each // 16):
                sums = rows(r + q * 16, 16, sums)
            return sums

        z = jnp.zeros((8, 128), F32)
        sums = lax.fori_loop(0, steps - 1, step, (z,) * count)
        return step(steps - 1, sums, last=True)

    n = 0
    for k in range(4):
        phase(f"power{k}")
        for s in power(k):
            mom[n:n + 1] = jnp.sum(s, axis=0, keepdims=True)
            n += 1
    mom[11:16] = jnp.zeros((5, 128), F32)

    phase("lane_sum")
    t = jnp.sum(mom[...], axis=1, keepdims=True)
    red_a[ci] = jnp.sum(jnp.where(iota((16, 128), 0) == iota((16, 128), 1), t, 0.0), axis=0, keepdims=True)

    def reduce_start(buf, axis, me, size, sems):
        for d in range(1, size):
            pltpu.make_async_remote_copy(
                src_ref=buf.at[me], dst_ref=buf.at[me], send_sem=sems.at[0], recv_sem=sems.at[1],
                device_id={axis: lax.rem(me + d, size)}, device_id_type=MESH,
            ).start()

    def reduce_finish(buf, size, sems):
        wait_bytes(buf.at[pl.ds(0, size - 1)], sems.at[1])
        t = buf[0]
        for q in range(1, size):
            t = t + buf[q]
        return t

    reduce_start(red_a, "col", ci, ncol, sum_sem.at[0])
    phase("gather12")
    gather(1)
    gather(2)
    phase("reduce_col")
    red_b[ri] = reduce_finish(red_a, ncol, sum_sem.at[0])
    reduce_start(red_b, "row", ri, nrow, sum_sem.at[1])
    phase("gather3")
    gather(3)
    vals[0] = vals[ncol]
    vals[ncol + 1] = vals[1]
    ar = Exchange(lambda p: vals.at[pl.ds(peer(p, 1), 3)], arrived, ar_s, ar_r, 1)
    vr = RowExchange(vals, arrived_row, vr_s, vr_r)
    for q in range(3):
        arrived[0, q] = vals[ci + q]
    phase("reduce_row")
    tot = reduce_finish(red_b, nrow, sum_sem.at[1])

    phase("solve")
    def m(q):
        return jnp.broadcast_to(jnp.sum(jnp.where(lane == q, tot, 0.0), axis=1, keepdims=True), (1, 128))

    eta = [m(q) for q in (0, 1, 4, 5, 8, 9, 10)]
    nu = [m(q) for q in (2, 3, 6, 7)]
    hm = [[eta[i + j] for j in range(4)] for i in range(4)]
    low = [[None] * 4 for _ in range(4)]
    piv = []
    for j in range(4):
        pj = hm[j][j]
        for q in range(j):
            pj = pj - low[j][q] * low[j][q] * piv[q]
        ok = pj > 1e-6 * hm[j][j]
        piv.append(pj)
        inv = jnp.where(ok, 1.0 / jnp.where(ok, pj, 1.0), 0.0)
        low[j][j] = inv
        for i in range(j + 1, 4):
            e = hm[i][j]
            for q in range(j):
                e = e - low[i][q] * low[j][q] * piv[q]
            low[i][j] = e * inv
    y = list(nu)
    for i in range(4):
        for q in range(i):
            y[i] = y[i] - low[i][q] * y[q]
    y = [y[i] * low[i][i] for i in range(4)]
    for i in (2, 1, 0):
        for q in range(i + 1, 4):
            y[i] = y[i] - low[q][i] * y[q]
    phase("combine")

    def combine(i, _):
        r = pl.multiple_of(i * 16, 16)
        for j in range(NB):
            rows = pl.ds(OWN + r, 16)
            a = y[0] * f0[j, rows]
            for k in range(1, 4):
                a = a + y[k] * field[k][j, rows]
            at = slice(j * 128, (j + 1) * 128)
            for x, buf in zip(parts(a, 3), (pa0, pb0, pa1)):
                buf[pl.ds(r, 16), at] = x
        return _

    lax.fori_loop(0, TILE // 16, combine, 0, unroll=4)
    for h in range(2):
        hs = slice(h * 256, (h + 1) * 256)
        fine_o[:, hs] = sum(dot(buf[...], perm[hs, :], NT) for buf in (pa0, pb0, pa1))

    fine_out = pltpu.make_async_copy(fine_o, fine_h, out_sem.at[0])
    fine_out.start()
    phase("wait_vals")
    coarse_wait(c1)
    coarse_wait(c2)
    i8, i16 = iota((8, 128), 0), iota((16, 128), 0)
    coef = jnp.concatenate(y, axis=0)

    def current(x):
        a = jnp.sum(coef * x, axis=0, keepdims=True)
        hi = a.astype(BF16).astype(F32)
        return hi, a - hi

    for p in range(ncol):
        ar.arrived(p)
        at = slice(p * 128, (p + 1) * 128)
        hot = crow[:, at]
        for n, x in enumerate(current(arrived[p, 1])):
            cva[n * 128:(n + 1) * 128, at] = hot * x.astype(BF16)
        for q, edge in ((0, GROUP - 1), (1, 0)):
            on = i8 * GROUP + edge == (held_side[p, 2 * q] & 127)
            x = [jnp.where(on, x, 0.0) for x in current(arrived[p, 2 * q])]
            cvb[q * 16:(q + 1) * 16, at] = jnp.concatenate(x, axis=0).astype(BF16)
    phase("sources")
    t = dot(cva[0:256, :], ccol[...], NT)
    src = t[:128] + t[128:]
    side = [dot(cvb[q * 16:(q + 1) * 16, :], side_hot[q], NT) for q in range(2)]
    phase("wait_rows")
    vr.arrived()
    for p in range(ncol):
        at = slice(p * 128, (p + 1) * 128)
        for q, edge in ((0, 127), (1, 0)):
            hi, lo = current(arrived_row[q, p])
            on = (held_row[q, p] >> 7) == edge
            x = jnp.where(i16 == 0, jnp.where(on, hi, 0.0), jnp.where(i16 == 1, jnp.where(on, lo, 0.0), 0.0))
            cvb[32 + q * 16:48 + q * 16, at] = x.astype(BF16)
    side += [dot(cvb[q * 16:(q + 1) * 16, :], side_hot[q], NT) for q in (2, 3)]
    phase("sweeps")
    u1 = p0 + rdiag * src
    beside1 = coarse_beside(
        u1,
        crecv[1, 0, 7:8] + crecv[2, 0, 7:8] * (side[2][0:1] + side[2][1:2]),
        crecv[1, 1, 0:1] + crecv[2, 1, 0:1] * (side[3][0:1] + side[3][1:2]),
        srecv[1, 0] + srecv[2, 0] * (side[0][0:8] + side[0][8:16]),
        srecv[1, 1] + srecv[2, 1] * (side[1][0:8] + side[1][8:16]),
    )
    coarse_o[...] = u1 + rdiag * (src + CG * beside1 - cdiag * u1)
    coarse_out = pltpu.make_async_copy(coarse_o, coarse_h, out_sem.at[1])
    coarse_out.start()
    phase("drain")
    for x in (rq, qs, rs, ar, qr, vr):
        x.sent()
    wait_bytes(red_a.at[pl.ds(0, ncol - 1)], sum_sem.at[0, 0])
    wait_bytes(red_b.at[pl.ds(0, nrow - 1)], sum_sem.at[1, 0])
    coarse_sent(c2)
    halo_sent(dcp)
    halo_sent(fcp)
    coarse_sent(c0)
    coarse_sent(c1)
    fine_out.wait()
    coarse_out.wait()
    phase("")


def solution(mesh):
    nrow, ncol = mesh.shape["row"], mesh.shape["col"]
    slots = ncol * 128
    dma = pltpu.SemaphoreType.DMA

    def step(*args):
        anyspace = pl.BlockSpec(memory_space=pl.ANY)
        hbm = pl.BlockSpec(memory_space=pltpu.HBM)
        slab = (NB, TILE, 128)
        row = (ncol, 1, 128)
        return pl.pallas_call(
            functools.partial(kernel, nrow, ncol),
            out_shape=(
                pltpu.VMEM((TILE, TILE), F32),
                pltpu.VMEM((COARSE, COARSE), F32),
            ),
            in_specs=[hbm] * 8,
            out_specs=(anyspace, anyspace),
            scratch_shapes=[
                pltpu.VMEM((TILE, TILE), F32), pltpu.VMEM((TILE, TILE), I32), pltpu.VMEM((TILE, TILE), F32),
                pltpu.VMEM((TILE, TILE), BF16),
                pltpu.VMEM((TILE, slots), BF16), pltpu.VMEM((TILE, slots), BF16),
                pltpu.VMEM((TILE, slots), BF16), pltpu.VMEM((TILE, slots), BF16),
                *[pltpu.VMEM((NB + 1, ROWS, 128), F32)] * 4, pltpu.VMEM((4, ROWS, 128), F32), pltpu.VMEM((NB + 1, ROWS, 128), F32),
                pltpu.VMEM(slab, F32), pltpu.VMEM(slab, F32),
                *[pltpu.VMEM((TILE, TILE), BF16)] * 8,
                pltpu.VMEM((ncol + 2, 1, 128), I32), pltpu.VMEM(row, I32),
                pltpu.VMEM((ncol, 3, 1, 128), I32), pltpu.VMEM((2, ncol, 1, 128), I32),
                pltpu.VMEM(row, F32), pltpu.VMEM(row, F32),
                pltpu.VMEM((ncol + 2, 4, 128), F32), pltpu.VMEM((ncol, 3, 4, 128), F32),
                pltpu.VMEM((2, ncol, 4, 128), F32), pltpu.VMEM((4, 128, slots), BF16),
                pltpu.VMEM((128, slots), BF16), pltpu.VMEM((128, slots), BF16),
                pltpu.VMEM((2, NB, 8, 128), F32), pltpu.VMEM((2, NB, 8, 128), F32),
                pltpu.VMEM((2, 8, TILE), F32), pltpu.VMEM((2, 8, TILE), F32),
                pltpu.VMEM((2, 4, 8, 128), F32), pltpu.VMEM((2, 2, 8, TILE), F32), pltpu.VMEM((2, 2, 8, 128), F32),
                pltpu.VMEM((16, 128), F32), pltpu.VMEM((ncol, 1, 128), F32), pltpu.VMEM((nrow, 1, 128), F32),
                pltpu.VMEM((256, 128), BF16),
                pltpu.VMEM((3, 128, 128), F32), pltpu.VMEM((3, 2, 8, 128), F32),
                pltpu.VMEM((3, 2, 8, 128), F32), pltpu.VMEM((3, 2, 8, 128), F32),
                pltpu.VMEM((TILE, TILE), F32), pltpu.VMEM((COARSE, COARSE), F32),
                pltpu.VMEM((COARSE, COARSE), F32), pltpu.VMEM((COARSE, COARSE), F32),
                pltpu.VMEM((1, slots), I32), pltpu.VMEM((1, slots), I32), pltpu.SMEM((1, ncol), I32),
                dma((3,)), dma((5,)), dma((2,)),
                *[dma(()), dma((2,))] * 3,
                pltpu.SemaphoreType.REGULAR((2,)),
                dma(()), dma((2,)), *[dma((2,))] * 4,
                dma((2, 8)), dma((2, 8)), dma((2, 2)),
                dma((3, 4)), dma((3, 4)),
            ],
            compiler_params=pltpu.CompilerParams(
                collective_id=0, has_side_effects=True, vmem_limit_bytes=50 << 20),
        )(*[pltpu.with_memory_space_constraint(x, pltpu.HBM) for x in args])

    spec = P("row", "col")
    return jax.shard_map(
        step, mesh=mesh, in_specs=(spec,) * 8, out_specs=(spec, spec), check_vma=False
    )
```

```python
import functools

import jax
import jax.numpy as jnp
from jax import lax
from jax.experimental import pallas as pl
from jax.experimental.pallas import tpu as pltpu
from jax.sharding import PartitionSpec as P

MESH = pl.DeviceIdType.MESH
F8 = jnp.float8_e4m3fn
HOT = 64.0
LOW = HOT * HOT
F32, BF16, I32 = jnp.float32, jnp.bfloat16, jnp.int32
GROUP = 16
NB = 4
OWN = 16
TILE = 512
ROWS = TILE + 2 * OWN
COARSE = 128
FUSED = ()
VIA = 2.0
CG = 4.0
RELAX = 0.8
NN = (((1,), (0,)), ((), ()))
NT = (((1,), (1,)), ((), ()))


def place(c):
    return (c & 3) * 128 + (c >> 2)


def iota(shape, dim):
    return lax.broadcasted_iota(I32, shape, dim)


def dot(a, b, dims):
    return lax.dot_general(a, b, dims, preferred_element_type=F32)


def parts(x, n):
    out = []
    for _ in range(n):
        p = x.astype(BF16)
        out.append(p)
        x = x - p.astype(F32)
    return out


class Phases:
    def __init__(self):
        self.open = None

    def __call__(self, name):
        if self.open is not None:
            self.open.__exit__(None, None, None)
        self.open = None
        if name:
            self.open = jax.named_scope(name)
            self.open.__enter__()


def peer_order(n):
    if n != 16:
        return list(range(n))
    return sorted(range(n), key=lambda d: min(d // 4, 4 - d // 4) + min(d % 4, 4 - d % 4))


def high_low(x):
    p = x.astype(BF16)
    return p, ((x - p.astype(F32)) * LOW).astype(F8)


def kernel(
    nrow, ncol,
    amp_h, mask_h, leak_h, cleak_h, cinit_h, vfine_h, vcoarse_h, vcount_h,
    fine_h, coarse_h,
    amp, mask, leak, perm, rt, ct, cva, cvb, f0, f1, f2, f3, turned, dinv, diag, inj, pa0, pa1, pa2, pa3, pb0, pb1, pb2, pb80, pb81, pb82, pb83, ct8, rt8, cvb8,
    req, held, held_side, held_row, look, atvia, vals, arrived, arrived_row, side_hot,
    crow, ccol, htop, hbot, hleft, hright, hcorner, csend, corner,
    mom, red_a, red_b, split, ubuf, seam, crecv, srecv, fine_o, coarse_o,
    cleak, cinit, vfine, vcoarse, vcount,
    in_sem, small_sem, out_sem, rq_s, rq_r, rs_s, rs_r, ar_s, ar_r,
    go, qs_s, qs_r, qr_s, qr_r, vr_s, vr_r, ha_s, ha_r, sum_sem, ce_s, ce_r,
):
    field, pa, pb8 = (f0, f1, f2, f3), (pa0, pa1, pa2, pa3), (pb80, pb81, pb82, pb83)
    slots = ncol * 128
    phase = Phases()
    phase("start")
    ri, ci = lax.axis_index("row"), lax.axis_index("col")

    small = []
    for n, (src, dst) in enumerate((
        (vcount_h, vcount), (vcoarse_h, vcoarse), (vfine_h, vfine), (cinit_h, cinit), (cleak_h, cleak)
    )):
        cp = pltpu.make_async_copy(src, dst, small_sem.at[n])
        cp.start()
        small.append(cp)
    loads = []
    for n, (src, dst) in enumerate(((leak_h, leak), (amp_h, amp), (mask_h, mask))):
        cp = pltpu.make_async_copy(src, dst, in_sem.at[n])
        cp.start()
        loads.append(cp)

    for buf in (htop, hbot, hleft, hright, hcorner, crecv, csend):
        buf[...] = jnp.zeros(buf.shape, F32)
    arrived_row[...] = jnp.zeros(arrived_row.shape, F32)
    held_row[...] = jnp.full(held_row.shape, -1, I32)

    phase("barrier")
    order = peer_order(ncol)

    def peer(p, sign):
        if ncol != 16:
            return lax.rem(ci + (order[p] if sign > 0 else ncol - order[p]), ncol)
        dy, dx = order[p] // 4, order[p] % 4
        y, x = ci // 4, lax.rem(ci, 4)
        if sign < 0:
            dy, dx = 4 - dy, 4 - dx
        return lax.rem(y + dy, 4) * 4 + lax.rem(x + dx, 4)

    bar = pltpu.get_barrier_semaphore()
    for d in range(1, ncol):
        pl.semaphore_signal(bar, inc=1, device_id={"col": lax.rem(ci + d, ncol)}, device_id_type=MESH)
    for d in range(1, nrow):
        pl.semaphore_signal(bar, inc=1, device_id={"row": lax.rem(ri + d, nrow)}, device_id_type=MESH)
    for dr in (1, nrow - 1):
        for dc in (1, ncol - 1):
            pl.semaphore_signal(
                bar, inc=1,
                device_id={"row": lax.rem(ri + dr, nrow), "col": lax.rem(ci + dc, ncol)},
                device_id_type=MESH,
            )
    phase("wait_small")
    for cp in small:
        cp.wait()
    lane = iota((1, 128), 1)

    def wait_bytes(ref, sem):
        pltpu.make_async_copy(ref, ref, sem).wait()

    half = ncol // 2

    class Exchange:
        def __init__(self, src, dst, ssem, rsem, sign):
            self.dst, self.ssem, self.rsem = dst, ssem, rsem
            for p in reversed(range(1, ncol)):
                pltpu.make_async_remote_copy(
                    src_ref=src(p), dst_ref=dst.at[p], send_sem=ssem, recv_sem=rsem.at[p // half],
                    device_id={"col": peer(p, sign)}, device_id_type=MESH,
                ).start()

        def arrived(self, p):
            if p == 1:
                wait_bytes(self.dst.at[pl.ds(1, half - 1)], self.rsem.at[0])
            if p == half:
                wait_bytes(self.dst.at[pl.ds(half, half)], self.rsem.at[1])

        def sent(self):
            wait_bytes(self.dst.at[pl.ds(1, ncol - 1)], self.ssem)

    class RowExchange:
        def __init__(self, src, dst, ssem, rsem):
            self.dst, self.ssem, self.rsem = dst, ssem, rsem
            self.sides = ((0, 1, ri < nrow - 1, ri > 0), (1, nrow - 1, ri > 0, ri < nrow - 1))
            for side, dr, to, _ in self.sides:

                @pl.when(to)
                def _():
                    for p in reversed(range(ncol)):
                        pltpu.make_async_remote_copy(
                            src_ref=src.at[1 + peer(p, 1)], dst_ref=dst.at[side, p],
                            send_sem=ssem.at[side], recv_sem=rsem.at[side],
                            device_id={"row": lax.rem(ri + dr, nrow), "col": peer(p, 1)}, device_id_type=MESH,
                        ).start()

        def arrived(self):
            for side, _, _, frm in self.sides:
                pl.when(frm)(lambda: wait_bytes(self.dst.at[side], self.rsem.at[side]))

        def sent(self):
            for side, _, to, _ in self.sides:
                pl.when(to)(lambda: wait_bytes(self.dst.at[side], self.ssem.at[side]))

    phase("requests")
    for p in reversed(range(ncol)):
        o = peer(p, 1)
        idx = vcoarse[:, pl.ds(pl.multiple_of(o * 128, 128), 128)]
        node = lax.shift_right_logical(idx, lax.full_like(idx, (slots).bit_length() - 1)) * 128 + (idx & 127)
        node = jnp.where(lane < vcount[0, o], node, -1)
        req[1 + o] = node
        if p == 0:
            held[0] = node
    req[0] = req[ncol]
    req[ncol + 1] = req[1]
    for q in range(3):
        held_side[0, q] = req[ci + q]
    phase("barrier_wait")
    pl.semaphore_wait(bar, ncol + nrow + 2)

    @pl.when(ri < nrow - 1)
    def _():
        pl.semaphore_signal(go.at[0], inc=1, device_id={"row": lax.rem(ri + 1, nrow)}, device_id_type=MESH)

    @pl.when(ri > 0)
    def _():
        pl.semaphore_signal(go.at[1], inc=1, device_id={"row": lax.rem(ri + nrow - 1, nrow)}, device_id_type=MESH)


    phase("send_req")
    rq = Exchange(lambda p: req.at[1 + peer(p, 1)], held, rq_s, rq_r, 1)

    phase("fine_onehot")
    for p in range(ncol):
        o = peer(p, 1)
        idx = vfine[:, pl.ds(pl.multiple_of(o * 128, 128), 128)]
        at = slice(p * 128, (p + 1) * 128)
        r = jnp.where(lane < vcount[0, o], idx >> 9, -1)
        c = place(idx & 511)
        for q in range(4):
            i = iota((128, 128), 0) + q * 128
            rt[q * 128:(q + 1) * 128, at] = jnp.where(i == r, 1.0, 0.0).astype(BF16)
            rt8[q * 128:(q + 1) * 128, at] = jnp.where(i == r, 1.0, 0.0).astype(F8)
            ct[q * 128:(q + 1) * 128, at] = jnp.where(i == c, HOT, 0.0).astype(BF16)
            ct8[q * 128:(q + 1) * 128, at] = jnp.where(i == c, 1.0 / HOT, 0.0).astype(F8)
    perm[...] = jnp.where(place(iota((TILE, TILE), 0)) == iota((TILE, TILE), 1), 1.0, 0.0).astype(BF16)
    phase("count_dot")
    loads[0].wait()
    pa2[...], pb2[...] = parts(leak[...], 2)
    for h in range(2):
        hs = slice(h * 256, (h + 1) * 256)
        t = (VIA * HOT) * dot(rt8[...], ct8[hs, :], NT)
        t = t + (dot(pa2[...], perm[:, hs], NN) + dot(pb2[...], perm[:, hs], NN))
        for q in range(2):
            j = 2 * h + q
            dg = 4.0 + t[:, q * 128:(q + 1) * 128]
            diag[j] = dg
            dinv[j, OWN:OWN + TILE] = 1.0 / dg

    row8 = iota((8, 128), 1)

    def halo_copies(f, src):
        up, dn = lax.rem(ri + nrow - 1, nrow), lax.rem(ri + 1, nrow)
        lf, rg = lax.rem(ci + ncol - 1, ncol), lax.rem(ci + 1, ncol)
        hu, hd, hl, hr = ri > 0, ri < nrow - 1, ci > 0, ci < ncol - 1
        first, last = pl.ds(OWN, 8), pl.ds(OWN + TILE - 8, 8)
        own = pl.ds(0, NB)
        plan = (
            (hu, hd, src.at[own, first], hbot.at[f], {"row": up}),
            (hd, hu, src.at[own, last], htop.at[f], {"row": dn}),
            (hl, hr, csend.at[f, 0], hright.at[f], {"col": lf}),
            (hr, hl, csend.at[f, 1], hleft.at[f], {"col": rg}),
            (hu & hl, hd & hr, corner.at[f, 0], hcorner.at[f, 0], {"row": up, "col": lf}),
            (hu & hr, hd & hl, corner.at[f, 0], hcorner.at[f, 1], {"row": up, "col": rg}),
            (hd & hl, hu & hr, corner.at[f, 1], hcorner.at[f, 2], {"row": dn, "col": lf}),
            (hd & hr, hu & hl, corner.at[f, 1], hcorner.at[f, 3], {"row": dn, "col": rg}),
        )
        out = []
        for n, (to, frm, s, d, dev) in enumerate(plan):
            cp = pltpu.make_async_remote_copy(
                src_ref=s, dst_ref=d, send_sem=ha_s.at[f, n], recv_sem=ha_r.at[f, n],
                device_id=dev, device_id_type=MESH,
            )
            out.append((to, frm, cp))
        return out

    def halo_start(f, src):
        own = slice(OWN, OWN + TILE)
        for j in range(NB):
            t = jnp.transpose(src[j, own])
            csend[f, 0, j:j + 1] = t[0:1]
            csend[f, 1, 4 + j:5 + j] = t[127:128]
        for e, r in enumerate((OWN, OWN + TILE - 8)):
            x = jnp.zeros((8, 128), F32)
            for j in range(NB):
                b = src[j, r:r + 8]
                x = jnp.where(row8 == j, pltpu.roll(b, j, 1) if j else b, x)
                x = jnp.where(row8 == 124 + j, pltpu.roll(b, 125 + j, 1) if j < 3 else b, x)
            corner[f, e] = x
        cps = halo_copies(f, src)
        for to, _, cp in cps:
            pl.when(to)(cp.start)
        return cps

    def halo_finish(f, dst, cps):
        for _, frm, cp in cps:
            pl.when(frm)(cp.wait_recv)
        dst[0:NB, OWN - 8:OWN] = htop[f]
        dst[0:NB, OWN + TILE:OWN + TILE + 8] = hbot[f]
        x = jnp.concatenate([hright[f], jnp.zeros((112, TILE), F32), hleft[f]], axis=0)
        dst[NB, OWN:OWN + TILE] = jnp.transpose(x)
        near = row8 < 64
        dst[NB, OWN + TILE:OWN + TILE + 8] = jnp.where(near, hcorner[f, 0], hcorner[f, 1])
        dst[NB, OWN - 8:OWN] = jnp.where(near, hcorner[f, 2], hcorner[f, 3])

    def halo_sent(cps):
        for to, _, cp in cps:
            pl.when(to)(cp.wait_send)

    phase("dinv_halo")
    for buf in (dinv, f0, f1, f2, f3):
        buf[:, 0:8] = jnp.zeros((NB + 1, 8, 128), F32)
        buf[:, ROWS - 8:ROWS] = jnp.zeros((NB + 1, 8, 128), F32)
    dcp = halo_start(0, dinv)
    phase("send_side")
    pl.when(ri > 0)(lambda: pl.semaphore_wait(go.at[0], 1))
    pl.when(ri < nrow - 1)(lambda: pl.semaphore_wait(go.at[1], 1))
    qs = Exchange(lambda p: req.at[pl.ds(peer(p, 1), 3)], held_side, qs_s, qs_r, 1)
    qr = RowExchange(req, held_row, qr_s, qr_r)

    phase("wait_req")
    u = cinit[...]
    split[0:256] = jnp.concatenate(parts(u, 2), axis=0)
    ci128 = iota((128, 128), 0)
    for p in range(ncol):
        rq.arrived(p)
        at = slice(p * 128, (p + 1) * 128)
        idx = held[p]
        crow[:, at] = jnp.where(ci128 == (idx >> 7), 1.0, 0.0).astype(BF16)
        ccol[:, at] = jnp.where(ci128 == (idx & 127), 1.0, 0.0).astype(BF16)
    phase("lookup")
    for n in range(ncol // 2):
        at = slice(n * 256, (n + 1) * 256)
        t = dot(split[0:256], ccol[:, at], NN)
        t = jnp.sum((t[:128] + t[128:]) * crow[:, at].astype(F32), axis=0, keepdims=True)
        for p in (2 * n, 2 * n + 1):
            (look if p else atvia)[p] = t[:, (p - 2 * n) * 128:(p - 2 * n + 1) * 128]
    rs = Exchange(lambda p: look.at[p], atvia, rs_s, rs_r, -1)

    phase("coarse_diag")
    cdiag = 4.0 * CG + cleak[...] + VIA * dot(crow[...], ccol[...], NT)
    rdiag = RELAX / cdiag

    def coarse_start(s, u):
        ubuf[s] = u
        seam_t = jnp.transpose(u)
        for e, j in enumerate((0, GROUP - 1)):
            seam[s, e] = jnp.concatenate(
                [seam_t[g * GROUP + j:g * GROUP + j + 1] for g in range(128 // GROUP)], axis=0
            )
        up, dn = lax.rem(ri + nrow - 1, nrow), lax.rem(ri + 1, nrow)
        lf, rg = lax.rem(ci + ncol - 1, ncol), lax.rem(ci + 1, ncol)
        true = ri >= 0
        plan = (
            (ri > 0, ri < nrow - 1, ubuf.at[s, pl.ds(0, 8)], crecv.at[s, 1], {"row": up}),
            (ri < nrow - 1, ri > 0, ubuf.at[s, pl.ds(120, 8)], crecv.at[s, 0], {"row": dn}),
            (None, None, seam.at[s, 0], srecv.at[s, 1], {"col": lf}),
            (None, None, seam.at[s, 1], srecv.at[s, 0], {"col": rg}),
        )
        cps = []
        for n, (to, frm, sr, ds, dev) in enumerate(plan):
            cp = pltpu.make_async_remote_copy(
                src_ref=sr, dst_ref=ds, send_sem=ce_s.at[s, n], recv_sem=ce_r.at[s, n],
                device_id=dev, device_id_type=MESH,
            )
            if to is None:
                cp.start()
            else:
                pl.when(to)(cp.start)
            cps.append((to, frm, cp))
        return cps

    def coarse_wait(cps):
        for _, frm, cp in cps:
            if frm is None:
                cp.wait_recv()
            else:
                pl.when(frm)(cp.wait_recv)

    def coarse_beside(u, up, dn, fl, fr):
        li, si = iota((128, 128), 1), ci128
        up = jnp.where(si == 0, up, pltpu.roll(u, 1, 0))
        dn = jnp.where(si == 127, dn, pltpu.roll(u, 127, 0))
        g = iota((8, 128), 0)
        fl = jnp.where(ci == 0, jnp.where(g == 0, 0.0, pltpu.roll(fl, 1, 0)), fl)
        fr = jnp.where(ci == ncol - 1, jnp.where(g == 7, 0.0, pltpu.roll(fr, 7, 0)), fr)

        def spread(x):
            return jnp.concatenate([jnp.broadcast_to(x[q:q + 1], (GROUP, 128)) for q in range(8)], axis=0)

        x = jnp.transpose(jnp.where(si % GROUP == 0, spread(fl), spread(fr)))
        left = jnp.where(li % GROUP == 0, x, pltpu.roll(u, 1, 1))
        right = jnp.where(li % GROUP == GROUP - 1, x, pltpu.roll(u, 127, 1))
        return up + dn + left + right

    def coarse_sent(cps):
        for to, _, cp in cps:
            if to is None:
                cp.wait_send()
            else:
                pl.when(to)(cp.wait_send)

    phase("coarse_start")
    c0 = coarse_start(0, u)
    phase("load")
    for cp in loads[1:]:
        cp.wait()
    pa1[...], pb1[...] = parts(amp[...] * mask[...].astype(F32), 2)
    for h in range(2):
        hs = slice(h * 256, (h + 1) * 256)
        t = dot(pa1[...], perm[:, hs], NN) + dot(pb1[...], perm[:, hs], NN)
        for q in range(2):
            inj[2 * h + q] = t[:, q * 128:(q + 1) * 128]
    phase("dinv_finish")
    halo_finish(0, dinv, dcp)

    def make_inj(o):
        at = pl.ds(pl.multiple_of(o * 128, 128), 128)
        p = parts(atvia[o], 2)
        col = ct[:, at]
        cva[:, at] = col * p[0]
        cvb[:, at] = col * p[1]

    v0 = f0
    for part in range(2):
        phase(f"wait_resp{part}")
        for p in range(part * half, (part + 1) * half):
            rs.arrived(p)
            at = slice(p * 128, (p + 1) * 128)
            c = vfine[:, pl.ds(pl.multiple_of(peer(p, 1) * 128, 128), 128)]
            c = place(c & 511)
            v = atvia[p]
            va = v.astype(BF16).astype(F32)
            vb = v - va
            for q in range(4):
                hot = iota((128, 128), 0) + q * 128 == c
                cva[q * 128:(q + 1) * 128, at] = jnp.where(hot, va, 0.0).astype(BF16)
                cvb8[q * 128:(q + 1) * 128, at] = jnp.where(hot, vb * LOW, 0.0).astype(F8)
        phase(f"inject_dot{part}")
        ks = slice(part * half * 128, (part + 1) * half * 128)
        for h in range(2):
            hs = slice(h * 256, (h + 1) * 256)
            t = dot(rt[:, ks], cva[hs, ks], NT) + (1.0 / LOW) * dot(rt8[:, ks], cvb8[hs, ks], NT)
            for q in range(2):
                j = 2 * h + q
                tq = VIA * t[:, q * 128:(q + 1) * 128]
                if part == 0:
                    inj[j] = inj[j] + tq
                else:
                    z = (inj[j] + tq) * dinv[j, OWN:OWN + TILE]
                    v0[j, OWN:OWN + TILE] = z
                    za, zb = high_low(z)
                    pa0[:, j * 128:(j + 1) * 128] = za
                    pb8[0][:, j * 128:(j + 1) * 128] = zb
    phase("halo_start")
    fcp = halo_start(1, v0)

    def gather_part(k, n):
        at = slice(n * 256, n * 256 + 256) if isinstance(n, int) else pl.ds(pl.multiple_of(n * 256, 256), 256)
        t = dot(pa[k][...], ct[:, at], NN) + dot(pb8[k][...], ct8[:, at], NN)
        t = (VIA / HOT) * jnp.sum(t * rt[:, at].astype(F32), axis=0, keepdims=True)
        for p in (2 * n, 2 * n + 1):
            vals[1 + peer(p, 1), k:k + 1] = t[:, (p - 2 * n) * 128:(p - 2 * n + 1) * 128]

    def gather(k):
        for n in range(ncol // 2):
            gather_part(k, n)

    phase("gather0")
    gather(0)
    phase("sweep_pre")
    coarse_wait(c0)
    p0 = u + rdiag * (
        CG * coarse_beside(u, crecv[0, 0, 7:8], crecv[0, 1, 0:1], srecv[0, 0], srecv[0, 1]) - cdiag * u
    )
    c1 = coarse_start(1, p0)
    c2 = coarse_start(2, rdiag)
    phase("side_hot")
    for p in (1, half):
        qs.arrived(p)
    qr.arrived()
    for p in range(ncol):
        at = slice(p * 128, (p + 1) * 128)
        nodes = (held_side[p, 0] >> 7, held_side[p, 2] >> 7, held_row[0, p] & 127, held_row[1, p] & 127)
        for q, x in enumerate(nodes):
            side_hot[q, :, at] = jnp.where(ci128 == x, 1.0, 0.0).astype(BF16)
    phase("halo_finish")
    halo_finish(1, v0, fcp)

    phase("powers")
    def turn(v, r, h):
        rows = pl.ds(r, h)
        first, last, halo = v[0, rows], v[NB - 1, rows], v[NB, rows]
        turned[0, rows] = pltpu.roll(last, 1, 1)
        turned[1, rows] = pltpu.roll(halo, 1, 1)
        turned[2, rows] = pltpu.roll(first, 127, 1)
        turned[3, rows] = pltpu.roll(halo, 127, 1)

    def beside(v, r, h):
        lanes = iota((h, 128), 1)
        first_lane, last_lane = lanes == 0, lanes == 127
        rows = pl.ds(r, h)
        c = [v[j, rows] for j in range(NB + 1)]
        last_r, halo_r, first_l, halo_l = (turned[q, rows] for q in range(4))
        left = [jnp.where(first_lane, halo_r, last_r), *c[:NB - 1], jnp.where(first_lane, last_r, halo_r)]
        right = [*c[1:NB], jnp.where(last_lane, halo_l, first_l), jnp.where(last_lane, first_l, halo_l)]
        out = [
            v[j, pl.ds(r - 1, h)] + v[j, pl.ds(r + 1, h)] + left[j] + right[j] for j in range(NB + 1)
        ]
        return c, out

    def power(k):
        v, nxt = field[k], field[k + 1] if k < 3 else None
        count = (4, 4, 2, 1)[k]

        def rows(r, h, sums):
            c, nb = beside(v, r, h)
            sums = list(sums) if sums is not None else None

            def add(n, x):
                for q in range(h // 8):
                    sums[n] = sums[n] + x[q * 8:(q + 1) * 8]

            for j in range(NB + 1):
                w = None
                if nxt is not None:
                    w = dinv[j, pl.ds(r, h)] * nb[j]
                    nxt[j, pl.ds(r, h)] = w
                if sums is not None and j < NB:
                    if nxt is not None:
                        wa, wb = high_low(w)
                        pa[k + 1][pl.ds(r - OWN, h), j * 128:(j + 1) * 128] = wa
                        pb8[k + 1][pl.ds(pl.multiple_of(r - OWN, 32), h), j * 128:(j + 1) * 128] = wb
                    dv = diag[j, pl.ds(r - OWN, h)] * c[j]
                    av = dv - nb[j]
                    add(0, c[j] * av)
                    if count > 1:
                        add(1, w * av)
                    if count > 2:
                        add(2, c[j] * dv)
                        add(3, c[j] * nb[j])
            return tuple(sums) if sums is not None else None

        steps = ncol // 2 if k in FUSED else 8
        each = TILE // steps
        turn(v, OWN, each)
        if nxt is not None:
            for r in (OWN - 8, OWN + TILE):
                turn(v, r, 8)
                rows(r, 8, None)

        def step(i, sums, last=False):
            r = OWN + i * each if last else OWN + pl.multiple_of(i * each, 32)
            if k in FUSED:
                gather_part(k, i)
            if not last:
                turn(v, r + each, each)
            for q in range(each // 32):
                sums = rows(r + q * 32, 32, sums)
            return sums

        z = jnp.zeros((8, 128), F32)
        sums = lax.fori_loop(0, steps - 1, step, (z,) * count)
        return step(steps - 1, sums, last=True)

    n = 0
    for k in range(4):
        phase(f"power{k}")
        for s in power(k):
            mom[n:n + 1] = jnp.sum(s, axis=0, keepdims=True)
            n += 1
    mom[11:16] = jnp.zeros((5, 128), F32)

    phase("lane_sum")
    t = jnp.sum(mom[...], axis=1, keepdims=True)
    red_a[ci] = jnp.sum(jnp.where(iota((16, 128), 0) == iota((16, 128), 1), t, 0.0), axis=0, keepdims=True)

    def reduce_start(buf, axis, me, size, sems):
        for d in range(1, size):
            pltpu.make_async_remote_copy(
                src_ref=buf.at[me], dst_ref=buf.at[me], send_sem=sems.at[0], recv_sem=sems.at[1],
                device_id={axis: lax.rem(me + d, size)}, device_id_type=MESH,
            ).start()

    def reduce_finish(buf, size, sems):
        wait_bytes(buf.at[pl.ds(0, size - 1)], sems.at[1])
        t = buf[0]
        for q in range(1, size):
            t = t + buf[q]
        return t

    reduce_start(red_a, "col", ci, ncol, sum_sem.at[0])
    phase("gather123")
    for k in range(1, 4):
        gather(k)
    vals[0] = vals[ncol]
    vals[ncol + 1] = vals[1]
    ar = Exchange(lambda p: vals.at[pl.ds(peer(p, 1), 3)], arrived, ar_s, ar_r, 1)
    vr = RowExchange(vals, arrived_row, vr_s, vr_r)
    for q in range(3):
        arrived[0, q] = vals[ci + q]
    phase("reduce_col")
    red_b[ri] = reduce_finish(red_a, ncol, sum_sem.at[0])
    reduce_start(red_b, "row", ri, nrow, sum_sem.at[1])
    phase("reduce_row")
    tot = reduce_finish(red_b, nrow, sum_sem.at[1])

    phase("solve")
    def m(q):
        return jnp.broadcast_to(jnp.sum(jnp.where(lane == q, tot, 0.0), axis=1, keepdims=True), (1, 128))

    eta = [m(q) for q in (0, 1, 4, 5, 8, 9, 10)]
    nu = [m(q) for q in (2, 3, 6, 7)]
    hm = [[eta[i + j] for j in range(4)] for i in range(4)]
    low = [[None] * 4 for _ in range(4)]
    piv = []
    for j in range(4):
        pj = hm[j][j]
        for q in range(j):
            pj = pj - low[j][q] * low[j][q] * piv[q]
        ok = pj > 1e-6 * hm[j][j]
        piv.append(pj)
        inv = jnp.where(ok, 1.0 / jnp.where(ok, pj, 1.0), 0.0)
        low[j][j] = inv
        for i in range(j + 1, 4):
            e = hm[i][j]
            for q in range(j):
                e = e - low[i][q] * low[j][q] * piv[q]
            low[i][j] = e * inv
    y = list(nu)
    for i in range(4):
        for q in range(i):
            y[i] = y[i] - low[i][q] * y[q]
    y = [y[i] * low[i][i] for i in range(4)]
    for i in (2, 1, 0):
        for q in range(i + 1, 4):
            y[i] = y[i] - low[q][i] * y[q]
    phase("combine")

    def combine(i, _):
        r = pl.multiple_of(i * 16, 16)
        for j in range(NB):
            rows = pl.ds(OWN + r, 16)
            a = y[0] * f0[j, rows]
            for k in range(1, 4):
                a = a + y[k] * field[k][j, rows]
            at = slice(j * 128, (j + 1) * 128)
            for x, buf in zip(parts(a, 3), (pa0, pb0, pa1)):
                buf[pl.ds(r, 16), at] = x
        return _

    lax.fori_loop(0, TILE // 16, combine, 0, unroll=4)
    for h in range(2):
        hs = slice(h * 256, (h + 1) * 256)
        fine_o[:, hs] = sum(dot(buf[...], perm[hs, :], NT) for buf in (pa0, pb0, pa1))

    fine_out = pltpu.make_async_copy(fine_o, fine_h, out_sem.at[0])
    fine_out.start()
    phase("wait_vals")
    coarse_wait(c1)
    coarse_wait(c2)
    i8, i16 = iota((8, 128), 0), iota((16, 128), 0)
    coef = jnp.concatenate(y, axis=0)

    def current(x):
        a = jnp.sum(coef * x, axis=0, keepdims=True)
        hi = a.astype(BF16).astype(F32)
        return hi, a - hi

    for p in range(ncol):
        ar.arrived(p)
        at = slice(p * 128, (p + 1) * 128)
        hot = crow[:, at]
        for n, x in enumerate(current(arrived[p, 1])):
            cva[n * 128:(n + 1) * 128, at] = hot * x.astype(BF16)
        for q, edge in ((0, GROUP - 1), (1, 0)):
            on = i8 * GROUP + edge == (held_side[p, 2 * q] & 127)
            x = [jnp.where(on, x, 0.0) for x in current(arrived[p, 2 * q])]
            cvb[q * 16:(q + 1) * 16, at] = jnp.concatenate(x, axis=0).astype(BF16)
    phase("sources")
    t = dot(cva[0:256, :], ccol[...], NT)
    src = t[:128] + t[128:]
    side = [dot(cvb[q * 16:(q + 1) * 16, :], side_hot[q], NT) for q in range(2)]
    phase("wait_rows")
    vr.arrived()
    for p in range(ncol):
        at = slice(p * 128, (p + 1) * 128)
        for q, edge in ((0, 127), (1, 0)):
            hi, lo = current(arrived_row[q, p])
            on = (held_row[q, p] >> 7) == edge
            x = jnp.where(i16 == 0, jnp.where(on, hi, 0.0), jnp.where(i16 == 1, jnp.where(on, lo, 0.0), 0.0))
            cvb[32 + q * 16:48 + q * 16, at] = x.astype(BF16)
    side += [dot(cvb[q * 16:(q + 1) * 16, :], side_hot[q], NT) for q in (2, 3)]
    phase("sweeps")
    u1 = p0 + rdiag * src
    beside1 = coarse_beside(
        u1,
        crecv[1, 0, 7:8] + crecv[2, 0, 7:8] * (side[2][0:1] + side[2][1:2]),
        crecv[1, 1, 0:1] + crecv[2, 1, 0:1] * (side[3][0:1] + side[3][1:2]),
        srecv[1, 0] + srecv[2, 0] * (side[0][0:8] + side[0][8:16]),
        srecv[1, 1] + srecv[2, 1] * (side[1][0:8] + side[1][8:16]),
    )
    coarse_o[...] = u1 + rdiag * (src + CG * beside1 - cdiag * u1)
    coarse_out = pltpu.make_async_copy(coarse_o, coarse_h, out_sem.at[1])
    coarse_out.start()
    phase("drain")
    for x in (rq, qs, rs, ar, qr, vr):
        x.sent()
    wait_bytes(red_a.at[pl.ds(0, ncol - 1)], sum_sem.at[0, 0])
    wait_bytes(red_b.at[pl.ds(0, nrow - 1)], sum_sem.at[1, 0])
    coarse_sent(c2)
    halo_sent(dcp)
    halo_sent(fcp)
    coarse_sent(c0)
    coarse_sent(c1)
    fine_out.wait()
    coarse_out.wait()
    phase("")


def hand_out(fine, coarse, fine_h, coarse_h, sem):
    copies = [pltpu.make_async_copy(fine, fine_h, sem.at[0]), pltpu.make_async_copy(coarse, coarse_h, sem.at[1])]
    for cp in copies:
        cp.start()
    for cp in copies:
        cp.wait()


def solution(mesh):
    nrow, ncol = mesh.shape["row"], mesh.shape["col"]
    slots = ncol * 128
    dma = pltpu.SemaphoreType.DMA

    def step(*args):
        anyspace = pl.BlockSpec(memory_space=pl.ANY)
        hbm = pl.BlockSpec(memory_space=pltpu.HBM)
        slab = (NB, TILE, 128)
        row = (ncol, 1, 128)
        fine, coarse = pl.pallas_call(
            functools.partial(kernel, nrow, ncol),
            out_shape=(
                pltpu.VMEM((TILE, TILE), F32),
                pltpu.VMEM((COARSE, COARSE), F32),
            ),
            in_specs=[hbm] * 8,
            out_specs=(anyspace, anyspace),
            scratch_shapes=[
                pltpu.VMEM((TILE, TILE), F32), pltpu.VMEM((TILE, TILE), I32), pltpu.VMEM((TILE, TILE), F32),
                pltpu.VMEM((TILE, TILE), BF16),
                pltpu.VMEM((TILE, slots), BF16), pltpu.VMEM((TILE, slots), BF16),
                pltpu.VMEM((TILE, slots), BF16), pltpu.VMEM((TILE, slots), BF16),
                *[pltpu.VMEM((NB + 1, ROWS, 128), F32)] * 4, pltpu.VMEM((4, ROWS, 128), F32), pltpu.VMEM((NB + 1, ROWS, 128), F32),
                pltpu.VMEM(slab, F32), pltpu.VMEM(slab, F32),
                *[pltpu.VMEM((TILE, TILE), BF16)] * 7, *[pltpu.VMEM((TILE, TILE), F8)] * 4, *[pltpu.VMEM((TILE, slots), F8)] * 3,
                pltpu.VMEM((ncol + 2, 1, 128), I32), pltpu.VMEM(row, I32),
                pltpu.VMEM((ncol, 3, 1, 128), I32), pltpu.VMEM((2, ncol, 1, 128), I32),
                pltpu.VMEM(row, F32), pltpu.VMEM(row, F32),
                pltpu.VMEM((ncol + 2, 4, 128), F32), pltpu.VMEM((ncol, 3, 4, 128), F32),
                pltpu.VMEM((2, ncol, 4, 128), F32), pltpu.VMEM((4, 128, slots), BF16),
                pltpu.VMEM((128, slots), BF16), pltpu.VMEM((128, slots), BF16),
                pltpu.VMEM((2, NB, 8, 128), F32), pltpu.VMEM((2, NB, 8, 128), F32),
                pltpu.VMEM((2, 8, TILE), F32), pltpu.VMEM((2, 8, TILE), F32),
                pltpu.VMEM((2, 4, 8, 128), F32), pltpu.VMEM((2, 2, 8, TILE), F32), pltpu.VMEM((2, 2, 8, 128), F32),
                pltpu.VMEM((16, 128), F32), pltpu.VMEM((ncol, 1, 128), F32), pltpu.VMEM((nrow, 1, 128), F32),
                pltpu.VMEM((256, 128), BF16),
                pltpu.VMEM((3, 128, 128), F32), pltpu.VMEM((3, 2, 8, 128), F32),
                pltpu.VMEM((3, 2, 8, 128), F32), pltpu.VMEM((3, 2, 8, 128), F32),
                pltpu.VMEM((TILE, TILE), F32), pltpu.VMEM((COARSE, COARSE), F32),
                pltpu.VMEM((COARSE, COARSE), F32), pltpu.VMEM((COARSE, COARSE), F32),
                pltpu.VMEM((1, slots), I32), pltpu.VMEM((1, slots), I32), pltpu.SMEM((1, ncol), I32),
                dma((3,)), dma((5,)), dma((2,)),
                *[dma(()), dma((2,))] * 3,
                pltpu.SemaphoreType.REGULAR((2,)),
                dma(()), dma((2,)), *[dma((2,))] * 4,
                dma((2, 8)), dma((2, 8)), dma((2, 2)),
                dma((3, 4)), dma((3, 4)),
            ],
            compiler_params=pltpu.CompilerParams(
                collective_id=0, has_side_effects=True, vmem_limit_bytes=50 << 20),
        )(*[pltpu.with_memory_space_constraint(x, pltpu.HBM) for x in args])
        return pl.pallas_call(
            hand_out,
            out_shape=(
                jax.ShapeDtypeStruct((TILE, TILE), F32),
                jax.ShapeDtypeStruct((COARSE, COARSE), F32),
            ),
            in_specs=[anyspace, anyspace],
            out_specs=(anyspace, anyspace),
            scratch_shapes=[dma((2,))],
        )(pltpu.with_memory_space_constraint(fine, pltpu.VMEM), pltpu.with_memory_space_constraint(coarse, pltpu.VMEM))

    spec = P("row", "col")
    return jax.shard_map(
        step, mesh=mesh, in_specs=(spec,) * 8, out_specs=(spec, spec), check_vma=False
    )
```

```python
import functools

import jax
import jax.numpy as jnp
from jax import lax
from jax.experimental import pallas as pl
from jax.experimental.pallas import tpu as pltpu
from jax.sharding import PartitionSpec as P

MESH = pl.DeviceIdType.MESH
F8 = jnp.float8_e4m3fn
HOT = 64.0
LOW = HOT * HOT
F32, BF16, I32 = jnp.float32, jnp.bfloat16, jnp.int32
GROUP = 16
NB = 4
OWN = 16
TILE = 512
ROWS = TILE + 2 * OWN
COARSE = 128
VIA = 2.0
CG = 4.0
RELAX = 0.8
NN = (((1,), (0,)), ((), ()))
NT = (((1,), (1,)), ((), ()))


def place(c):
    return (c & 3) * 128 + (c >> 2)


def iota(shape, dim):
    return lax.broadcasted_iota(I32, shape, dim)


def dot(a, b, dims):
    return lax.dot_general(a, b, dims, preferred_element_type=F32)


def parts(x, n):
    out = []
    for _ in range(n):
        p = x.astype(BF16)
        out.append(p)
        x = x - p.astype(F32)
    return out


class Phases:
    def __init__(self):
        self.open = None

    def __call__(self, name):
        if self.open is not None:
            self.open.__exit__(None, None, None)
        self.open = None
        if name:
            self.open = jax.named_scope(name)
            self.open.__enter__()


def peer_order(n):
    if n != 16:
        return list(range(n))
    return sorted(range(n), key=lambda d: min(d // 4, 4 - d // 4) + min(d % 4, 4 - d % 4))


def high_low(x):
    p = x.astype(BF16)
    return p, ((x - p.astype(F32)) * LOW).astype(F8)


def kernel(
    nrow, ncol,
    amp_h, mask_h, leak_h, cleak_h, cinit_h, vfine_h, vcoarse_h, vcount_h,
    fine_h, coarse_h,
    amp, mask, leak, perm, rt, ct, cva, cvb, f0, f1, f2, f3, turned, dinv, diag, inj, pa0, pa1, pa2, pa3, pb0, pb1, pb2, pb80, pb81, pb82, pb83, ct8, rt8, cvb8,
    req, held, held_side, held_row, look, atvia, vals, arrived, arrived_row, side_hot,
    crow, ccol, htop, hbot, hleft, hright, hcorner, csend, corner,
    mom, red_a, red_b, split, ubuf, seam, crecv, srecv, fine_o, coarse_o,
    cleak, cinit, vfine, vcoarse, vcount,
    in_sem, small_sem, out_sem, rq_s, rq_r, rs_s, rs_r, ar_s, ar_r,
    go, qs_s, qs_r, qr_s, qr_r, vr_s, vr_r, ha_s, ha_r, sum_sem, ce_s, ce_r,
):
    field, pa, pb8 = (f0, f1, f2, f3), (pa0, pa1, pa2, pa3), (pb80, pb81, pb82, pb83)
    slots = ncol * 128
    phase = Phases()
    phase("start")
    ri, ci = lax.axis_index("row"), lax.axis_index("col")

    small = []
    for n, (src, dst) in enumerate((
        (vcount_h, vcount), (vcoarse_h, vcoarse), (vfine_h, vfine), (cinit_h, cinit), (cleak_h, cleak)
    )):
        cp = pltpu.make_async_copy(src, dst, small_sem.at[n])
        cp.start()
        small.append(cp)
    loads = []
    for n, (src, dst) in enumerate(((leak_h, leak), (amp_h, amp), (mask_h, mask))):
        cp = pltpu.make_async_copy(src, dst, in_sem.at[n])
        cp.start()
        loads.append(cp)

    for buf in (htop, hbot, hleft, hright, hcorner, crecv, csend):
        buf[...] = jnp.zeros(buf.shape, F32)
    arrived_row[...] = jnp.zeros(arrived_row.shape, F32)
    held_row[...] = jnp.full(held_row.shape, -1, I32)

    phase("barrier")
    order = peer_order(ncol)

    def peer(p, sign):
        if ncol != 16:
            return lax.rem(ci + (order[p] if sign > 0 else ncol - order[p]), ncol)
        dy, dx = order[p] // 4, order[p] % 4
        y, x = ci // 4, lax.rem(ci, 4)
        if sign < 0:
            dy, dx = 4 - dy, 4 - dx
        return lax.rem(y + dy, 4) * 4 + lax.rem(x + dx, 4)

    bar = pltpu.get_barrier_semaphore()
    for d in range(1, ncol):
        pl.semaphore_signal(bar, inc=1, device_id={"col": lax.rem(ci + d, ncol)}, device_id_type=MESH)
    for d in range(1, nrow):
        pl.semaphore_signal(bar, inc=1, device_id={"row": lax.rem(ri + d, nrow)}, device_id_type=MESH)
    for dr in (1, nrow - 1):
        for dc in (1, ncol - 1):
            pl.semaphore_signal(
                bar, inc=1,
                device_id={"row": lax.rem(ri + dr, nrow), "col": lax.rem(ci + dc, ncol)},
                device_id_type=MESH,
            )
    phase("wait_small")
    for cp in small:
        cp.wait()
    lane = iota((1, 128), 1)

    def wait_bytes(ref, sem):
        pltpu.make_async_copy(ref, ref, sem).wait()

    half = ncol // 2

    class Exchange:
        def __init__(self, src, dst, ssem, rsem, sign):
            self.dst, self.ssem, self.rsem = dst, ssem, rsem
            for p in reversed(range(1, ncol)):
                pltpu.make_async_remote_copy(
                    src_ref=src(p), dst_ref=dst.at[p], send_sem=ssem, recv_sem=rsem.at[p // half],
                    device_id={"col": peer(p, sign)}, device_id_type=MESH,
                ).start()

        def arrived(self, p):
            if p == 1:
                wait_bytes(self.dst.at[pl.ds(1, half - 1)], self.rsem.at[0])
            if p == half:
                wait_bytes(self.dst.at[pl.ds(half, half)], self.rsem.at[1])

        def sent(self):
            wait_bytes(self.dst.at[pl.ds(1, ncol - 1)], self.ssem)

    class RowExchange:
        def __init__(self, src, dst, ssem, rsem):
            self.dst, self.ssem, self.rsem = dst, ssem, rsem
            self.sides = ((0, 1, ri < nrow - 1, ri > 0), (1, nrow - 1, ri > 0, ri < nrow - 1))
            for side, dr, to, _ in self.sides:

                @pl.when(to)
                def _():
                    for p in reversed(range(ncol)):
                        pltpu.make_async_remote_copy(
                            src_ref=src.at[1 + peer(p, 1)], dst_ref=dst.at[side, p],
                            send_sem=ssem.at[side], recv_sem=rsem.at[side],
                            device_id={"row": lax.rem(ri + dr, nrow), "col": peer(p, 1)}, device_id_type=MESH,
                        ).start()

        def arrived(self):
            for side, _, _, frm in self.sides:
                pl.when(frm)(lambda: wait_bytes(self.dst.at[side], self.rsem.at[side]))

        def sent(self):
            for side, _, to, _ in self.sides:
                pl.when(to)(lambda: wait_bytes(self.dst.at[side], self.ssem.at[side]))

    phase("requests")
    for p in reversed(range(ncol)):
        o = peer(p, 1)
        idx = vcoarse[:, pl.ds(pl.multiple_of(o * 128, 128), 128)]
        node = lax.shift_right_logical(idx, lax.full_like(idx, (slots).bit_length() - 1)) * 128 + (idx & 127)
        node = jnp.where(lane < vcount[0, o], node, -1)
        req[1 + o] = node
        if p == 0:
            held[0] = node
    req[0] = req[ncol]
    req[ncol + 1] = req[1]
    for q in range(3):
        held_side[0, q] = req[ci + q]
    phase("barrier_wait")
    pl.semaphore_wait(bar, ncol + nrow + 2)

    @pl.when(ri < nrow - 1)
    def _():
        pl.semaphore_signal(go.at[0], inc=1, device_id={"row": lax.rem(ri + 1, nrow)}, device_id_type=MESH)

    @pl.when(ri > 0)
    def _():
        pl.semaphore_signal(go.at[1], inc=1, device_id={"row": lax.rem(ri + nrow - 1, nrow)}, device_id_type=MESH)


    phase("send_req")
    rq = Exchange(lambda p: req.at[1 + peer(p, 1)], held, rq_s, rq_r, 1)

    phase("fine_onehot")
    for p in range(ncol):
        o = peer(p, 1)
        idx = vfine[:, pl.ds(pl.multiple_of(o * 128, 128), 128)]
        at = slice(p * 128, (p + 1) * 128)
        r = jnp.where(lane < vcount[0, o], idx >> 9, -1)
        c = place(idx & 511)
        for q in range(4):
            i = iota((128, 128), 0) + q * 128
            rt[q * 128:(q + 1) * 128, at] = jnp.where(i == r, 1.0, 0.0).astype(BF16)
            rt8[q * 128:(q + 1) * 128, at] = jnp.where(i == r, 1.0, 0.0).astype(F8)
            ct[q * 128:(q + 1) * 128, at] = jnp.where(i == c, HOT, 0.0).astype(BF16)
            ct8[q * 128:(q + 1) * 128, at] = jnp.where(i == c, 1.0 / HOT, 0.0).astype(F8)
    perm[...] = jnp.where(place(iota((TILE, TILE), 0)) == iota((TILE, TILE), 1), 1.0, 0.0).astype(BF16)
    phase("count_dot")
    loads[0].wait()
    pa2[...], pb2[...] = parts(leak[...], 2)
    for h in range(2):
        hs = slice(h * 256, (h + 1) * 256)
        t = (VIA * HOT) * dot(rt8[...], ct8[hs, :], NT)
        t = t + (dot(pa2[...], perm[:, hs], NN) + dot(pb2[...], perm[:, hs], NN))
        for q in range(2):
            j = 2 * h + q
            dg = 4.0 + t[:, q * 128:(q + 1) * 128]
            diag[j] = dg
            dinv[j, OWN:OWN + TILE] = 1.0 / dg

    row8 = iota((8, 128), 1)

    def halo_copies(f, src):
        up, dn = lax.rem(ri + nrow - 1, nrow), lax.rem(ri + 1, nrow)
        lf, rg = lax.rem(ci + ncol - 1, ncol), lax.rem(ci + 1, ncol)
        hu, hd, hl, hr = ri > 0, ri < nrow - 1, ci > 0, ci < ncol - 1
        first, last = pl.ds(OWN, 8), pl.ds(OWN + TILE - 8, 8)
        own = pl.ds(0, NB)
        plan = (
            (hu, hd, src.at[own, first], hbot.at[f], {"row": up}),
            (hd, hu, src.at[own, last], htop.at[f], {"row": dn}),
            (hl, hr, csend.at[f, 0], hright.at[f], {"col": lf}),
            (hr, hl, csend.at[f, 1], hleft.at[f], {"col": rg}),
            (hu & hl, hd & hr, corner.at[f, 0], hcorner.at[f, 0], {"row": up, "col": lf}),
            (hu & hr, hd & hl, corner.at[f, 0], hcorner.at[f, 1], {"row": up, "col": rg}),
            (hd & hl, hu & hr, corner.at[f, 1], hcorner.at[f, 2], {"row": dn, "col": lf}),
            (hd & hr, hu & hl, corner.at[f, 1], hcorner.at[f, 3], {"row": dn, "col": rg}),
        )
        out = []
        for n, (to, frm, s, d, dev) in enumerate(plan):
            cp = pltpu.make_async_remote_copy(
                src_ref=s, dst_ref=d, send_sem=ha_s.at[n], recv_sem=ha_r.at[f, n],
                device_id=dev, device_id_type=MESH,
            )
            out.append((to, frm, cp))
        return out

    def halo_start(f, src):
        own = slice(OWN, OWN + TILE)
        for j in range(NB):
            t = jnp.transpose(src[j, own])
            csend[f, 0, j:j + 1] = t[0:1]
            csend[f, 1, 4 + j:5 + j] = t[127:128]
        for e, r in enumerate((OWN, OWN + TILE - 8)):
            x = jnp.zeros((8, 128), F32)
            for j in range(NB):
                b = src[j, r:r + 8]
                x = jnp.where(row8 == j, pltpu.roll(b, j, 1) if j else b, x)
                x = jnp.where(row8 == 124 + j, pltpu.roll(b, 125 + j, 1) if j < 3 else b, x)
            corner[f, e] = x
        cps = halo_copies(f, src)
        for to, _, cp in cps:
            pl.when(to)(cp.start)
        return cps

    def halo_finish(f, dst, cps):
        for _, frm, cp in cps:
            pl.when(frm)(cp.wait_recv)
        dst[0:NB, OWN - 8:OWN] = htop[f]
        dst[0:NB, OWN + TILE:OWN + TILE + 8] = hbot[f]
        x = jnp.concatenate([hright[f], jnp.zeros((112, TILE), F32), hleft[f]], axis=0)
        dst[NB, OWN:OWN + TILE] = jnp.transpose(x)
        near = row8 < 64
        dst[NB, OWN + TILE:OWN + TILE + 8] = jnp.where(near, hcorner[f, 0], hcorner[f, 1])
        dst[NB, OWN - 8:OWN] = jnp.where(near, hcorner[f, 2], hcorner[f, 3])

    def halo_sent(cps):
        for n, (to, _, _) in enumerate(cps):
            both = htop if n < 2 else hleft if n < 4 else corner.at[0]
            pl.when(to)(lambda: wait_bytes(both, ha_s.at[n]))

    for buf in (dinv, f0, f1, f2, f3):
        buf[:, 0:8] = jnp.zeros((NB + 1, 8, 128), F32)
        buf[:, ROWS - 8:ROWS] = jnp.zeros((NB + 1, 8, 128), F32)
    dcp = halo_start(0, dinv)
    phase("send_side")
    pl.when(ri > 0)(lambda: pl.semaphore_wait(go.at[0], 1))
    pl.when(ri < nrow - 1)(lambda: pl.semaphore_wait(go.at[1], 1))
    qs = Exchange(lambda p: req.at[pl.ds(peer(p, 1), 3)], held_side, qs_s, qs_r, 1)
    qr = RowExchange(req, held_row, qr_s, qr_r)

    phase("wait_req")
    u = cinit[...]
    split[0:256] = jnp.concatenate(parts(u, 2), axis=0)
    ci128 = iota((128, 128), 0)
    for p in range(ncol):
        rq.arrived(p)
        at = slice(p * 128, (p + 1) * 128)
        idx = held[p]
        crow[:, at] = jnp.where(ci128 == (idx >> 7), 1.0, 0.0).astype(BF16)
        ccol[:, at] = jnp.where(ci128 == (idx & 127), 1.0, 0.0).astype(BF16)
    phase("lookup")
    for n in range(ncol // 2):
        at = slice(n * 256, (n + 1) * 256)
        t = dot(split[0:256], ccol[:, at], NN)
        t = jnp.sum((t[:128] + t[128:]) * crow[:, at].astype(F32), axis=0, keepdims=True)
        for p in (2 * n, 2 * n + 1):
            (look if p else atvia)[p] = t[:, (p - 2 * n) * 128:(p - 2 * n + 1) * 128]
    rs = Exchange(lambda p: look.at[p], atvia, rs_s, rs_r, -1)

    phase("coarse_diag")
    cdiag = 4.0 * CG + cleak[...] + VIA * dot(crow[...], ccol[...], NT)
    rdiag = RELAX / cdiag

    def coarse_start(s, u):
        ubuf[s] = u
        seam_t = jnp.transpose(u)
        for e, j in enumerate((0, GROUP - 1)):
            seam[s, e] = jnp.concatenate(
                [seam_t[g * GROUP + j:g * GROUP + j + 1] for g in range(128 // GROUP)], axis=0
            )
        up, dn = lax.rem(ri + nrow - 1, nrow), lax.rem(ri + 1, nrow)
        lf, rg = lax.rem(ci + ncol - 1, ncol), lax.rem(ci + 1, ncol)
        true = ri >= 0
        plan = (
            (ri > 0, ri < nrow - 1, ubuf.at[s, pl.ds(0, 8)], crecv.at[s, 1], {"row": up}),
            (ri < nrow - 1, ri > 0, ubuf.at[s, pl.ds(120, 8)], crecv.at[s, 0], {"row": dn}),
            (None, None, seam.at[s, 0], srecv.at[s, 1], {"col": lf}),
            (None, None, seam.at[s, 1], srecv.at[s, 0], {"col": rg}),
        )
        cps = []
        for n, (to, frm, sr, ds, dev) in enumerate(plan):
            cp = pltpu.make_async_remote_copy(
                src_ref=sr, dst_ref=ds, send_sem=ce_s.at[min(n, 2)], recv_sem=ce_r.at[s, min(n, 2)],
                device_id=dev, device_id_type=MESH,
            )
            if to is None:
                cp.start()
            else:
                pl.when(to)(cp.start)
            cps.append((to, frm, cp))
        return cps

    def coarse_wait(s, cps):
        for _, frm, cp in cps[:2]:
            pl.when(frm)(cp.wait_recv)
        wait_bytes(srecv.at[s], ce_r.at[s, 2])

    def coarse_beside(u, up, dn, fl, fr):
        li, si = iota((128, 128), 1), ci128
        up = jnp.where(si == 0, up, pltpu.roll(u, 1, 0))
        dn = jnp.where(si == 127, dn, pltpu.roll(u, 127, 0))
        g = iota((8, 128), 0)
        fl = jnp.where(ci == 0, jnp.where(g == 0, 0.0, pltpu.roll(fl, 1, 0)), fl)
        fr = jnp.where(ci == ncol - 1, jnp.where(g == 7, 0.0, pltpu.roll(fr, 7, 0)), fr)

        def spread(x):
            return jnp.concatenate([jnp.broadcast_to(x[q:q + 1], (GROUP, 128)) for q in range(8)], axis=0)

        x = jnp.transpose(jnp.where(si % GROUP == 0, spread(fl), spread(fr)))
        left = jnp.where(li % GROUP == 0, x, pltpu.roll(u, 1, 1))
        right = jnp.where(li % GROUP == GROUP - 1, x, pltpu.roll(u, 127, 1))
        return up + dn + left + right

    def coarse_sent(cps):
        for n in range(2):
            pl.when(cps[n][0])(lambda: wait_bytes(ubuf.at[0, pl.ds(0, 24)], ce_s.at[n]))
        wait_bytes(seam, ce_s.at[2])

    phase("coarse_start")
    c0 = coarse_start(0, u)
    phase("load")
    for cp in loads[1:]:
        cp.wait()
    pa1[...], pb1[...] = parts(amp[...] * mask[...].astype(F32), 2)
    for h in range(2):
        hs = slice(h * 256, (h + 1) * 256)
        t = dot(pa1[...], perm[:, hs], NN) + dot(pb1[...], perm[:, hs], NN)
        for q in range(2):
            inj[2 * h + q] = t[:, q * 128:(q + 1) * 128]
    phase("dinv_finish")
    halo_finish(0, dinv, dcp)

    def make_inj(o):
        at = pl.ds(pl.multiple_of(o * 128, 128), 128)
        p = parts(atvia[o], 2)
        col = ct[:, at]
        cva[:, at] = col * p[0]
        cvb[:, at] = col * p[1]

    v0 = f0
    for part in range(2):
        phase(f"wait_resp{part}")
        for p in range(part * half, (part + 1) * half):
            rs.arrived(p)
            at = slice(p * 128, (p + 1) * 128)
            c = vfine[:, pl.ds(pl.multiple_of(peer(p, 1) * 128, 128), 128)]
            c = place(c & 511)
            v = atvia[p]
            va = v.astype(BF16).astype(F32)
            vb = v - va
            for q in range(4):
                hot = iota((128, 128), 0) + q * 128 == c
                cva[q * 128:(q + 1) * 128, at] = jnp.where(hot, va, 0.0).astype(BF16)
                cvb8[q * 128:(q + 1) * 128, at] = jnp.where(hot, vb * LOW, 0.0).astype(F8)
        phase(f"inject_dot{part}")
        ks = slice(part * half * 128, (part + 1) * half * 128)
        for h in range(2):
            hs = slice(h * 256, (h + 1) * 256)
            t = dot(rt[:, ks], cva[hs, ks], NT) + (1.0 / LOW) * dot(rt8[:, ks], cvb8[hs, ks], NT)
            for q in range(2):
                j = 2 * h + q
                tq = VIA * t[:, q * 128:(q + 1) * 128]
                if part == 0:
                    inj[j] = inj[j] + tq
                else:
                    z = (inj[j] + tq) * dinv[j, OWN:OWN + TILE]
                    v0[j, OWN:OWN + TILE] = z
                    za, zb = high_low(z)
                    pa0[:, j * 128:(j + 1) * 128] = za
                    pb8[0][:, j * 128:(j + 1) * 128] = zb
    phase("halo_start")
    fcp = halo_start(1, v0)

    def gather_part(k, n):
        at = slice(n * 256, n * 256 + 256) if isinstance(n, int) else pl.ds(pl.multiple_of(n * 256, 256), 256)
        t = dot(pa[k][...], ct[:, at], NN) + dot(pb8[k][...], ct8[:, at], NN)
        t = (VIA / HOT) * jnp.sum(t * rt[:, at].astype(F32), axis=0, keepdims=True)
        for p in (2 * n, 2 * n + 1):
            vals[1 + peer(p, 1), k:k + 1] = t[:, (p - 2 * n) * 128:(p - 2 * n + 1) * 128]

    def gather(k):
        for n in range(ncol // 2):
            gather_part(k, n)

    phase("gather0")
    gather(0)
    phase("sweep_pre")
    coarse_wait(0, c0)
    p0 = u + rdiag * (
        CG * coarse_beside(u, crecv[0, 0, 7:8], crecv[0, 1, 0:1], srecv[0, 0], srecv[0, 1]) - cdiag * u
    )
    c1 = coarse_start(1, p0)
    c2 = coarse_start(2, rdiag)
    phase("side_hot")
    for p in (1, half):
        qs.arrived(p)
    qr.arrived()
    for p in range(ncol):
        at = slice(p * 128, (p + 1) * 128)
        nodes = (held_side[p, 0] >> 7, held_side[p, 2] >> 7, held_row[0, p] & 127, held_row[1, p] & 127)
        for q, x in enumerate(nodes):
            side_hot[q, :, at] = jnp.where(ci128 == x, 1.0, 0.0).astype(BF16)
    phase("halo_finish")
    halo_finish(1, v0, fcp)

    phase("powers")
    def turn(v, r, h):
        rows = pl.ds(r, h)
        first, last, halo = v[0, rows], v[NB - 1, rows], v[NB, rows]
        turned[0, rows] = pltpu.roll(last, 1, 1)
        turned[1, rows] = pltpu.roll(halo, 1, 1)
        turned[2, rows] = pltpu.roll(first, 127, 1)
        turned[3, rows] = pltpu.roll(halo, 127, 1)

    def beside(v, r, h):
        lanes = iota((h, 128), 1)
        first_lane, last_lane = lanes == 0, lanes == 127
        rows = pl.ds(r, h)
        c = [v[j, rows] for j in range(NB + 1)]
        last_r, halo_r, first_l, halo_l = (turned[q, rows] for q in range(4))
        left = [jnp.where(first_lane, halo_r, last_r), *c[:NB - 1], jnp.where(first_lane, last_r, halo_r)]
        right = [*c[1:NB], jnp.where(last_lane, halo_l, first_l), jnp.where(last_lane, first_l, halo_l)]
        out = [
            v[j, pl.ds(r - 1, h)] + v[j, pl.ds(r + 1, h)] + left[j] + right[j] for j in range(NB + 1)
        ]
        return c, out

    def power(k):
        v, nxt = field[k], field[k + 1] if k < 3 else None
        count = (4, 4, 2, 1)[k]

        def rows(r, h, sums):
            c, nb = beside(v, r, h)
            sums = list(sums) if sums is not None else None

            def add(n, x):
                for q in range(h // 8):
                    sums[n] = sums[n] + x[q * 8:(q + 1) * 8]

            for j in range(NB + 1):
                w = None
                if nxt is not None:
                    w = dinv[j, pl.ds(r, h)] * nb[j]
                    nxt[j, pl.ds(r, h)] = w
                if sums is not None and j < NB:
                    if nxt is not None:
                        wa, wb = high_low(w)
                        pa[k + 1][pl.ds(r - OWN, h), j * 128:(j + 1) * 128] = wa
                        pb8[k + 1][pl.ds(pl.multiple_of(r - OWN, 32), h), j * 128:(j + 1) * 128] = wb
                    dv = diag[j, pl.ds(r - OWN, h)] * c[j]
                    av = dv - nb[j]
                    add(0, c[j] * av)
                    if count > 1:
                        add(1, w * av)
                    if count > 2:
                        add(2, c[j] * dv)
                        add(3, c[j] * nb[j])
            return tuple(sums) if sums is not None else None

        steps = 4 if k == 3 else 8
        each = TILE // steps
        turn(v, OWN, each)
        if nxt is not None:
            for r in (OWN - 8, OWN + TILE):
                turn(v, r, 8)
                rows(r, 8, None)

        def step(i, sums, last=False):
            r = OWN + i * each if last else OWN + pl.multiple_of(i * each, 32)
            if not last:
                turn(v, r + each, each)
            for q in range(each // 32):
                sums = rows(r + q * 32, 32, sums)
            return sums

        z = jnp.zeros((8, 128), F32)
        sums = lax.fori_loop(0, steps - 1, step, (z,) * count)
        return step(steps - 1, sums, last=True)

    n = 0
    for k in range(4):
        phase(f"power{k}")
        for s in power(k):
            mom[n:n + 1] = jnp.sum(s, axis=0, keepdims=True)
            n += 1
    mom[11:16] = jnp.zeros((5, 128), F32)

    phase("lane_sum")
    t = jnp.sum(mom[...], axis=1, keepdims=True)
    red_a[ci] = jnp.sum(jnp.where(iota((16, 128), 0) == iota((16, 128), 1), t, 0.0), axis=0, keepdims=True)

    def reduce_start(buf, axis, me, size, sems):
        for d in range(1, size):
            pltpu.make_async_remote_copy(
                src_ref=buf.at[me], dst_ref=buf.at[me], send_sem=sems.at[0], recv_sem=sems.at[1],
                device_id={axis: lax.rem(me + d, size)}, device_id_type=MESH,
            ).start()

    def reduce_finish(buf, size, sems):
        wait_bytes(buf.at[pl.ds(0, size - 1)], sems.at[1])
        t = buf[0]
        for q in range(1, size):
            t = t + buf[q]
        return t

    reduce_start(red_a, "col", ci, ncol, sum_sem.at[0])
    phase("gather123")
    for k in range(1, 4):
        gather(k)
    vals[0] = vals[ncol]
    vals[ncol + 1] = vals[1]
    ar = Exchange(lambda p: vals.at[pl.ds(peer(p, 1), 3)], arrived, ar_s, ar_r, 1)
    vr = RowExchange(vals, arrived_row, vr_s, vr_r)
    for q in range(3):
        arrived[0, q] = vals[ci + q]
    phase("reduce_col")
    red_b[ri] = reduce_finish(red_a, ncol, sum_sem.at[0])
    reduce_start(red_b, "row", ri, nrow, sum_sem.at[1])
    phase("reduce_row")
    tot = reduce_finish(red_b, nrow, sum_sem.at[1])

    phase("solve")
    def m(q):
        return jnp.broadcast_to(jnp.sum(jnp.where(lane == q, tot, 0.0), axis=1, keepdims=True), (1, 128))

    eta = [m(q) for q in (0, 1, 4, 5, 8, 9, 10)]
    nu = [m(q) for q in (2, 3, 6, 7)]
    hm = [[eta[i + j] for j in range(4)] for i in range(4)]
    low = [[None] * 4 for _ in range(4)]
    piv = []
    for j in range(4):
        pj = hm[j][j]
        for q in range(j):
            pj = pj - low[j][q] * low[j][q] * piv[q]
        ok = pj > 1e-6 * hm[j][j]
        piv.append(pj)
        inv = jnp.where(ok, 1.0 / jnp.where(ok, pj, 1.0), 0.0)
        low[j][j] = inv
        for i in range(j + 1, 4):
            e = hm[i][j]
            for q in range(j):
                e = e - low[i][q] * low[j][q] * piv[q]
            low[i][j] = e * inv
    y = list(nu)
    for i in range(4):
        for q in range(i):
            y[i] = y[i] - low[i][q] * y[q]
    y = [y[i] * low[i][i] for i in range(4)]
    for i in (2, 1, 0):
        for q in range(i + 1, 4):
            y[i] = y[i] - low[q][i] * y[q]
    phase("combine")

    def combine(i, _):
        r = pl.multiple_of(i * 16, 16)
        for j in range(NB):
            rows = pl.ds(OWN + r, 16)
            a = y[0] * f0[j, rows]
            for k in range(1, 4):
                a = a + y[k] * field[k][j, rows]
            at = slice(j * 128, (j + 1) * 128)
            for x, buf in zip(parts(a, 2), (pa0, pb0)):
                buf[pl.ds(r, 16), at] = x
        return _

    lax.fori_loop(0, TILE // 16, combine, 0, unroll=4)
    for h in range(2):
        hs = slice(h * 256, (h + 1) * 256)
        fine_o[:, hs] = sum(dot(buf[...], perm[hs, :], NT) for buf in (pa0, pb0))

    fine_out = pltpu.make_async_copy(fine_o, fine_h, out_sem.at[0])
    fine_out.start()
    phase("wait_vals")
    coarse_wait(1, c1)
    coarse_wait(2, c2)
    i8, i16 = iota((8, 128), 0), iota((16, 128), 0)
    coef = jnp.concatenate(y, axis=0)

    def current(x):
        a = jnp.sum(coef * x, axis=0, keepdims=True)
        hi = a.astype(BF16).astype(F32)
        return hi, a - hi

    for p in range(ncol):
        ar.arrived(p)
        at = slice(p * 128, (p + 1) * 128)
        hot = crow[:, at]
        for n, x in enumerate(current(arrived[p, 1])):
            cva[n * 128:(n + 1) * 128, at] = hot * x.astype(BF16)
        for q, edge in ((0, GROUP - 1), (1, 0)):
            on = i8 * GROUP + edge == (held_side[p, 2 * q] & 127)
            x = [jnp.where(on, x, 0.0) for x in current(arrived[p, 2 * q])]
            cvb[q * 16:(q + 1) * 16, at] = jnp.concatenate(x, axis=0).astype(BF16)
    phase("sources")
    t = dot(cva[0:256, :], ccol[...], NT)
    src = t[:128] + t[128:]
    side = [dot(cvb[q * 16:(q + 1) * 16, :], side_hot[q], NT) for q in range(2)]
    phase("wait_rows")
    vr.arrived()
    for p in range(ncol):
        at = slice(p * 128, (p + 1) * 128)
        for q, edge in ((0, 127), (1, 0)):
            hi, lo = current(arrived_row[q, p])
            on = (held_row[q, p] >> 7) == edge
            x = jnp.where(i16 == 0, jnp.where(on, hi, 0.0), jnp.where(i16 == 1, jnp.where(on, lo, 0.0), 0.0))
            cvb[32 + q * 16:48 + q * 16, at] = x.astype(BF16)
    side += [dot(cvb[q * 16:(q + 1) * 16, :], side_hot[q], NT) for q in (2, 3)]
    phase("sweeps")
    u1 = p0 + rdiag * src
    beside1 = coarse_beside(
        u1,
        crecv[1, 0, 7:8] + crecv[2, 0, 7:8] * (side[2][0:1] + side[2][1:2]),
        crecv[1, 1, 0:1] + crecv[2, 1, 0:1] * (side[3][0:1] + side[3][1:2]),
        srecv[1, 0] + srecv[2, 0] * (side[0][0:8] + side[0][8:16]),
        srecv[1, 1] + srecv[2, 1] * (side[1][0:8] + side[1][8:16]),
    )
    coarse_o[...] = u1 + rdiag * (src + CG * beside1 - cdiag * u1)
    coarse_out = pltpu.make_async_copy(coarse_o, coarse_h, out_sem.at[1])
    coarse_out.start()
    phase("drain")
    for x in (rq, qs, rs, ar, qr, vr):
        x.sent()
    wait_bytes(red_a.at[pl.ds(0, ncol - 1)], sum_sem.at[0, 0])
    wait_bytes(red_b.at[pl.ds(0, nrow - 1)], sum_sem.at[1, 0])
    halo_sent(fcp)
    coarse_sent(c0)
    fine_out.wait()
    coarse_out.wait()
    phase("")


def hand_out(fine, coarse, fine_h, coarse_h, sem):
    copies = [pltpu.make_async_copy(fine, fine_h, sem.at[0]), pltpu.make_async_copy(coarse, coarse_h, sem.at[1])]
    for cp in copies:
        cp.start()
    for cp in copies:
        cp.wait()


def solution(mesh):
    nrow, ncol = mesh.shape["row"], mesh.shape["col"]
    slots = ncol * 128
    dma = pltpu.SemaphoreType.DMA

    def step(*args):
        anyspace = pl.BlockSpec(memory_space=pl.ANY)
        hbm = pl.BlockSpec(memory_space=pltpu.HBM)
        slab = (NB, TILE, 128)
        row = (ncol, 1, 128)
        fine, coarse = pl.pallas_call(
            functools.partial(kernel, nrow, ncol),
            out_shape=(
                pltpu.VMEM((TILE, TILE), F32),
                pltpu.VMEM((COARSE, COARSE), F32),
            ),
            in_specs=[hbm] * 8,
            out_specs=(anyspace, anyspace),
            scratch_shapes=[
                pltpu.VMEM((TILE, TILE), F32), pltpu.VMEM((TILE, TILE), I32), pltpu.VMEM((TILE, TILE), F32),
                pltpu.VMEM((TILE, TILE), BF16),
                pltpu.VMEM((TILE, slots), BF16), pltpu.VMEM((TILE, slots), BF16),
                pltpu.VMEM((TILE, slots), BF16), pltpu.VMEM((TILE, slots), BF16),
                *[pltpu.VMEM((NB + 1, ROWS, 128), F32)] * 4, pltpu.VMEM((4, ROWS, 128), F32), pltpu.VMEM((NB + 1, ROWS, 128), F32),
                pltpu.VMEM(slab, F32), pltpu.VMEM(slab, F32),
                *[pltpu.VMEM((TILE, TILE), BF16)] * 7, *[pltpu.VMEM((TILE, TILE), F8)] * 4, *[pltpu.VMEM((TILE, slots), F8)] * 3,
                pltpu.VMEM((ncol + 2, 1, 128), I32), pltpu.VMEM(row, I32),
                pltpu.VMEM((ncol, 3, 1, 128), I32), pltpu.VMEM((2, ncol, 1, 128), I32),
                pltpu.VMEM(row, F32), pltpu.VMEM(row, F32),
                pltpu.VMEM((ncol + 2, 4, 128), F32), pltpu.VMEM((ncol, 3, 4, 128), F32),
                pltpu.VMEM((2, ncol, 4, 128), F32), pltpu.VMEM((4, 128, slots), BF16),
                pltpu.VMEM((128, slots), BF16), pltpu.VMEM((128, slots), BF16),
                pltpu.VMEM((2, NB, 8, 128), F32), pltpu.VMEM((2, NB, 8, 128), F32),
                pltpu.VMEM((2, 8, TILE), F32), pltpu.VMEM((2, 8, TILE), F32),
                pltpu.VMEM((2, 4, 8, 128), F32), pltpu.VMEM((2, 2, 8, TILE), F32), pltpu.VMEM((2, 2, 8, 128), F32),
                pltpu.VMEM((16, 128), F32), pltpu.VMEM((ncol, 1, 128), F32), pltpu.VMEM((nrow, 1, 128), F32),
                pltpu.VMEM((256, 128), BF16),
                pltpu.VMEM((3, 128, 128), F32), pltpu.VMEM((3, 2, 8, 128), F32),
                pltpu.VMEM((3, 2, 8, 128), F32), pltpu.VMEM((3, 2, 8, 128), F32),
                pltpu.VMEM((TILE, TILE), F32), pltpu.VMEM((COARSE, COARSE), F32),
                pltpu.VMEM((COARSE, COARSE), F32), pltpu.VMEM((COARSE, COARSE), F32),
                pltpu.VMEM((1, slots), I32), pltpu.VMEM((1, slots), I32), pltpu.SMEM((1, ncol), I32),
                dma((3,)), dma((5,)), dma((2,)),
                *[dma(()), dma((2,))] * 3,
                pltpu.SemaphoreType.REGULAR((2,)),
                dma(()), dma((2,)), *[dma((2,))] * 4,
                dma((8,)), dma((2, 8)), dma((2, 2)),
                dma((3,)), dma((3, 3)),
            ],
            compiler_params=pltpu.CompilerParams(
                collective_id=0, has_side_effects=True, vmem_limit_bytes=50 << 20),
        )(*[pltpu.with_memory_space_constraint(x, pltpu.HBM) for x in args])
        return pl.pallas_call(
            hand_out,
            out_shape=(
                jax.ShapeDtypeStruct((TILE, TILE), F32),
                jax.ShapeDtypeStruct((COARSE, COARSE), F32),
            ),
            in_specs=[anyspace, anyspace],
            out_specs=(anyspace, anyspace),
            scratch_shapes=[dma((2,))],
        )(pltpu.with_memory_space_constraint(fine, pltpu.VMEM), pltpu.with_memory_space_constraint(coarse, pltpu.VMEM))

    spec = P("row", "col")
    return jax.shard_map(
        step, mesh=mesh, in_specs=(spec,) * 8, out_specs=(spec, spec), check_vma=False
    )
```

```python
import functools

import jax
import jax.numpy as jnp
from jax import lax
from jax.experimental import pallas as pl
from jax.experimental.pallas import tpu as pltpu
from jax.sharding import PartitionSpec as P

MESH = pl.DeviceIdType.MESH
F8 = jnp.float8_e4m3fn
HOT = 64.0
LOW = HOT * HOT
F32, BF16, I32 = jnp.float32, jnp.bfloat16, jnp.int32
GROUP = 16
NB = 4
OWN = 16
TILE = 512
ROWS = TILE + 2 * OWN
COARSE = 128
VIA = 2.0
CG = 4.0
RELAX = 0.8
NN = (((1,), (0,)), ((), ()))
NT = (((1,), (1,)), ((), ()))


def place(c):
    return (c & 3) * 128 + (c >> 2)


def iota(shape, dim):
    return lax.broadcasted_iota(I32, shape, dim)


def dot(a, b, dims):
    return lax.dot_general(a, b, dims, preferred_element_type=F32)


def parts(x, n):
    out = []
    for _ in range(n):
        p = x.astype(BF16)
        out.append(p)
        x = x - p.astype(F32)
    return out


class Phases:
    def __init__(self):
        self.open = None

    def __call__(self, name):
        if self.open is not None:
            self.open.__exit__(None, None, None)
        self.open = None
        if name:
            self.open = jax.named_scope(name)
            self.open.__enter__()


def peer_order(n):
    if n != 16:
        return list(range(n))
    return sorted(range(n), key=lambda d: min(d // 4, 4 - d // 4) + min(d % 4, 4 - d % 4))


def high_low(x):
    p = x.astype(BF16)
    return p, ((x - p.astype(F32)) * LOW).astype(F8)


def kernel(
    nrow, ncol,
    amp_h, mask_h, leak_h, cleak_h, cinit_h, vfine_h, vcoarse_h, vcount_h,
    fine_h, coarse_h,
    amp, mask, leak, perm, rt, ct, cva, cvb, f0, f1, f2, f3, turned, dinv, diag, inj, pa0, pa1, pa2, pa3, pb0, pb1, pb2, pb80, pb81, pb82, pb83, ct8, rt8, cvb8,
    req, held, held_side, held_row, look, atvia, vals, arrived, arrived_row, side_hot,
    crow, ccol, htop, hbot, hleft, hright, hcorner, csend, corner,
    mom, red_a, red_b, split, ubuf, seam, crecv, srecv, fine_o, coarse_o,
    cleak, cinit, vfine, vcoarse, vcount,
    in_sem, small_sem, out_sem, rq_s, rq_r, rs_s, rs_r, ar_s, ar_r,
    go, qs_s, qs_r, qr_s, qr_r, vr_s, vr_r, ha_s, ha_r, sum_sem, ce_s, ce_r,
):
    field, pa, pb8 = (f0, f1, f2, f3), (pa0, pa1, pa2, pa3), (pb80, pb81, pb82, pb83)
    slots = ncol * 128
    phase = Phases()
    phase("start")
    ri, ci = lax.axis_index("row"), lax.axis_index("col")

    small = []
    for n, (src, dst) in enumerate((
        (vcount_h, vcount), (vcoarse_h, vcoarse), (vfine_h, vfine), (cinit_h, cinit), (cleak_h, cleak)
    )):
        cp = pltpu.make_async_copy(src, dst, small_sem.at[n])
        cp.start()
        small.append(cp)
    loads = []
    for n, (src, dst) in enumerate(((leak_h, leak), (amp_h, amp), (mask_h, mask))):
        cp = pltpu.make_async_copy(src, dst, in_sem.at[n])
        cp.start()
        loads.append(cp)

    for buf in (htop, hbot, hleft, hright, hcorner, crecv, csend):
        buf[...] = jnp.zeros(buf.shape, F32)
    arrived_row[...] = jnp.zeros(arrived_row.shape, F32)
    held_row[...] = jnp.full(held_row.shape, -1, I32)

    phase("barrier")
    order = peer_order(ncol)

    def peer(p, sign):
        if ncol != 16:
            return lax.rem(ci + (order[p] if sign > 0 else ncol - order[p]), ncol)
        dy, dx = order[p] // 4, order[p] % 4
        y, x = ci // 4, lax.rem(ci, 4)
        if sign < 0:
            dy, dx = 4 - dy, 4 - dx
        return lax.rem(y + dy, 4) * 4 + lax.rem(x + dx, 4)

    bar = pltpu.get_barrier_semaphore()
    for d in range(1, ncol):
        pl.semaphore_signal(bar, inc=1, device_id={"col": lax.rem(ci + d, ncol)}, device_id_type=MESH)
    for d in range(1, nrow):
        pl.semaphore_signal(bar, inc=1, device_id={"row": lax.rem(ri + d, nrow)}, device_id_type=MESH)
    for dr in (1, nrow - 1):
        for dc in (1, ncol - 1):
            pl.semaphore_signal(
                bar, inc=1,
                device_id={"row": lax.rem(ri + dr, nrow), "col": lax.rem(ci + dc, ncol)},
                device_id_type=MESH,
            )
    phase("wait_small")
    for cp in small:
        cp.wait()
    lane = iota((1, 128), 1)

    def wait_bytes(ref, sem):
        pltpu.make_async_copy(ref, ref, sem).wait()

    half = ncol // 2

    class Exchange:
        def __init__(self, src, dst, ssem, rsem, sign):
            self.dst, self.ssem, self.rsem = dst, ssem, rsem
            for p in reversed(range(1, ncol)):
                pltpu.make_async_remote_copy(
                    src_ref=src(p), dst_ref=dst.at[p], send_sem=ssem, recv_sem=rsem.at[p // half],
                    device_id={"col": peer(p, sign)}, device_id_type=MESH,
                ).start()

        def arrived(self, p):
            if p == 1:
                wait_bytes(self.dst.at[pl.ds(1, half - 1)], self.rsem.at[0])
            if p == half:
                wait_bytes(self.dst.at[pl.ds(half, half)], self.rsem.at[1])

        def sent(self):
            wait_bytes(self.dst.at[pl.ds(1, ncol - 1)], self.ssem)

    class RowExchange:
        def __init__(self, src, dst, ssem, rsem):
            self.dst, self.ssem, self.rsem = dst, ssem, rsem
            self.sides = ((0, 1, ri < nrow - 1, ri > 0), (1, nrow - 1, ri > 0, ri < nrow - 1))
            for side, dr, to, _ in self.sides:

                @pl.when(to)
                def _():
                    for p in reversed(range(ncol)):
                        pltpu.make_async_remote_copy(
                            src_ref=src.at[1 + peer(p, 1)], dst_ref=dst.at[side, p],
                            send_sem=ssem.at[side], recv_sem=rsem.at[side],
                            device_id={"row": lax.rem(ri + dr, nrow), "col": peer(p, 1)}, device_id_type=MESH,
                        ).start()

        def arrived(self):
            for side, _, _, frm in self.sides:
                pl.when(frm)(lambda: wait_bytes(self.dst.at[side], self.rsem.at[side]))

        def sent(self):
            for side, _, to, _ in self.sides:
                pl.when(to)(lambda: wait_bytes(self.dst.at[side], self.ssem.at[side]))

    phase("requests")
    for p in reversed(range(ncol)):
        o = peer(p, 1)
        idx = vcoarse[:, pl.ds(pl.multiple_of(o * 128, 128), 128)]
        node = lax.shift_right_logical(idx, lax.full_like(idx, (slots).bit_length() - 1)) * 128 + (idx & 127)
        node = jnp.where(lane < vcount[0, o], node, -1)
        req[1 + o] = node
        if p == 0:
            held[0] = node
    req[0] = req[ncol]
    req[ncol + 1] = req[1]
    for q in range(3):
        held_side[0, q] = req[ci + q]
    phase("barrier_wait")
    pl.semaphore_wait(bar, ncol + nrow + 2)

    @pl.when(ri < nrow - 1)
    def _():
        pl.semaphore_signal(go.at[0], inc=1, device_id={"row": lax.rem(ri + 1, nrow)}, device_id_type=MESH)

    @pl.when(ri > 0)
    def _():
        pl.semaphore_signal(go.at[1], inc=1, device_id={"row": lax.rem(ri + nrow - 1, nrow)}, device_id_type=MESH)


    phase("send_req")
    rq = Exchange(lambda p: req.at[1 + peer(p, 1)], held, rq_s, rq_r, 1)

    phase("fine_onehot")
    for p in range(ncol):
        o = peer(p, 1)
        idx = vfine[:, pl.ds(pl.multiple_of(o * 128, 128), 128)]
        at = slice(p * 128, (p + 1) * 128)
        r = jnp.where(lane < vcount[0, o], idx >> 9, -1)
        c = place(idx & 511)
        for q in range(4):
            i = iota((128, 128), 0) + q * 128
            rt[q * 128:(q + 1) * 128, at] = jnp.where(i == r, 1.0, 0.0).astype(BF16)
            rt8[q * 128:(q + 1) * 128, at] = jnp.where(i == r, 1.0, 0.0).astype(F8)
            ct[q * 128:(q + 1) * 128, at] = jnp.where(i == c, HOT, 0.0).astype(BF16)
            ct8[q * 128:(q + 1) * 128, at] = jnp.where(i == c, 1.0 / HOT, 0.0).astype(F8)
    perm[...] = jnp.where(place(iota((TILE, TILE), 0)) == iota((TILE, TILE), 1), 1.0, 0.0).astype(BF16)
    phase("count_dot")
    loads[0].wait()
    pa2[...], pb2[...] = parts(leak[...], 2)
    for h in range(2):
        hs = slice(h * 256, (h + 1) * 256)
        t = (VIA * HOT) * dot(rt8[...], ct8[hs, :], NT)
        t = t + (dot(pa2[...], perm[:, hs], NN) + dot(pb2[...], perm[:, hs], NN))
        for q in range(2):
            j = 2 * h + q
            dg = 4.0 + t[:, q * 128:(q + 1) * 128]
            diag[j] = dg
            dinv[j, OWN:OWN + TILE] = 1.0 / dg

    row8 = iota((8, 128), 1)

    def halo_copies(f, src):
        up, dn = lax.rem(ri + nrow - 1, nrow), lax.rem(ri + 1, nrow)
        lf, rg = lax.rem(ci + ncol - 1, ncol), lax.rem(ci + 1, ncol)
        hu, hd, hl, hr = ri > 0, ri < nrow - 1, ci > 0, ci < ncol - 1
        first, last = pl.ds(OWN, 8), pl.ds(OWN + TILE - 8, 8)
        own = pl.ds(0, NB)
        plan = (
            (hu, hd, src.at[own, first], hbot.at[f], {"row": up}),
            (hd, hu, src.at[own, last], htop.at[f], {"row": dn}),
            (hl, hr, csend.at[f, 0], hright.at[f], {"col": lf}),
            (hr, hl, csend.at[f, 1], hleft.at[f], {"col": rg}),
            (hu & hl, hd & hr, corner.at[f, 0], hcorner.at[f, 0], {"row": up, "col": lf}),
            (hu & hr, hd & hl, corner.at[f, 0], hcorner.at[f, 1], {"row": up, "col": rg}),
            (hd & hl, hu & hr, corner.at[f, 1], hcorner.at[f, 2], {"row": dn, "col": lf}),
            (hd & hr, hu & hl, corner.at[f, 1], hcorner.at[f, 3], {"row": dn, "col": rg}),
        )
        out = []
        for n, (to, frm, s, d, dev) in enumerate(plan):
            cp = pltpu.make_async_remote_copy(
                src_ref=s, dst_ref=d, send_sem=ha_s.at[n], recv_sem=ha_r.at[f, n],
                device_id=dev, device_id_type=MESH,
            )
            out.append((to, frm, cp))
        return out

    def halo_start(f, src):
        own = slice(OWN, OWN + TILE)
        for j in range(NB):
            t = jnp.transpose(src[j, own])
            csend[f, 0, j:j + 1] = t[0:1]
            csend[f, 1, 4 + j:5 + j] = t[127:128]
        for e, r in enumerate((OWN, OWN + TILE - 8)):
            x = jnp.zeros((8, 128), F32)
            for j in range(NB):
                b = src[j, r:r + 8]
                x = jnp.where(row8 == j, pltpu.roll(b, j, 1) if j else b, x)
                x = jnp.where(row8 == 124 + j, pltpu.roll(b, 125 + j, 1) if j < 3 else b, x)
            corner[f, e] = x
        cps = halo_copies(f, src)
        for to, _, cp in cps:
            pl.when(to)(cp.start)
        return cps

    def halo_finish(f, dst, cps):
        for _, frm, cp in cps:
            pl.when(frm)(cp.wait_recv)
        dst[0:NB, OWN - 8:OWN] = htop[f]
        dst[0:NB, OWN + TILE:OWN + TILE + 8] = hbot[f]
        x = jnp.concatenate([hright[f], jnp.zeros((112, TILE), F32), hleft[f]], axis=0)
        dst[NB, OWN:OWN + TILE] = jnp.transpose(x)
        near = row8 < 64
        dst[NB, OWN + TILE:OWN + TILE + 8] = jnp.where(near, hcorner[f, 0], hcorner[f, 1])
        dst[NB, OWN - 8:OWN] = jnp.where(near, hcorner[f, 2], hcorner[f, 3])

    def halo_sent(cps):
        for n, (to, _, _) in enumerate(cps):
            both = htop if n < 2 else hleft if n < 4 else corner.at[0]
            pl.when(to)(lambda: wait_bytes(both, ha_s.at[n]))

    for buf in (dinv, f0, f1, f2, f3):
        buf[:, 0:8] = jnp.zeros((NB + 1, 8, 128), F32)
        buf[:, ROWS - 8:ROWS] = jnp.zeros((NB + 1, 8, 128), F32)
    dcp = halo_start(0, dinv)
    phase("send_side")
    pl.when(ri > 0)(lambda: pl.semaphore_wait(go.at[0], 1))
    pl.when(ri < nrow - 1)(lambda: pl.semaphore_wait(go.at[1], 1))
    qs = Exchange(lambda p: req.at[pl.ds(peer(p, 1), 3)], held_side, qs_s, qs_r, 1)
    qr = RowExchange(req, held_row, qr_s, qr_r)

    phase("wait_req")
    u = cinit[...]
    split[0:256] = jnp.concatenate(parts(u, 2), axis=0)
    ci128 = iota((128, 128), 0)
    for p in range(ncol):
        rq.arrived(p)
        at = slice(p * 128, (p + 1) * 128)
        idx = held[p]
        crow[:, at] = jnp.where(ci128 == (idx >> 7), 1.0, 0.0).astype(BF16)
        ccol[:, at] = jnp.where(ci128 == (idx & 127), 1.0, 0.0).astype(BF16)
    phase("lookup")
    for n in range(ncol // 2):
        at = slice(n * 256, (n + 1) * 256)
        t = dot(split[0:256], ccol[:, at], NN)
        t = jnp.sum((t[:128] + t[128:]) * crow[:, at].astype(F32), axis=0, keepdims=True)
        for p in (2 * n, 2 * n + 1):
            (look if p else atvia)[p] = t[:, (p - 2 * n) * 128:(p - 2 * n + 1) * 128]
    rs = Exchange(lambda p: look.at[p], atvia, rs_s, rs_r, -1)

    phase("coarse_diag")
    cdiag = 4.0 * CG + cleak[...] + VIA * dot(crow[...], ccol[...], NT)
    rdiag = RELAX / cdiag

    def coarse_start(s, u):
        ubuf[s] = u
        seam_t = jnp.transpose(u)
        for e, j in enumerate((0, GROUP - 1)):
            seam[s, e] = jnp.concatenate(
                [seam_t[g * GROUP + j:g * GROUP + j + 1] for g in range(128 // GROUP)], axis=0
            )
        up, dn = lax.rem(ri + nrow - 1, nrow), lax.rem(ri + 1, nrow)
        lf, rg = lax.rem(ci + ncol - 1, ncol), lax.rem(ci + 1, ncol)
        true = ri >= 0
        plan = (
            (ri > 0, ri < nrow - 1, ubuf.at[s, pl.ds(0, 8)], crecv.at[s, 1], {"row": up}),
            (ri < nrow - 1, ri > 0, ubuf.at[s, pl.ds(120, 8)], crecv.at[s, 0], {"row": dn}),
            (None, None, seam.at[s, 0], srecv.at[s, 1], {"col": lf}),
            (None, None, seam.at[s, 1], srecv.at[s, 0], {"col": rg}),
        )
        cps = []
        for n, (to, frm, sr, ds, dev) in enumerate(plan):
            cp = pltpu.make_async_remote_copy(
                src_ref=sr, dst_ref=ds, send_sem=ce_s.at[min(n, 2)], recv_sem=ce_r.at[s, min(n, 2)],
                device_id=dev, device_id_type=MESH,
            )
            if to is None:
                cp.start()
            else:
                pl.when(to)(cp.start)
            cps.append((to, frm, cp))
        return cps

    def coarse_wait(s, cps):
        for _, frm, cp in cps[:2]:
            pl.when(frm)(cp.wait_recv)
        wait_bytes(srecv.at[s], ce_r.at[s, 2])

    def coarse_beside(u, up, dn, fl, fr):
        li, si = iota((128, 128), 1), ci128
        up = jnp.where(si == 0, up, pltpu.roll(u, 1, 0))
        dn = jnp.where(si == 127, dn, pltpu.roll(u, 127, 0))
        g = iota((8, 128), 0)
        fl = jnp.where(ci == 0, jnp.where(g == 0, 0.0, pltpu.roll(fl, 1, 0)), fl)
        fr = jnp.where(ci == ncol - 1, jnp.where(g == 7, 0.0, pltpu.roll(fr, 7, 0)), fr)

        def spread(x):
            return jnp.concatenate([jnp.broadcast_to(x[q:q + 1], (GROUP, 128)) for q in range(8)], axis=0)

        x = jnp.transpose(jnp.where(si % GROUP == 0, spread(fl), spread(fr)))
        left = jnp.where(li % GROUP == 0, x, pltpu.roll(u, 1, 1))
        right = jnp.where(li % GROUP == GROUP - 1, x, pltpu.roll(u, 127, 1))
        return up + dn + left + right

    def coarse_sent(cps):
        for n in range(2):
            pl.when(cps[n][0])(lambda: wait_bytes(ubuf.at[0, pl.ds(0, 24)], ce_s.at[n]))
        wait_bytes(seam, ce_s.at[2])

    phase("coarse_start")
    c0 = coarse_start(0, u)
    phase("load")
    for cp in loads[1:]:
        cp.wait()
    pa1[...], pb1[...] = parts(amp[...] * mask[...].astype(F32), 2)
    for h in range(2):
        hs = slice(h * 256, (h + 1) * 256)
        t = dot(pa1[...], perm[:, hs], NN) + dot(pb1[...], perm[:, hs], NN)
        for q in range(2):
            inj[2 * h + q] = t[:, q * 128:(q + 1) * 128]

    def make_inj(o):
        at = pl.ds(pl.multiple_of(o * 128, 128), 128)
        p = parts(atvia[o], 2)
        col = ct[:, at]
        cva[:, at] = col * p[0]
        cvb[:, at] = col * p[1]

    v0 = f0
    for part in range(2):
        phase(f"wait_resp{part}")
        for p in range(part * half, (part + 1) * half):
            rs.arrived(p)
            at = slice(p * 128, (p + 1) * 128)
            c = vfine[:, pl.ds(pl.multiple_of(peer(p, 1) * 128, 128), 128)]
            c = place(c & 511)
            v = atvia[p]
            va = v.astype(BF16).astype(F32)
            vb = v - va
            for q in range(4):
                hot = iota((128, 128), 0) + q * 128 == c
                cva[q * 128:(q + 1) * 128, at] = jnp.where(hot, va, 0.0).astype(BF16)
                cvb8[q * 128:(q + 1) * 128, at] = jnp.where(hot, vb * LOW, 0.0).astype(F8)
        phase(f"inject_dot{part}")
        ks = slice(part * half * 128, (part + 1) * half * 128)
        for h in range(2):
            hs = slice(h * 256, (h + 1) * 256)
            t = dot(rt[:, ks], cva[hs, ks], NT) + (1.0 / LOW) * dot(rt8[:, ks], cvb8[hs, ks], NT)
            for q in range(2):
                j = 2 * h + q
                tq = VIA * t[:, q * 128:(q + 1) * 128]
                if part == 0:
                    inj[j] = inj[j] + tq
                else:
                    z = (inj[j] + tq) * dinv[j, OWN:OWN + TILE]
                    v0[j, OWN:OWN + TILE] = z
                    za, zb = high_low(z)
                    pa0[:, j * 128:(j + 1) * 128] = za
                    pb8[0][:, j * 128:(j + 1) * 128] = zb
    phase("halo_start")
    fcp = halo_start(1, v0)

    def gather_part(k, n):
        at = slice(n * 256, n * 256 + 256) if isinstance(n, int) else pl.ds(pl.multiple_of(n * 256, 256), 256)
        t = dot(pa[k][...], ct[:, at], NN) + dot(pb8[k][...], ct8[:, at], NN)
        t = (VIA / HOT) * jnp.sum(t * rt[:, at].astype(F32), axis=0, keepdims=True)
        for p in (2 * n, 2 * n + 1):
            vals[1 + peer(p, 1), k:k + 1] = t[:, (p - 2 * n) * 128:(p - 2 * n + 1) * 128]

    def gather(k):
        for n in range(ncol // 2):
            gather_part(k, n)

    phase("gather0")
    gather(0)
    phase("sweep_pre")
    coarse_wait(0, c0)
    p0 = u + rdiag * (
        CG * coarse_beside(u, crecv[0, 0, 7:8], crecv[0, 1, 0:1], srecv[0, 0], srecv[0, 1]) - cdiag * u
    )
    c1 = coarse_start(1, p0)
    c2 = coarse_start(2, rdiag)
    phase("side_hot")
    for p in (1, half):
        qs.arrived(p)
    qr.arrived()
    for p in range(ncol):
        at = slice(p * 128, (p + 1) * 128)
        nodes = (held_side[p, 0] >> 7, held_side[p, 2] >> 7, held_row[0, p] & 127, held_row[1, p] & 127)
        for q, x in enumerate(nodes):
            side_hot[q, :, at] = jnp.where(ci128 == x, 1.0, 0.0).astype(BF16)
    phase("dinv_finish")
    halo_finish(0, dinv, dcp)
    phase("halo_finish")
    halo_finish(1, v0, fcp)

    phase("powers")
    def turn(v, r, h):
        rows = pl.ds(r, h)
        first, last, halo = v[0, rows], v[NB - 1, rows], v[NB, rows]
        turned[0, rows] = pltpu.roll(last, 1, 1)
        turned[1, rows] = pltpu.roll(halo, 1, 1)
        turned[2, rows] = pltpu.roll(first, 127, 1)
        turned[3, rows] = pltpu.roll(halo, 127, 1)

    def beside(v, r, h):
        lanes = iota((h, 128), 1)
        first_lane, last_lane = lanes == 0, lanes == 127
        rows = pl.ds(r, h)
        c = [v[j, rows] for j in range(NB + 1)]
        last_r, halo_r, first_l, halo_l = (turned[q, rows] for q in range(4))
        left = [jnp.where(first_lane, halo_r, last_r), *c[:NB - 1], jnp.where(first_lane, last_r, halo_r)]
        right = [*c[1:NB], jnp.where(last_lane, halo_l, first_l), jnp.where(last_lane, first_l, halo_l)]
        out = [
            v[j, pl.ds(r - 1, h)] + v[j, pl.ds(r + 1, h)] + left[j] + right[j] for j in range(NB + 1)
        ]
        return c, out

    def power(k):
        v, nxt = field[k], field[k + 1] if k < 3 else None
        count = (4, 4, 2, 1)[k]

        def rows(r, h, sums):
            c, nb = beside(v, r, h)
            sums = list(sums) if sums is not None else None

            def add(n, x):
                for q in range(h // 8):
                    sums[n] = sums[n] + x[q * 8:(q + 1) * 8]

            for j in range(NB + 1):
                w = None
                if nxt is not None:
                    w = dinv[j, pl.ds(r, h)] * nb[j]
                    nxt[j, pl.ds(r, h)] = w
                if sums is not None and j < NB:
                    if nxt is not None:
                        wa, wb = high_low(w)
                        pa[k + 1][pl.ds(r - OWN, h), j * 128:(j + 1) * 128] = wa
                        pb8[k + 1][pl.ds(pl.multiple_of(r - OWN, 32), h), j * 128:(j + 1) * 128] = wb
                    dv = diag[j, pl.ds(r - OWN, h)] * c[j]
                    av = dv - nb[j]
                    add(0, c[j] * av)
                    if count > 1:
                        add(1, w * av)
                    if count > 2:
                        add(2, c[j] * dv)
                        add(3, c[j] * nb[j])
            return tuple(sums) if sums is not None else None

        steps = 4 if k == 3 else 8
        each = TILE // steps
        turn(v, OWN, each)
        if nxt is not None:
            for r in (OWN - 8, OWN + TILE):
                turn(v, r, 8)
                rows(r, 8, None)

        def step(i, sums, last=False):
            r = OWN + i * each if last else OWN + pl.multiple_of(i * each, 32)
            if not last:
                turn(v, r + each, each)
            for q in range(each // 32):
                sums = rows(r + q * 32, 32, sums)
            return sums

        z = jnp.zeros((8, 128), F32)
        sums = lax.fori_loop(0, steps - 1, step, (z,) * count)
        return step(steps - 1, sums, last=True)

    n = 0
    for k in range(4):
        phase(f"power{k}")
        for s in power(k):
            mom[n:n + 1] = jnp.sum(s, axis=0, keepdims=True)
            n += 1
    mom[11:16] = jnp.zeros((5, 128), F32)

    phase("lane_sum")
    t = jnp.sum(mom[...], axis=1, keepdims=True)
    red_a[ci] = jnp.sum(jnp.where(iota((16, 128), 0) == iota((16, 128), 1), t, 0.0), axis=0, keepdims=True)

    def reduce_start(buf, axis, me, size, sems):
        for d in range(1, size):
            pltpu.make_async_remote_copy(
                src_ref=buf.at[me], dst_ref=buf.at[me], send_sem=sems.at[0], recv_sem=sems.at[1],
                device_id={axis: lax.rem(me + d, size)}, device_id_type=MESH,
            ).start()

    def reduce_finish(buf, size, sems):
        wait_bytes(buf.at[pl.ds(0, size - 1)], sems.at[1])
        t = buf[0]
        for q in range(1, size):
            t = t + buf[q]
        return t

    reduce_start(red_a, "col", ci, ncol, sum_sem.at[0])
    phase("gather123")
    for k in range(1, 4):
        gather(k)
    vals[0] = vals[ncol]
    vals[ncol + 1] = vals[1]
    ar = Exchange(lambda p: vals.at[pl.ds(peer(p, 1), 3)], arrived, ar_s, ar_r, 1)
    vr = RowExchange(vals, arrived_row, vr_s, vr_r)
    for q in range(3):
        arrived[0, q] = vals[ci + q]
    phase("reduce_col")
    red_b[ri] = reduce_finish(red_a, ncol, sum_sem.at[0])
    reduce_start(red_b, "row", ri, nrow, sum_sem.at[1])
    phase("reduce_row")
    tot = reduce_finish(red_b, nrow, sum_sem.at[1])

    phase("solve")
    def m(q):
        return jnp.broadcast_to(jnp.sum(jnp.where(lane == q, tot, 0.0), axis=1, keepdims=True), (1, 128))

    eta = [m(q) for q in (0, 1, 4, 5, 8, 9, 10)]
    nu = [m(q) for q in (2, 3, 6, 7)]
    hm = [[eta[i + j] for j in range(4)] for i in range(4)]
    low = [[None] * 4 for _ in range(4)]
    piv = []
    for j in range(4):
        pj = hm[j][j]
        for q in range(j):
            pj = pj - low[j][q] * low[j][q] * piv[q]
        ok = pj > 1e-6 * hm[j][j]
        piv.append(pj)
        inv = jnp.where(ok, 1.0 / jnp.where(ok, pj, 1.0), 0.0)
        low[j][j] = inv
        for i in range(j + 1, 4):
            e = hm[i][j]
            for q in range(j):
                e = e - low[i][q] * low[j][q] * piv[q]
            low[i][j] = e * inv
    y = list(nu)
    for i in range(4):
        for q in range(i):
            y[i] = y[i] - low[i][q] * y[q]
    y = [y[i] * low[i][i] for i in range(4)]
    for i in (2, 1, 0):
        for q in range(i + 1, 4):
            y[i] = y[i] - low[q][i] * y[q]
    phase("combine")

    def combine(i, _):
        r = pl.multiple_of(i * 16, 16)
        for j in range(NB):
            rows = pl.ds(OWN + r, 16)
            a = y[0] * f0[j, rows]
            for k in range(1, 4):
                a = a + y[k] * field[k][j, rows]
            at = slice(j * 128, (j + 1) * 128)
            for x, buf in zip(parts(a, 2), (pa0, pb0)):
                buf[pl.ds(r, 16), at] = x
        return _

    lax.fori_loop(0, TILE // 16, combine, 0, unroll=4)
    for h in range(2):
        hs = slice(h * 256, (h + 1) * 256)
        fine_o[:, hs] = sum(dot(buf[...], perm[hs, :], NT) for buf in (pa0, pb0))

    fine_out = pltpu.make_async_copy(fine_o, fine_h, out_sem.at[0])
    fine_out.start()
    phase("wait_vals")
    coarse_wait(1, c1)
    coarse_wait(2, c2)
    i8, i16 = iota((8, 128), 0), iota((16, 128), 0)
    coef = jnp.concatenate(y, axis=0)

    def current(x):
        a = jnp.sum(coef * x, axis=0, keepdims=True)
        hi = a.astype(BF16).astype(F32)
        return hi, a - hi

    for p in range(ncol):
        ar.arrived(p)
        at = slice(p * 128, (p + 1) * 128)
        hot = crow[:, at]
        for n, x in enumerate(current(arrived[p, 1])):
            cva[n * 128:(n + 1) * 128, at] = hot * x.astype(BF16)
        for q, edge in ((0, GROUP - 1), (1, 0)):
            on = i8 * GROUP + edge == (held_side[p, 2 * q] & 127)
            x = [jnp.where(on, x, 0.0) for x in current(arrived[p, 2 * q])]
            cvb[q * 16:(q + 1) * 16, at] = jnp.concatenate(x, axis=0).astype(BF16)
    phase("sources")
    t = dot(cva[0:256, :], ccol[...], NT)
    src = t[:128] + t[128:]
    side = [dot(cvb[q * 16:(q + 1) * 16, :], side_hot[q], NT) for q in range(2)]
    phase("wait_rows")
    vr.arrived()
    for p in range(ncol):
        at = slice(p * 128, (p + 1) * 128)
        for q, edge in ((0, 127), (1, 0)):
            hi, lo = current(arrived_row[q, p])
            on = (held_row[q, p] >> 7) == edge
            x = jnp.where(i16 == 0, jnp.where(on, hi, 0.0), jnp.where(i16 == 1, jnp.where(on, lo, 0.0), 0.0))
            cvb[32 + q * 16:48 + q * 16, at] = x.astype(BF16)
    side += [dot(cvb[q * 16:(q + 1) * 16, :], side_hot[q], NT) for q in (2, 3)]
    phase("sweeps")
    u1 = p0 + rdiag * src
    beside1 = coarse_beside(
        u1,
        crecv[1, 0, 7:8] + crecv[2, 0, 7:8] * (side[2][0:1] + side[2][1:2]),
        crecv[1, 1, 0:1] + crecv[2, 1, 0:1] * (side[3][0:1] + side[3][1:2]),
        srecv[1, 0] + srecv[2, 0] * (side[0][0:8] + side[0][8:16]),
        srecv[1, 1] + srecv[2, 1] * (side[1][0:8] + side[1][8:16]),
    )
    coarse_o[...] = u1 + rdiag * (src + CG * beside1 - cdiag * u1)
    coarse_out = pltpu.make_async_copy(coarse_o, coarse_h, out_sem.at[1])
    coarse_out.start()
    phase("drain")
    for x in (rq, qs, rs, ar, qr, vr):
        x.sent()
    wait_bytes(red_a.at[pl.ds(0, ncol - 1)], sum_sem.at[0, 0])
    wait_bytes(red_b.at[pl.ds(0, nrow - 1)], sum_sem.at[1, 0])
    halo_sent(fcp)
    coarse_sent(c0)
    fine_out.wait()
    coarse_out.wait()
    phase("")


def hand_out(fine, coarse, fine_h, coarse_h, sem):
    copies = [pltpu.make_async_copy(fine, fine_h, sem.at[0]), pltpu.make_async_copy(coarse, coarse_h, sem.at[1])]
    for cp in copies:
        cp.start()
    for cp in copies:
        cp.wait()


def solution(mesh):
    nrow, ncol = mesh.shape["row"], mesh.shape["col"]
    slots = ncol * 128
    dma = pltpu.SemaphoreType.DMA

    def step(*args):
        anyspace = pl.BlockSpec(memory_space=pl.ANY)
        hbm = pl.BlockSpec(memory_space=pltpu.HBM)
        slab = (NB, TILE, 128)
        row = (ncol, 1, 128)
        fine, coarse = pl.pallas_call(
            functools.partial(kernel, nrow, ncol),
            out_shape=(
                pltpu.VMEM((TILE, TILE), F32),
                pltpu.VMEM((COARSE, COARSE), F32),
            ),
            in_specs=[hbm] * 8,
            out_specs=(anyspace, anyspace),
            scratch_shapes=[
                pltpu.VMEM((TILE, TILE), F32), pltpu.VMEM((TILE, TILE), I32), pltpu.VMEM((TILE, TILE), F32),
                pltpu.VMEM((TILE, TILE), BF16),
                pltpu.VMEM((TILE, slots), BF16), pltpu.VMEM((TILE, slots), BF16),
                pltpu.VMEM((TILE, slots), BF16), pltpu.VMEM((TILE, slots), BF16),
                *[pltpu.VMEM((NB + 1, ROWS, 128), F32)] * 4, pltpu.VMEM((4, ROWS, 128), F32), pltpu.VMEM((NB + 1, ROWS, 128), F32),
                pltpu.VMEM(slab, F32), pltpu.VMEM(slab, F32),
                *[pltpu.VMEM((TILE, TILE), BF16)] * 7, *[pltpu.VMEM((TILE, TILE), F8)] * 4, *[pltpu.VMEM((TILE, slots), F8)] * 3,
                pltpu.VMEM((ncol + 2, 1, 128), I32), pltpu.VMEM(row, I32),
                pltpu.VMEM((ncol, 3, 1, 128), I32), pltpu.VMEM((2, ncol, 1, 128), I32),
                pltpu.VMEM(row, F32), pltpu.VMEM(row, F32),
                pltpu.VMEM((ncol + 2, 4, 128), F32), pltpu.VMEM((ncol, 3, 4, 128), F32),
                pltpu.VMEM((2, ncol, 4, 128), F32), pltpu.VMEM((4, 128, slots), BF16),
                pltpu.VMEM((128, slots), BF16), pltpu.VMEM((128, slots), BF16),
                pltpu.VMEM((2, NB, 8, 128), F32), pltpu.VMEM((2, NB, 8, 128), F32),
                pltpu.VMEM((2, 8, TILE), F32), pltpu.VMEM((2, 8, TILE), F32),
                pltpu.VMEM((2, 4, 8, 128), F32), pltpu.VMEM((2, 2, 8, TILE), F32), pltpu.VMEM((2, 2, 8, 128), F32),
                pltpu.VMEM((16, 128), F32), pltpu.VMEM((ncol, 1, 128), F32), pltpu.VMEM((nrow, 1, 128), F32),
                pltpu.VMEM((256, 128), BF16),
                pltpu.VMEM((3, 128, 128), F32), pltpu.VMEM((3, 2, 8, 128), F32),
                pltpu.VMEM((3, 2, 8, 128), F32), pltpu.VMEM((3, 2, 8, 128), F32),
                pltpu.VMEM((TILE, TILE), F32), pltpu.VMEM((COARSE, COARSE), F32),
                pltpu.VMEM((COARSE, COARSE), F32), pltpu.VMEM((COARSE, COARSE), F32),
                pltpu.VMEM((1, slots), I32), pltpu.VMEM((1, slots), I32), pltpu.SMEM((1, ncol), I32),
                dma((3,)), dma((5,)), dma((2,)),
                *[dma(()), dma((2,))] * 3,
                pltpu.SemaphoreType.REGULAR((2,)),
                dma(()), dma((2,)), *[dma((2,))] * 4,
                dma((8,)), dma((2, 8)), dma((2, 2)),
                dma((3,)), dma((3, 3)),
            ],
            compiler_params=pltpu.CompilerParams(
                collective_id=0, has_side_effects=True, vmem_limit_bytes=50 << 20),
        )(*[pltpu.with_memory_space_constraint(x, pltpu.HBM) for x in args])
        return pl.pallas_call(
            hand_out,
            out_shape=(
                jax.ShapeDtypeStruct((TILE, TILE), F32),
                jax.ShapeDtypeStruct((COARSE, COARSE), F32),
            ),
            in_specs=[anyspace, anyspace],
            out_specs=(anyspace, anyspace),
            scratch_shapes=[dma((2,))],
        )(pltpu.with_memory_space_constraint(fine, pltpu.VMEM), pltpu.with_memory_space_constraint(coarse, pltpu.VMEM))

    spec = P("row", "col")
    return jax.shard_map(
        step, mesh=mesh, in_specs=(spec,) * 8, out_specs=(spec, spec), check_vma=False
    )
```
